8 devices in a mesh: dp: 1 (over z), col: 2 (over y), row: 4 (over x, core).
Axes of the slice: x: 2, y: 2, z: 1, core: 2. Of those that a mesh axis runs over, the one named last changes fastest.
Arguments:
- latent: bfloat16 [16, 16, 96, 384], P('dp', 'row', 'col')
- t_emb: bfloat16 [16, 768], P('dp')
- res_norm: bfloat16 [2, 2, 2, 384], replicated
- res_conv: bfloat16 [2, 2, 3, 3, 384, 384], replicated
- res_temb: bfloat16 [2, 768, 384], replicated
- attn_norm: bfloat16 [2, 384], replicated
- attn_proj: bfloat16 [4, 12, 384, 32], replicated
Outputs:
- output: bfloat16 [16, 16, 96, 384], P('dp', 'row', 'col')
All inputs are finite; a program needn't handle non-finite values.
Results may differ from the reference program's by a relative error of at most 0.00941283.
Values are sent between devices in bfloat16 or wider.
A program may use at most 1 GiB of HBM per device.

```python
import jax
import jax.numpy as jnp
from jax import lax

BATCH = 16
HEIGHT = 16
WIDTH = 96
CHANNELS = 384
HEADS = 12
TEMB_DIM = 768
GROUPS = 32
Q_BLOCK = 192
EPS = 1e-5
HEAD_DIM = CHANNELS // HEADS


def setup_inputs(seed: int = 0, part: int = 0) -> dict:
    part_keys = jax.random.split(jax.random.fold_in(jax.random.key(seed), part), 3)
    shared_keys = jax.random.split(jax.random.key(seed + 1), 5)
    base_noise = jax.random.normal(part_keys[0], (BATCH, HEIGHT, WIDTH, CHANNELS), jnp.float32)
    slopes = 1.5 * jax.random.normal(part_keys[1], (2, BATCH, 1, 1, CHANNELS), jnp.float32)
    ramp_rows = jnp.linspace(-1.0, 1.0, HEIGHT)[None, :, None, None]
    ramp_cols = jnp.linspace(-1.0, 1.0, WIDTH)[None, None, :, None]
    latent = base_noise + slopes[0] * ramp_rows + slopes[1] * ramp_cols
    t_emb = jax.random.normal(part_keys[2], (BATCH, TEMB_DIM), jnp.float32)
    norm_draw = jax.random.normal(shared_keys[0], (2, 2, 2, CHANNELS), jnp.float32)
    res_norm = jnp.stack([1.0 + 0.3 * norm_draw[:, :, 0], 0.5 * norm_draw[:, :, 1]], axis=2)
    res_conv = jax.random.normal(shared_keys[1], (2, 2, 3, 3, CHANNELS, CHANNELS), jnp.float32) * (9 * CHANNELS) ** -0.5
    res_temb = jax.random.normal(shared_keys[2], (2, TEMB_DIM, CHANNELS), jnp.float32) * TEMB_DIM ** -0.5
    attn_draw = jax.random.normal(shared_keys[3], (2, CHANNELS), jnp.float32)
    attn_norm = jnp.stack([1.0 + 0.3 * attn_draw[0], 0.5 * attn_draw[1]])
    proj_gain = jnp.array([1.5, 1.5, 1.0, 1.5], jnp.float32)[:, None, None, None]
    attn_proj = jax.random.normal(shared_keys[4], (4, HEADS, CHANNELS, HEAD_DIM), jnp.float32) * proj_gain * CHANNELS ** -0.5
    return {
        'latent': latent.astype(jnp.bfloat16),
        't_emb': t_emb.astype(jnp.bfloat16),
        'res_norm': res_norm.astype(jnp.bfloat16),
        'res_conv': res_conv.astype(jnp.bfloat16),
        'res_temb': res_temb.astype(jnp.bfloat16),
        'attn_norm': attn_norm.astype(jnp.bfloat16),
        'attn_proj': attn_proj.astype(jnp.bfloat16),
    }


def group_norm(values, gn_scale, gn_shift):
    group_ch = CHANNELS // GROUPS
    grouped = values.astype(jnp.float32).reshape(BATCH, HEIGHT, WIDTH, GROUPS, group_ch)
    elem_count = HEIGHT * WIDTH * group_ch
    mean_val = jnp.sum(grouped, axis=(1, 2, 4)) / elem_count
    mean_sq = jnp.sum(grouped * grouped, axis=(1, 2, 4)) / elem_count
    inv_std = lax.rsqrt(mean_sq - mean_val * mean_val + EPS)
    normed = (grouped - mean_val[:, None, None, :, None]) * inv_std[:, None, None, :, None]
    return normed.reshape(values.shape) * gn_scale.astype(jnp.float32) + gn_shift.astype(jnp.float32)


def conv3x3(acts_in, kernel):
    return lax.conv_general_dilated(acts_in.astype(jnp.float32), kernel.astype(jnp.float32), (1, 1), ((1, 1), (1, 1)), dimension_numbers=('NHWC', 'HWIO', 'NHWC'))


def res_block(latent, t_emb, norm_par, kernels, w_temb):
    t_act = jax.nn.silu(t_emb.astype(jnp.float32)).astype(jnp.bfloat16)
    t_proj = jnp.dot(t_act, w_temb, preferred_element_type=jnp.float32)
    first_act = jax.nn.silu(group_norm(latent, norm_par[0, 0], norm_par[0, 1])).astype(jnp.bfloat16)
    hidden = (conv3x3(first_act, kernels[0]) + t_proj[:, None, None, :]).astype(jnp.bfloat16)
    second_act = jax.nn.silu(group_norm(hidden, norm_par[1, 0], norm_par[1, 1])).astype(jnp.bfloat16)
    return (latent.astype(jnp.float32) + conv3x3(second_act, kernels[1])).astype(jnp.bfloat16)


def attn_block(latent, norm_par, proj_w):
    n_tok = HEIGHT * WIDTH
    normed = group_norm(latent, norm_par[0], norm_par[1]).astype(jnp.bfloat16).reshape(BATCH, n_tok, CHANNELS)
    qkv_all = jnp.einsum('bnc,khcd->kbnhd', normed.astype(jnp.float32), proj_w[:3].astype(jnp.float32)).astype(jnp.bfloat16)
    q_blocks = qkv_all[0].reshape(BATCH, n_tok // Q_BLOCK, Q_BLOCK, HEADS, HEAD_DIM)
    k_all = qkv_all[1].astype(jnp.float32)
    v_all = qkv_all[2].astype(jnp.float32)

    def one_image(image_args):
        q_img, k_img, v_img = image_args

        def one_block(q_blk):
            logits = jnp.einsum('qhd,khd->hqk', q_blk.astype(jnp.float32), k_img) * HEAD_DIM ** -0.5
            att_weights = jax.nn.softmax(logits, axis=-1)
            return jnp.einsum('hqk,khd->qhd', att_weights, v_img)

        return lax.map(one_block, q_img)

    attn_out = lax.map(one_image, (q_blocks, k_all, v_all)).reshape(BATCH, n_tok, HEADS, HEAD_DIM)
    out_proj = jnp.einsum('bnhd,hcd->bnc', attn_out.astype(jnp.bfloat16).astype(jnp.float32), proj_w[3].astype(jnp.float32))
    return (latent.astype(jnp.float32) + out_proj.reshape(latent.shape)).astype(jnp.bfloat16)


def reference(latent, t_emb, res_norm, res_conv, res_temb, attn_norm, attn_proj):
    hidden = res_block(latent, t_emb, res_norm[0], res_conv[0], res_temb[0])
    hidden = attn_block(hidden, attn_norm, attn_proj)
    return res_block(hidden, t_emb, res_norm[1], res_conv[1], res_temb[1])
```

```python
import functools

import jax
import jax.numpy as jnp
from jax import lax
from jax.experimental import pallas as pl
from jax.experimental.pallas import tpu as pltpu
from jax.sharding import PartitionSpec as P

MESH = pl.DeviceIdType.MESH
GROUPS = 32
EPS = 1e-5
LOG2E = 1.4426950408889634
F32 = jnp.float32
BF16 = jnp.bfloat16
Q_TILE = 256
ROWS_PER_CHUNK = 4


def _peers(n_row, n_col):
    me_r, me_c = lax.axis_index('row'), lax.axis_index('col')
    out = []
    for k in range(1, n_row * n_col):
        r = lax.rem(me_r + k // n_col, n_row)
        c = lax.rem(me_c + k % n_col, n_col)
        out.append((r, c))
    return me_r, me_c, out


def _barrier(peers):
    sem = pltpu.get_barrier_semaphore()
    for r, c in peers:
        pl.semaphore_signal(sem, inc=1, device_id={'row': r, 'col': c}, device_id_type=MESH)
    pl.semaphore_wait(sem, len(peers))


def _gather_kernel(n_row, n_col, x_ref, o_ref, send_sem, recv_sem, loc_sem):
    me_r, me_c, peers = _peers(n_row, n_col)
    n_img, bh, bw = o_ref.shape[0], x_ref.shape[1], x_ref.shape[2]
    place = o_ref.at[:, pl.ds(me_r * bh, bh), pl.ds(pl.multiple_of(me_c * bw, bw), bw), :]
    _barrier(peers)
    copies = []
    for k, (r, c) in enumerate(peers):
        dst = r * n_col + c
        copies.append(pltpu.make_async_remote_copy(
            x_ref.at[pl.ds(dst * n_img, n_img)], place, send_sem.at[k], recv_sem.at[k],
            device_id={'row': r, 'col': c}, device_id_type=MESH))
    for cp in copies:
        cp.start()
    me = me_r * n_col + me_c
    loc = pltpu.make_async_copy(x_ref.at[pl.ds(me * n_img, n_img)], place, loc_sem)
    loc.start()
    for cp in copies:
        cp.wait()
    loc.wait()


def _scatter_kernel(n_row, n_col, y_ref, o_ref, send_sem, recv_sem, loc_sem):
    me_r, me_c, peers = _peers(n_row, n_col)
    n_img, bh, bw = y_ref.shape[0], o_ref.shape[1], o_ref.shape[2]
    me = me_r * n_col + me_c
    place = o_ref.at[pl.ds(me * n_img, n_img)]

    def block(r, c):
        return y_ref.at[:, pl.ds(r * bh, bh), pl.ds(pl.multiple_of(c * bw, bw), bw), :]

    _barrier(peers)
    copies = []
    for k, (r, c) in enumerate(peers):
        copies.append(pltpu.make_async_remote_copy(
            block(r, c), place, send_sem.at[k], recv_sem.at[k],
            device_id={'row': r, 'col': c}, device_id_type=MESH))
    for cp in copies:
        cp.start()
    loc = pltpu.make_async_copy(block(me_r, me_c), place, loc_sem)
    loc.start()
    for cp in copies:
        cp.wait()
    loc.wait()


def _exchange(kernel, arr, out_shape, n_dev, cid):
    return pl.pallas_call(
        kernel,
        out_shape=jax.ShapeDtypeStruct(out_shape, arr.dtype),
        in_specs=[pl.BlockSpec(memory_space=pl.ANY)],
        out_specs=pl.BlockSpec(memory_space=pl.ANY),
        scratch_shapes=[
            pltpu.SemaphoreType.DMA((n_dev - 1,)),
            pltpu.SemaphoreType.DMA((n_dev - 1,)),
            pltpu.SemaphoreType.DMA,
        ],
        compiler_params=pltpu.CompilerParams(collective_id=cid, has_side_effects=True),
    )(arr)


def _dot(a, b, dims=((1,), (0,))):
    return lax.dot_general(a, b, (dims, ((), ())), preferred_element_type=F32)


def _stage_kernel(n_col, hh, ww, x_ref, temb_ref, rnorm_ref, conv_hbm, wtemb_ref, anorm_ref, proj_ref,
                  o_ref, wconv, act, hid, res, temb_s, g_buf, k_buf, q_buf, v_buf, ot_buf, grp_s, sem):
    img = pl.program_id(0)
    n_pos, n_ch = hh * ww, x_ref.shape[-1]
    n_imgs = pl.num_programs(0)
    count = float(n_pos * (n_ch // GROUPS))
    chunk = ROWS_PER_CHUNK * ww
    n_chunks = n_pos // chunk
    me = lax.axis_index('row') * n_col + lax.axis_index('col')

    def weight_copy(i):
        return pltpu.make_async_copy(conv_hbm.at[i // 2, i % 2], wconv.at[i], sem.at[i])

    @pl.when(img == 0)
    def _():
        for i in range(4):
            weight_copy(i).start()
        te = temb_ref[...].astype(F32)
        t_act = (te * jax.nn.sigmoid(te)).astype(BF16)
        for r in range(2):
            temb_s[r] = _dot(t_act, wtemb_ref[r])
        per = n_ch // GROUPS
        gi = lax.broadcasted_iota(jnp.int32, (n_ch, n_ch), 0) // per
        gj = lax.broadcasted_iota(jnp.int32, (n_ch, n_ch), 1) // per
        grp_s[...] = jnp.where(gi == gj, 1.0, 0.0).astype(BF16)
        zeros = jnp.zeros((ww, act.shape[1]), BF16)
        act[0:ww, :] = zeros
        act[(hh + 1) * ww:(hh + 2) * ww, :] = zeros

    def moments(s1, s2):
        st = jnp.concatenate([s1, s2, jnp.zeros((6, n_ch), F32)], axis=0)
        hi = st.astype(BF16)
        r1 = st - hi.astype(F32)
        mid = r1.astype(BF16)
        lo = (r1 - mid.astype(F32)).astype(BF16)
        grp = grp_s[...]
        tot = (_dot(lo, grp) + _dot(mid, grp)) + _dot(hi, grp)
        mean = tot[0:1] / count
        var = tot[1:2] / count - mean * mean
        return mean, lax.rsqrt(var + EPS)

    def chan_sums(v):
        return jnp.sum(v, axis=0, keepdims=True), jnp.sum(v * v, axis=0, keepdims=True)

    zero_sums = (jnp.zeros((1, n_ch), F32), jnp.zeros((1, n_ch), F32))

    def fill_act(src, mean, inv, scale, shift):
        a_mul = inv * scale.astype(F32)
        b_add = shift.astype(F32)
        col = lax.broadcasted_iota(jnp.int32, (ww, 1), 0)

        def row(i, carry):
            r0 = pl.multiple_of(i * ww, ww)
            v = src(r0, ww).astype(F32)
            u = (v - mean) * a_mul + b_add
            a = u * (0.5 * jnp.tanh(0.5 * u) + 0.5)
            left = jnp.where(col == 0, 0.0, pltpu.roll(a, 1, 0))
            right = jnp.where(col == ww - 1, 0.0, pltpu.roll(a, ww - 1, 0))
            d0 = pl.multiple_of(r0 + ww, ww)
            act[pl.ds(d0, ww), 0:n_ch] = left.astype(BF16)
            act[pl.ds(d0, ww), n_ch:2 * n_ch] = a.astype(BF16)
            act[pl.ds(d0, ww), 2 * n_ch:3 * n_ch] = right.astype(BF16)
            return carry

        lax.fori_loop(0, hh, row, 0)

    def conv(w_idx, epilogue):
        @pl.when(img == 0)
        def _():
            weight_copy(w_idx).wait()

        def body(i, sums):
            r0 = pl.multiple_of(i * chunk, chunk)
            lhs = jnp.concatenate([act[pl.ds(pl.multiple_of(r0 + dy * ww, ww), chunk), :] for dy in range(3)], axis=1)
            out = epilogue(r0, _dot(lhs, wconv[w_idx]))
            d1, d2 = chan_sums(out.astype(F32))
            return sums[0] + d1, sums[1] + d2

        return lax.fori_loop(0, n_chunks, body, zero_sums, unroll=2)

    def res_block(r, src, sums, dst):
        mean, inv = moments(*sums)
        fill_act(src, mean, inv, rnorm_ref[r, 0, 0:1], rnorm_ref[r, 0, 1:2])
        t_row = temb_s[r, pl.ds(me * n_imgs + img, 1), :]

        def first(r0, acc):
            out = (acc + t_row).astype(BF16)
            hid[pl.ds(r0, chunk), :] = out
            return out

        sums = conv(2 * r, first)
        mean, inv = moments(*sums)
        fill_act(lambda r0, n: hid[pl.ds(r0, n), :], mean, inv, rnorm_ref[r, 1, 0:1], rnorm_ref[r, 1, 1:2])

        def second(r0, acc):
            out = (src(r0, chunk).astype(F32) + acc).astype(BF16)
            dst(r0, out)
            return out

        return conv(2 * r + 1, second)

    def read_x(r0, n):
        return x_ref[0, pl.ds(r0, n), :]

    def read_res(r0, n):
        return res[pl.ds(r0, n), :]

    def write_res(r0, v):
        res[pl.ds(r0, chunk), :] = v

    def write_out(r0, v):
        o_ref[0, pl.ds(r0, chunk), :] = v

    def x_sums(i, sums):
        d1, d2 = chan_sums(read_x(pl.multiple_of(i * chunk, chunk), chunk).astype(F32))
        return sums[0] + d1, sums[1] + d2

    sums = lax.fori_loop(0, n_chunks, x_sums, zero_sums)
    sums = res_block(0, read_x, sums, write_res)

    mean, inv = moments(*sums)
    a_mul = inv * anorm_ref[0:1].astype(F32)
    b_add = anorm_ref[1:2].astype(F32)

    def project(i, carry):
        r0 = pl.multiple_of(i * Q_TILE, Q_TILE)
        g = ((read_res(r0, Q_TILE).astype(F32) - mean) * a_mul + b_add).astype(BF16)
        q_buf[:, pl.ds(r0, Q_TILE)] = _dot(proj_ref[0], g, ((1,), (1,))).astype(BF16)
        v_buf[:, pl.ds(r0, Q_TILE)] = _dot(proj_ref[2], g, ((1,), (1,))).astype(BF16)
        k_buf[pl.ds(r0, Q_TILE), :] = _dot(g, proj_ref[1], ((1,), (1,))).astype(BF16)
        return carry

    lax.fori_loop(0, n_pos // Q_TILE, project, 0)

    head_dim = 32
    n_heads = n_ch // head_dim
    per_blk = 128 // head_dim
    n_tiles = n_pos // Q_TILE
    scale = LOG2E * head_dim ** -0.5
    row_head = lax.broadcasted_iota(jnp.int32, (128, Q_TILE), 0) // head_dim

    def attend(i, carry):
        h = i // n_tiles
        q0 = pl.multiple_of((i % n_tiles) * Q_TILE, Q_TILE)
        b0 = pl.multiple_of((h // per_blk) * 128, 128)
        h0 = pl.multiple_of(h * head_dim, head_dim)
        qm = jnp.where(row_head == h % per_blk, q_buf[pl.ds(b0, 128), pl.ds(q0, Q_TILE)], 0)
        s = _dot(k_buf[:, pl.ds(b0, 128)], qm)
        m = jnp.max(s, axis=0, keepdims=True)
        p = jnp.exp2((s - m) * scale)
        l = jnp.sum(p, axis=0, keepdims=True)
        o = _dot(v_buf[pl.ds(h0, head_dim), :], p.astype(BF16))
        ot_buf[pl.ds(h0, head_dim), pl.ds(q0, Q_TILE)] = (o / l).astype(BF16)
        return carry

    lax.fori_loop(0, n_heads * n_tiles, attend, 0)

    def out_proj(i, sums):
        r0 = pl.multiple_of(i * chunk, chunk)
        acc = _dot(ot_buf[:, pl.ds(r0, chunk)], proj_ref[3], ((0,), (0,)))
        out = (read_res(r0, chunk).astype(F32) + acc).astype(BF16)
        write_res(r0, out)
        d1, d2 = chan_sums(out.astype(F32))
        return sums[0] + d1, sums[1] + d2

    sums = lax.fori_loop(0, n_chunks, out_proj, zero_sums)
    res_block(1, read_res, sums, write_out)


def _stage(images, hh, ww, n_col, t_emb, res_norm, res_conv, res_temb, attn_norm, attn_proj):
    n_img, n_pos, n_ch = images.shape
    proj = jnp.transpose(attn_proj, (0, 1, 3, 2)).reshape(4, n_ch, n_ch)
    conv_w = res_conv.reshape(2, 2, 9 * n_ch, n_ch)

    def whole(a):
        return pl.BlockSpec(a.shape, lambda i, nd=a.ndim: (0,) * nd, pipeline_mode=pl.Buffered(1))

    img_spec = pl.BlockSpec((1, n_pos, n_ch), lambda i: (i, 0, 0))
    return pl.pallas_call(
        functools.partial(_stage_kernel, n_col, hh, ww),
        grid=(n_img,),
        out_shape=jax.ShapeDtypeStruct(images.shape, BF16),
        in_specs=[img_spec, whole(t_emb), whole(res_norm), pl.BlockSpec(memory_space=pl.ANY), whole(res_temb),
                  whole(attn_norm), whole(proj)],
        out_specs=img_spec,
        scratch_shapes=[
            pltpu.VMEM((4, 9 * n_ch, n_ch), BF16),
            pltpu.VMEM(((hh + 2) * ww, 3 * n_ch), BF16),
            pltpu.VMEM((n_pos, n_ch), BF16),
            pltpu.VMEM((n_pos, n_ch), BF16),
            pltpu.VMEM((2, t_emb.shape[0], n_ch), F32),
            pltpu.VMEM((8, n_ch), BF16),
            pltpu.VMEM((n_pos, n_ch), BF16),
            pltpu.VMEM((n_ch, n_pos), BF16),
            pltpu.VMEM((n_ch, n_pos), BF16),
            pltpu.VMEM((n_ch, n_pos), BF16),
            pltpu.VMEM((n_ch, n_ch), BF16),
            pltpu.SemaphoreType.DMA((4,)),
        ],
        compiler_params=pltpu.CompilerParams(dimension_semantics=("arbitrary",), vmem_limit_bytes=60 * 1024 * 1024),
    )(images, t_emb, res_norm, conv_w, res_temb, attn_norm, proj)


def solution(mesh):
    n_row, n_col = mesh.shape['row'], mesh.shape['col']
    n_dev = n_row * n_col

    def run_stage(latent, t_emb, res_norm, res_conv, res_temb, attn_norm, attn_proj):
        n_batch, bh, bw, n_ch = latent.shape
        hh, ww = bh * n_row, bw * n_col
        n_img = n_batch // n_dev
        images = _exchange(functools.partial(_gather_kernel, n_row, n_col), latent, (n_img, hh, ww, n_ch), n_dev, 0)
        out = _stage(images.reshape(n_img, hh * ww, n_ch), hh, ww, n_col, t_emb, res_norm, res_conv, res_temb,
                     attn_norm, attn_proj)
        return _exchange(functools.partial(_scatter_kernel, n_row, n_col), out.reshape(n_img, hh, ww, n_ch),
                         latent.shape, n_dev, 1)

    spec_x = P('dp', 'row', 'col', None)
    return jax.shard_map(run_stage, mesh=mesh, in_specs=(spec_x, P('dp', None), P(), P(), P(), P(), P()), out_specs=spec_x, check_vma=False)
```

```python
import functools

import jax
import jax.numpy as jnp
from jax import lax
from jax.experimental import pallas as pl
from jax.experimental.pallas import tpu as pltpu
from jax.sharding import PartitionSpec as P

MESH = pl.DeviceIdType.MESH
GROUPS = 32
EPS = 1e-5
LOG2E = 1.4426950408889634
F32 = jnp.float32
BF16 = jnp.bfloat16
Q_TILE = 512
K_CHUNK = 256
AHEAD = 2
ROWS_PER_CHUNK = 4


def _me_and_peers(n_row, n_col):
    me_r, me_c = lax.axis_index('row'), lax.axis_index('col')
    peers = []
    for k in range(1, n_row * n_col):
        peers.append((lax.rem(me_r + k // n_col, n_row), lax.rem(me_c + k % n_col, n_col)))
    return me_r, me_c, peers


def _barrier(peers):
    sem = pltpu.get_barrier_semaphore()
    for r, c in peers:
        pl.semaphore_signal(sem, inc=1, device_id={'row': r, 'col': c}, device_id_type=MESH)
    pl.semaphore_wait(sem, len(peers))


def _dot(a, b, dims=((1,), (0,))):
    return lax.dot_general(a, b, (dims, ((), ())), preferred_element_type=F32)


def _chan_sums(v):
    return jnp.sum(v, axis=0, keepdims=True), jnp.sum(v * v, axis=0, keepdims=True)


def _group_matrix(n_ch):
    per = n_ch // GROUPS
    gi = lax.broadcasted_iota(jnp.int32, (n_ch, n_ch), 0) // per
    gj = lax.broadcasted_iota(jnp.int32, (n_ch, n_ch), 1) // per
    return jnp.where(gi == gj, 1.0, 0.0).astype(BF16)


def _moments(s1, s2, grp, count):
    n_ch = s1.shape[1]
    st = jnp.concatenate([s1, s2, jnp.zeros((6, n_ch), F32)], axis=0)
    hi = st.astype(BF16)
    r1 = st - hi.astype(F32)
    mid = r1.astype(BF16)
    lo = (r1 - mid.astype(F32)).astype(BF16)
    tot = (_dot(lo, grp) + _dot(mid, grp)) + _dot(hi, grp)
    mean = tot[0:1] / count
    var = tot[1:2] / count - mean * mean
    return mean, lax.rsqrt(var + EPS)


def _zero_sums(n_ch):
    return jnp.zeros((1, n_ch), F32), jnp.zeros((1, n_ch), F32)


class _ResBlock:
    def __init__(self, hh, ww, n_ch, rnorm_ref, wconv, act, hid, temb_s, grp_s):
        self.hh, self.ww, self.n_ch = hh, ww, n_ch
        self.rnorm_ref, self.wconv, self.act, self.hid = rnorm_ref, wconv, act, hid
        self.temb_s, self.grp_s = temb_s, grp_s
        self.chunk = ROWS_PER_CHUNK * ww
        self.n_chunks = hh // ROWS_PER_CHUNK
        self.count = float(hh * ww * (n_ch // GROUPS))

    def setup(self, temb_ref, wtemb_ref):
        te = temb_ref[...].astype(F32)
        t_act = (te * jax.nn.sigmoid(te)).astype(BF16)
        self.temb_s[...] = _dot(t_act, wtemb_ref[...])
        self.grp_s[...] = _group_matrix(self.n_ch)
        zeros = jnp.zeros((self.ww, self.act.shape[1]), BF16)
        self.act[0:self.ww, :] = zeros
        self.act[(self.hh + 1) * self.ww:(self.hh + 2) * self.ww, :] = zeros

    def fill(self, src, sums, scale, shift):
        ww, n_ch, act = self.ww, self.n_ch, self.act
        mean, inv = _moments(*sums, self.grp_s[...], self.count)
        a_mul = inv * scale.astype(F32)
        b_add = shift.astype(F32)
        col = lax.broadcasted_iota(jnp.int32, (ww, 1), 0)

        def row(i, carry):
            r0 = pl.multiple_of(i * ww, ww)
            v = src(r0, ww).astype(F32)
            u = (v - mean) * a_mul + b_add
            a = u * (0.5 * jnp.tanh(0.5 * u) + 0.5)
            left = jnp.where(col == 0, 0.0, pltpu.roll(a, 1, 0))
            right = jnp.where(col == ww - 1, 0.0, pltpu.roll(a, ww - 1, 0))
            d0 = pl.multiple_of(r0 + ww, ww)
            act[pl.ds(d0, ww), 0:n_ch] = left.astype(BF16)
            act[pl.ds(d0, ww), n_ch:2 * n_ch] = a.astype(BF16)
            act[pl.ds(d0, ww), 2 * n_ch:3 * n_ch] = right.astype(BF16)
            return carry

        lax.fori_loop(0, self.hh, row, 0)

    def conv(self, j, first_chunk, epilogue):
        chunk, ww = self.chunk, self.ww

        def body(i, sums):
            k = lax.rem(i + first_chunk, self.n_chunks)
            r0 = pl.multiple_of(k * chunk, chunk)
            lhs = jnp.concatenate(
                [self.act[pl.ds(pl.multiple_of(r0 + dy * ww, ww), chunk), :] for dy in range(3)], axis=1)
            out = epilogue(k, r0, _dot(lhs, self.wconv[j]))
            d1, d2 = _chan_sums(out.astype(F32))
            return sums[0] + d1, sums[1] + d2

        return lax.fori_loop(0, self.n_chunks, body, _zero_sums(self.n_ch))

    def input_sums(self, src):
        def body(i, sums):
            d1, d2 = _chan_sums(src(pl.multiple_of(i * self.chunk, self.chunk), self.chunk).astype(F32))
            return sums[0] + d1, sums[1] + d2

        return lax.fori_loop(0, self.n_chunks, body, _zero_sums(self.n_ch))

    def run(self, src, img, wait_weight, first_chunk, dst):
        chunk, hid, rnorm_ref = self.chunk, self.hid, self.rnorm_ref
        self.fill(src, self.input_sums(src), rnorm_ref[0, 0:1], rnorm_ref[0, 1:2])
        t_row = self.temb_s[pl.ds(img, 1), :]

        def first(k, r0, acc):
            out = (acc + t_row).astype(BF16)
            hid[pl.ds(r0, chunk), :] = out
            return out

        wait_weight(0)
        sums = self.conv(0, 0, first)
        self.fill(lambda r0, n: hid[pl.ds(r0, n), :], sums, rnorm_ref[1, 0:1], rnorm_ref[1, 1:2])

        def second(k, r0, acc):
            out = (src(r0, chunk).astype(F32) + acc).astype(BF16)
            dst(k, r0, out)
            return out

        wait_weight(1)
        self.conv(1, first_chunk, second)


def _weight_copies(r, conv_hbm, wconv, wtemb_hbm, wtemb, sem):
    convs = [pltpu.make_async_copy(conv_hbm.at[r, i], wconv.at[i], sem.at[i]) for i in range(2)]
    return convs, pltpu.make_async_copy(wtemb_hbm.at[r], wtemb, sem.at[2])


def _first_kernel(n_row, n_col, lat_ref, temb_ref, rnorm_ref, conv_hbm, wtemb_hbm, o_ref,
                  xv, wconv, wtemb, act, hid, temb_s, grp_s, wsem, send_sem, recv_sem, loc_sem):
    me_r, me_c, peers = _me_and_peers(n_row, n_col)
    me = me_r * n_col + me_c
    n_img, hh, ww, n_ch = xv.shape
    bh, bw = hh // n_row, ww // n_col
    weights, temb_copy = _weight_copies(0, conv_hbm, wconv, wtemb_hbm, wtemb, wsem)
    for w in [temb_copy, *weights]:
        w.start()

    def place(s):
        return xv.at[s, pl.ds(me_r * bh, bh), pl.ds(pl.multiple_of(me_c * bw, bw), bw), :]

    def copy(s, k):
        r, c = peers[k]
        return pltpu.make_async_remote_copy(
            lat_ref.at[(r * n_col + c) * n_img + s], place(s), send_sem.at[s, k], recv_sem.at[s, k],
            device_id={'row': r, 'col': c}, device_id_type=MESH)

    def own(s):
        return pltpu.make_async_copy(lat_ref.at[me * n_img + s], place(s), loc_sem.at[s])

    _barrier(peers)
    for s in range(n_img):
        for k in range(len(peers)):
            copy(s, k).start()
        own(s).start()

    blk = _ResBlock(hh, ww, n_ch, rnorm_ref.at[0], wconv, act, hid, temb_s, grp_s)
    temb_copy.wait()
    blk.setup(temb_ref, wtemb)

    def image(s, carry):
        for k in range(len(peers)):
            copy(s, k).wait_recv()
        own(s).wait()

        def src(r0, n):
            return xv[s, pl.ds(r0 // ww, n // ww)].reshape(n, n_ch)

        def dst(k, r0, v):
            o_ref[s, pl.ds(r0, blk.chunk), :] = v

        def wait_weight(j):
            @pl.when(s == 0)
            def _():
                weights[j].wait()

        blk.run(src, me * n_img + s, wait_weight, 0, dst)
        return carry

    lax.fori_loop(0, n_img, image, 0)
    for s in range(n_img):
        for k in range(len(peers)):
            copy(s, k).wait_send()


def _last_kernel(n_row, n_col, x_ref, temb_ref, rnorm_ref, conv_hbm, wtemb_hbm, o_ref,
                 yv, wconv, wtemb, act, hid, temb_s, grp_s, wsem, send_sem, recv_sem, loc_sem):
    me_r, me_c, peers = _me_and_peers(n_row, n_col)
    me = me_r * n_col + me_c
    n_img, hh, ww, n_ch = yv.shape
    bh, bw = hh // n_row, ww // n_col
    weights, temb_copy = _weight_copies(1, conv_hbm, wconv, wtemb_hbm, wtemb, wsem)
    for w in [temb_copy, *weights]:
        w.start()
    blk = _ResBlock(hh, ww, n_ch, rnorm_ref.at[1], wconv, act, hid, temb_s, grp_s)
    temb_copy.wait()
    blk.setup(temb_ref, wtemb)
    _barrier(peers)
    first_chunk = lax.rem(me_r + n_row // 2, n_row) // (n_row // 2) * (n_row // 2)

    def block(s, k, c):
        return yv.at[s, pl.ds(k * bh, bh), pl.ds(pl.multiple_of(c * bw, bw), bw), :]

    def rel(k, c):
        return lax.rem(k - me_r + n_row, n_row) * n_col + lax.rem(c - me_c + n_col, n_col)

    def copy(s, k, c):
        return pltpu.make_async_remote_copy(
            block(s, k, c), o_ref.at[me * n_img + s], send_sem.at[s, rel(k, c)], recv_sem.at[s, rel(k, c)],
            device_id={'row': k, 'col': c}, device_id_type=MESH)

    def own(s):
        return pltpu.make_async_copy(block(s, me_r, me_c), o_ref.at[me * n_img + s], loc_sem.at[s])

    def image(s, carry):
        def src(r0, n):
            return x_ref[s, pl.ds(r0, n), :]

        def dst(k, r0, v):
            yv[s, pl.ds(r0 // ww, ROWS_PER_CHUNK)] = v.reshape(ROWS_PER_CHUNK, ww, n_ch)
            for d in range(n_col):
                c = lax.rem(me_c + 1 + d, n_col)
                remote = (k != me_r) | (c != me_c)

                @pl.when(remote)
                def _():
                    copy(s, k, c).start()

                @pl.when(jnp.logical_not(remote))
                def _():
                    own(s).start()

        def wait_weight(j):
            @pl.when(s == 0)
            def _():
                weights[j].wait()

        blk.run(src, me * n_img + s, wait_weight, first_chunk, dst)
        return carry

    lax.fori_loop(0, n_img, image, 0)
    for s in range(n_img):
        for r, c in peers:
            copy(s, r, c).wait()
        own(s).wait()


def _attn_kernel(x_ref, anorm_ref, proj_ref, o_ref, grp_s, k_buf, q_buf, v_buf, ot_buf):
    n_pos, n_ch = x_ref.shape[1:]
    count = float(n_pos * (n_ch // GROUPS))
    head_dim = 32
    n_heads = n_ch // head_dim
    per_blk = 128 // head_dim
    scale = LOG2E * head_dim ** -0.5

    @pl.when(pl.program_id(0) == 0)
    def _():
        grp_s[...] = _group_matrix(n_ch)

    def in_sums(i, sums):
        d1, d2 = _chan_sums(x_ref[0, pl.ds(pl.multiple_of(i * 256, 256), 256), :].astype(F32))
        return sums[0] + d1, sums[1] + d2

    sums = lax.fori_loop(0, n_pos // 256, in_sums, _zero_sums(n_ch))
    mean, inv = _moments(*sums, grp_s[...], count)
    a_mul = inv * anorm_ref[0:1].astype(F32)
    b_add = anorm_ref[1:2].astype(F32)
    head_rows = jnp.where(lax.broadcasted_iota(jnp.int32, (16, n_ch), 0)
                          == lax.broadcasted_iota(jnp.int32, (16, n_ch), 1) // head_dim, 1.0, 0.0).astype(BF16)

    def project(i, tops):
        r0 = pl.multiple_of(i * 256, 256)
        g = ((x_ref[0, pl.ds(r0, 256), :].astype(F32) - mean) * a_mul + b_add).astype(BF16)
        q = _dot(proj_ref[0], g, ((1,), (1,))).astype(BF16)
        v = _dot(proj_ref[2], g, ((1,), (1,))).astype(BF16)
        k = _dot(g, proj_ref[1], ((1,), (1,))).astype(BF16)
        q_buf[:, pl.ds(r0, 256)] = q
        v_buf[:, pl.ds(r0, 256)] = v
        k_buf[pl.ds(r0, 256), :] = k
        q2 = _dot(head_rows, (q.astype(F32) * q.astype(F32)).astype(BF16))
        k2 = _dot(head_rows, (k.astype(F32) * k.astype(F32)).astype(BF16), ((1,), (1,)))
        v_top = jnp.max(jnp.abs(v.astype(F32)), axis=0, keepdims=True)
        return jnp.maximum(tops[0], q2), jnp.maximum(tops[1], k2), jnp.maximum(tops[2], v_top)

    tops = lax.fori_loop(0, n_pos // 256, project,
                         (jnp.zeros((16, 256), F32), jnp.zeros((16, 256), F32), jnp.zeros((1, 256), F32)))
    small = (jnp.max(tops[0]) * scale * scale * jnp.max(tops[1]) < 1600.0) & (jnp.max(tops[2]) < 2.0 ** 60)

    @pl.when(small)
    def _():
        rh = lax.broadcasted_iota(jnp.int32, (128, Q_TILE), 0) // head_dim
        n_kc = n_pos // K_CHUNK

        def heads(b, carry):
            b0 = pl.multiple_of(b * 128, 128)
            tiles = [(j, t * Q_TILE) for j in range(per_blk) for t in range(n_pos // Q_TILE)]
            steps = [(tile, c) for tile in tiles for c in range(n_kc)]
            masked = {}

            def score(step):
                tile, c = step
                if tile not in masked:
                    j, q0 = tile
                    masked[tile] = jnp.where(rh == j, q_buf[pl.ds(b0, 128), q0:q0 + Q_TILE], 0)
                return _dot(k_buf[c * K_CHUNK:(c + 1) * K_CHUNK, pl.ds(b0, 128)], masked[tile])

            pending = [score(s) for s in steps[:AHEAD]]
            tot = out = None
            for n, ((j, q0), c) in enumerate(steps):
                if n + AHEAD < len(steps):
                    pending.append(score(steps[n + AHEAD]))
                p = jnp.exp2(pending.pop(0) * scale)
                h0 = pl.multiple_of(b0 + j * head_dim, head_dim)
                part = jnp.sum(p.reshape(K_CHUNK // 8, 8, Q_TILE), axis=0)
                pv = _dot(v_buf[pl.ds(h0, head_dim), c * K_CHUNK:(c + 1) * K_CHUNK], p.astype(BF16))
                tot, out = (part, pv) if c == 0 else (tot + part, out + pv)
                if c == n_kc - 1:
                    res = out / jnp.sum(tot, axis=0, keepdims=True)
                    ot_buf[pl.ds(h0, head_dim), q0:q0 + Q_TILE] = res.astype(BF16)
            return carry

        lax.fori_loop(0, n_ch // 128, heads, 0)

    @pl.when(jnp.logical_not(small))
    def _():
        rh = lax.broadcasted_iota(jnp.int32, (128, 256), 0) // head_dim
        n_tiles = n_pos // 256

        def tile(i, carry):
            h = i // n_tiles
            q0 = pl.multiple_of((i % n_tiles) * 256, 256)
            b0 = pl.multiple_of((h // per_blk) * 128, 128)
            h0 = pl.multiple_of(h * head_dim, head_dim)
            qm = jnp.where(rh == h % per_blk, q_buf[pl.ds(b0, 128), pl.ds(q0, 256)], 0)
            s = _dot(k_buf[:, pl.ds(b0, 128)], qm)
            p = jnp.exp2((s - jnp.max(s, axis=0, keepdims=True)) * scale)
            o = _dot(v_buf[pl.ds(h0, head_dim), :], p.astype(BF16))
            ot_buf[pl.ds(h0, head_dim), pl.ds(q0, 256)] = (o / jnp.sum(p, axis=0, keepdims=True)).astype(BF16)
            return carry

        lax.fori_loop(0, n_heads * n_tiles, tile, 0)

    def out_proj(i, carry):
        r0 = pl.multiple_of(i * 256, 256)
        acc = _dot(ot_buf[:, pl.ds(r0, 256)], proj_ref[3], ((0,), (0,)))
        o_ref[0, pl.ds(r0, 256), :] = (x_ref[0, pl.ds(r0, 256), :].astype(F32) + acc).astype(BF16)
        return carry

    lax.fori_loop(0, n_pos // 256, out_proj, 0)


VMEM_LIMIT = 60 * 1024 * 1024


def _res_scratch(hh, ww, n_ch, n_batch, n_temb, n_img, n_dev):
    return [
        pltpu.VMEM((n_img, hh, ww, n_ch), BF16),
        pltpu.VMEM((2, 9 * n_ch, n_ch), BF16),
        pltpu.VMEM((n_temb, n_ch), BF16),
        pltpu.VMEM(((hh + 2) * ww, 3 * n_ch), BF16),
        pltpu.VMEM((hh * ww, n_ch), BF16),
        pltpu.VMEM((n_batch, n_ch), F32),
        pltpu.VMEM((n_ch, n_ch), BF16),
        pltpu.SemaphoreType.DMA((3,)),
        pltpu.SemaphoreType.DMA((n_img, n_dev)),
        pltpu.SemaphoreType.DMA((n_img, n_dev)),
        pltpu.SemaphoreType.DMA((n_img,)),
    ]


def solution(mesh):
    n_row, n_col = mesh.shape['row'], mesh.shape['col']
    n_dev = n_row * n_col
    vmem, hbm = pl.BlockSpec(memory_space=pltpu.VMEM), pl.BlockSpec(memory_space=pl.ANY)

    def run_stage(latent, t_emb, res_norm, res_conv, res_temb, attn_norm, attn_proj):
        n_batch, bh, bw, n_ch = latent.shape
        hh, ww = bh * n_row, bw * n_col
        n_pos, n_img = hh * ww, n_batch // n_dev
        proj = jnp.transpose(attn_proj, (0, 1, 3, 2)).reshape(4, n_ch, n_ch)
        conv_w = res_conv.reshape(2, 2, 9 * n_ch, n_ch)
        scratch = _res_scratch(hh, ww, n_ch, n_batch, t_emb.shape[1], n_img, n_dev)

        x1 = pl.pallas_call(
            functools.partial(_first_kernel, n_row, n_col),
            out_shape=jax.ShapeDtypeStruct((n_img, n_pos, n_ch), BF16),
            in_specs=[hbm, vmem, vmem, hbm, hbm],
            out_specs=vmem,
            scratch_shapes=scratch,
            compiler_params=pltpu.CompilerParams(collective_id=0, has_side_effects=True, vmem_limit_bytes=VMEM_LIMIT),
        )(latent, t_emb, res_norm, conv_w, res_temb)

        def whole(a):
            return pl.BlockSpec(a.shape, lambda i, nd=a.ndim: (0,) * nd, pipeline_mode=pl.Buffered(1))

        img_spec = pl.BlockSpec((1, n_pos, n_ch), lambda i: (i, 0, 0))
        x2 = pl.pallas_call(
            _attn_kernel,
            grid=(n_img,),
            out_shape=jax.ShapeDtypeStruct((n_img, n_pos, n_ch), BF16),
            in_specs=[img_spec, whole(attn_norm), whole(proj)],
            out_specs=img_spec,
            scratch_shapes=[
                pltpu.VMEM((n_ch, n_ch), BF16),
                pltpu.VMEM((n_pos, n_ch), BF16),
                pltpu.VMEM((n_ch, n_pos), BF16),
                pltpu.VMEM((n_ch, n_pos), BF16),
                pltpu.VMEM((n_ch, n_pos), BF16),
            ],
            compiler_params=pltpu.CompilerParams(dimension_semantics=("arbitrary",), vmem_limit_bytes=VMEM_LIMIT),
        )(x1, attn_norm, proj)

        return pl.pallas_call(
            functools.partial(_last_kernel, n_row, n_col),
            out_shape=jax.ShapeDtypeStruct(latent.shape, BF16),
            in_specs=[vmem, vmem, vmem, hbm, hbm],
            out_specs=hbm,
            scratch_shapes=scratch,
            compiler_params=pltpu.CompilerParams(collective_id=1, has_side_effects=True, vmem_limit_bytes=VMEM_LIMIT),
        )(x2, t_emb, res_norm, conv_w, res_temb)

    spec_x = P('dp', 'row', 'col', None)
    return jax.shard_map(run_stage, mesh=mesh, in_specs=(spec_x, P('dp', None), P(), P(), P(), P(), P()), out_specs=spec_x, check_vma=False)
```

```python
import functools

import jax
import jax.numpy as jnp
from jax import lax
from jax.experimental import pallas as pl
from jax.experimental.pallas import tpu as pltpu
from jax.sharding import PartitionSpec as P

MESH = pl.DeviceIdType.MESH
GROUPS = 32
EPS = 1e-5
LOG2E = 1.4426950408889634
F32 = jnp.float32
BF16 = jnp.bfloat16
Q_TILE = 512
K_CHUNK = 256
AHEAD = 2
ROWS_PER_CHUNK = 4


def _me_and_peers(n_row, n_col):
    me_r, me_c = lax.axis_index('row'), lax.axis_index('col')
    peers = []
    for k in range(1, n_row * n_col):
        peers.append((lax.rem(me_r + k // n_col, n_row), lax.rem(me_c + k % n_col, n_col)))
    return me_r, me_c, peers


def _barrier(peers):
    sem = pltpu.get_barrier_semaphore()
    for r, c in peers:
        pl.semaphore_signal(sem, inc=1, device_id={'row': r, 'col': c}, device_id_type=MESH)
    pl.semaphore_wait(sem, len(peers))


def _dot(a, b, dims=((1,), (0,))):
    return lax.dot_general(a, b, (dims, ((), ())), preferred_element_type=F32)


def _chan_sums(v):
    return jnp.sum(v, axis=0, keepdims=True), jnp.sum(v * v, axis=0, keepdims=True)


def _group_matrix(n_ch):
    per = n_ch // GROUPS
    gi = lax.broadcasted_iota(jnp.int32, (n_ch, n_ch), 0) // per
    gj = lax.broadcasted_iota(jnp.int32, (n_ch, n_ch), 1) // per
    return jnp.where(gi == gj, 1.0, 0.0).astype(BF16)


def _moments(s1, s2, grp, count):
    n_ch = s1.shape[1]
    st = jnp.concatenate([s1, s2, jnp.zeros((6, n_ch), F32)], axis=0)
    hi = st.astype(BF16)
    r1 = st - hi.astype(F32)
    mid = r1.astype(BF16)
    lo = (r1 - mid.astype(F32)).astype(BF16)
    tot = (_dot(lo, grp) + _dot(mid, grp)) + _dot(hi, grp)
    mean = tot[0:1] / count
    var = tot[1:2] / count - mean * mean
    return mean, lax.rsqrt(var + EPS)


def _zero_sums(n_ch):
    return jnp.zeros((1, n_ch), F32), jnp.zeros((1, n_ch), F32)


class _ResBlock:
    def __init__(self, hh, ww, n_ch, rnorm_ref, wconv, act, hid, temb_s, grp_s):
        self.hh, self.ww, self.n_ch = hh, ww, n_ch
        self.rnorm_ref, self.wconv, self.act, self.hid = rnorm_ref, wconv, act, hid
        self.temb_s, self.grp_s = temb_s, grp_s
        self.chunk = ROWS_PER_CHUNK * ww
        self.n_chunks = hh // ROWS_PER_CHUNK
        self.count = float(hh * ww * (n_ch // GROUPS))

    def setup(self, temb_ref, wtemb_ref):
        te = temb_ref[...].astype(F32)
        t_act = (te * jax.nn.sigmoid(te)).astype(BF16)
        self.temb_s[...] = _dot(t_act, wtemb_ref[...])
        self.grp_s[...] = _group_matrix(self.n_ch)
        zeros = jnp.zeros((self.ww, self.act.shape[1]), BF16)
        self.act[0:self.ww, :] = zeros
        self.act[(self.hh + 1) * self.ww:(self.hh + 2) * self.ww, :] = zeros

    def fill(self, src, sums, scale, shift):
        ww, n_ch, act = self.ww, self.n_ch, self.act
        mean, inv = _moments(*sums, self.grp_s[...], self.count)
        a_mul = inv * scale.astype(F32)
        b_add = shift.astype(F32)
        col = lax.broadcasted_iota(jnp.int32, (ww, 1), 0)

        def row(i, carry):
            r0 = pl.multiple_of(i * ww, ww)
            v = src(r0, ww).astype(F32)
            u = (v - mean) * a_mul + b_add
            a = u * (0.5 * jnp.tanh(0.5 * u) + 0.5)
            left = jnp.where(col == 0, 0.0, pltpu.roll(a, 1, 0))
            right = jnp.where(col == ww - 1, 0.0, pltpu.roll(a, ww - 1, 0))
            d0 = pl.multiple_of(r0 + ww, ww)
            act[pl.ds(d0, ww), 0:n_ch] = left.astype(BF16)
            act[pl.ds(d0, ww), n_ch:2 * n_ch] = a.astype(BF16)
            act[pl.ds(d0, ww), 2 * n_ch:3 * n_ch] = right.astype(BF16)
            return carry

        lax.fori_loop(0, self.hh, row, 0)

    def conv(self, j, first_chunk, epilogue):
        chunk, ww = self.chunk, self.ww

        def body(i, sums):
            k = lax.rem(i + first_chunk, self.n_chunks)
            r0 = pl.multiple_of(k * chunk, chunk)
            lhs = jnp.concatenate(
                [self.act[pl.ds(pl.multiple_of(r0 + dy * ww, ww), chunk), :] for dy in range(3)], axis=1)
            out = epilogue(k, r0, _dot(lhs, self.wconv[j]))
            d1, d2 = _chan_sums(out.astype(F32))
            return sums[0] + d1, sums[1] + d2

        return lax.fori_loop(0, self.n_chunks, body, _zero_sums(self.n_ch))

    def input_sums(self, src):
        def body(i, sums):
            d1, d2 = _chan_sums(src(pl.multiple_of(i * self.chunk, self.chunk), self.chunk).astype(F32))
            return sums[0] + d1, sums[1] + d2

        return lax.fori_loop(0, self.n_chunks, body, _zero_sums(self.n_ch))

    def run(self, src, img, wait_weight, first_chunk, dst):
        chunk, hid, rnorm_ref = self.chunk, self.hid, self.rnorm_ref
        self.fill(src, self.input_sums(src), rnorm_ref[0, 0:1], rnorm_ref[0, 1:2])
        t_row = self.temb_s[pl.ds(img, 1), :]

        def first(k, r0, acc):
            out = (acc + t_row).astype(BF16)
            hid[pl.ds(r0, chunk), :] = out
            return out

        wait_weight(0)
        sums = self.conv(0, 0, first)
        self.fill(lambda r0, n: hid[pl.ds(r0, n), :], sums, rnorm_ref[1, 0:1], rnorm_ref[1, 1:2])

        def second(k, r0, acc):
            out = (src(r0, chunk).astype(F32) + acc).astype(BF16)
            dst(k, r0, out)
            return out

        wait_weight(1)
        self.conv(1, first_chunk, second)


def _weight_copies(r, conv_hbm, wconv, wtemb_hbm, wtemb, sem):
    convs = [pltpu.make_async_copy(conv_hbm.at[r, i], wconv.at[i], sem.at[i]) for i in range(2)]
    return convs, pltpu.make_async_copy(wtemb_hbm.at[r], wtemb, sem.at[2])


def _first_kernel(n_row, n_col, lat_ref, temb_ref, rnorm_ref, conv_hbm, wtemb_hbm, o_ref,
                  xv, wconv, wtemb, act, hid, temb_s, grp_s, wsem, send_sem, recv_sem, loc_sem):
    me_r, me_c, peers = _me_and_peers(n_row, n_col)
    me = me_r * n_col + me_c
    n_img, hh, ww, n_ch = xv.shape
    bh, bw = hh // n_row, ww // n_col
    weights, temb_copy = _weight_copies(0, conv_hbm, wconv, wtemb_hbm, wtemb, wsem)
    for w in [temb_copy, *weights]:
        w.start()

    def place(s):
        return xv.at[s, pl.ds(me_r * bh, bh), pl.ds(pl.multiple_of(me_c * bw, bw), bw), :]

    def copy(s, k):
        r, c = peers[k]
        return pltpu.make_async_remote_copy(
            lat_ref.at[(r * n_col + c) * n_img + s], place(s), send_sem.at[s, k], recv_sem.at[s, k],
            device_id={'row': r, 'col': c}, device_id_type=MESH)

    def own(s):
        return pltpu.make_async_copy(lat_ref.at[me * n_img + s], place(s), loc_sem.at[s])

    _barrier(peers)
    for s in range(n_img):
        for k in range(len(peers)):
            copy(s, k).start()
        own(s).start()

    blk = _ResBlock(hh, ww, n_ch, rnorm_ref.at[0], wconv, act, hid, temb_s, grp_s)
    temb_copy.wait()
    blk.setup(temb_ref, wtemb)

    def image(s, carry):
        for k in range(len(peers)):
            copy(s, k).wait_recv()
        own(s).wait()

        def src(r0, n):
            return xv[s, pl.ds(r0 // ww, n // ww)].reshape(n, n_ch)

        def dst(k, r0, v):
            o_ref[s, pl.ds(r0, blk.chunk), :] = v

        def wait_weight(j):
            @pl.when(s == 0)
            def _():
                weights[j].wait()

        blk.run(src, me * n_img + s, wait_weight, 0, dst)
        return carry

    lax.fori_loop(0, n_img, image, 0)
    for s in range(n_img):
        for k in range(len(peers)):
            copy(s, k).wait_send()


def _last_kernel(n_row, n_col, x_ref, temb_ref, rnorm_ref, conv_hbm, wtemb_hbm, o_ref,
                 yv, wconv, wtemb, act, hid, temb_s, grp_s, wsem, send_sem, recv_sem, loc_sem):
    me_r, me_c, peers = _me_and_peers(n_row, n_col)
    me = me_r * n_col + me_c
    n_img, hh, ww, n_ch = yv.shape
    bh, bw = hh // n_row, ww // n_col
    weights, temb_copy = _weight_copies(1, conv_hbm, wconv, wtemb_hbm, wtemb, wsem)
    for w in [temb_copy, *weights]:
        w.start()
    blk = _ResBlock(hh, ww, n_ch, rnorm_ref.at[1], wconv, act, hid, temb_s, grp_s)
    temb_copy.wait()
    blk.setup(temb_ref, wtemb)
    _barrier(peers)
    first_chunk = lax.rem(me_r + n_row // 2, n_row) // (n_row // 2) * (n_row // 2)

    def block(s, k, c):
        return yv.at[s, pl.ds(k * bh, bh), pl.ds(pl.multiple_of(c * bw, bw), bw), :]

    def rel(k, c):
        return lax.rem(k - me_r + n_row, n_row) * n_col + lax.rem(c - me_c + n_col, n_col)

    def copy(s, k, c):
        return pltpu.make_async_remote_copy(
            block(s, k, c), o_ref.at[me * n_img + s], send_sem.at[s, rel(k, c)], recv_sem.at[s, rel(k, c)],
            device_id={'row': k, 'col': c}, device_id_type=MESH)

    def own(s):
        return pltpu.make_async_copy(block(s, me_r, me_c), o_ref.at[me * n_img + s], loc_sem.at[s])

    def image(s, carry):
        def src(r0, n):
            return x_ref[s, pl.ds(r0, n), :]

        def dst(k, r0, v):
            yv[s, pl.ds(r0 // ww, ROWS_PER_CHUNK)] = v.reshape(ROWS_PER_CHUNK, ww, n_ch)
            for d in range(n_col):
                c = lax.rem(me_c + 1 + d, n_col)
                remote = (k != me_r) | (c != me_c)

                @pl.when(remote)
                def _():
                    copy(s, k, c).start()

                @pl.when(jnp.logical_not(remote))
                def _():
                    own(s).start()

        def wait_weight(j):
            @pl.when(s == 0)
            def _():
                weights[j].wait()

        blk.run(src, me * n_img + s, wait_weight, first_chunk, dst)
        return carry

    lax.fori_loop(0, n_img, image, 0)
    for s in range(n_img):
        for r, c in peers:
            copy(s, r, c).wait()
        own(s).wait()


def _attn_kernel(x_ref, anorm_ref, proj_ref, o_ref, grp_s, k_buf, q_buf, v_buf, ot_buf):
    n_pos, n_ch = x_ref.shape[1:]
    count = float(n_pos * (n_ch // GROUPS))
    head_dim = 32
    n_heads = n_ch // head_dim
    per_blk = 128 // head_dim
    scale = LOG2E * head_dim ** -0.5

    @pl.when(pl.program_id(0) == 0)
    def _():
        grp_s[...] = _group_matrix(n_ch)

    def in_sums(i, sums):
        d1, d2 = _chan_sums(x_ref[0, pl.ds(pl.multiple_of(i * 256, 256), 256), :].astype(F32))
        return sums[0] + d1, sums[1] + d2

    sums = lax.fori_loop(0, n_pos // 256, in_sums, _zero_sums(n_ch))
    mean, inv = _moments(*sums, grp_s[...], count)
    a_mul = inv * anorm_ref[0:1].astype(F32)
    b_add = anorm_ref[1:2].astype(F32)
    head_rows = jnp.where(lax.broadcasted_iota(jnp.int32, (16, n_ch), 0)
                          == lax.broadcasted_iota(jnp.int32, (16, n_ch), 1) // head_dim, 1.0, 0.0).astype(BF16)

    def project(i, tops):
        r0 = pl.multiple_of(i * 256, 256)
        g = ((x_ref[0, pl.ds(r0, 256), :].astype(F32) - mean) * a_mul + b_add).astype(BF16)
        q = _dot(proj_ref[0], g, ((1,), (1,))).astype(BF16)
        v = _dot(proj_ref[2], g, ((1,), (1,))).astype(BF16)
        k = _dot(g, proj_ref[1], ((1,), (1,))).astype(BF16)
        q_buf[:, pl.ds(r0, 256)] = q
        v_buf[:, pl.ds(r0, 256)] = v
        k_buf[pl.ds(r0, 256), :] = k
        q2 = _dot(head_rows, (q.astype(F32) * q.astype(F32)).astype(BF16))
        k2 = _dot(head_rows, (k.astype(F32) * k.astype(F32)).astype(BF16), ((1,), (1,)))
        v_top = jnp.max(jnp.abs(v.astype(F32)), axis=0, keepdims=True)
        return jnp.maximum(tops[0], q2), jnp.maximum(tops[1], k2), jnp.maximum(tops[2], v_top)

    tops = lax.fori_loop(0, n_pos // 256, project,
                         (jnp.zeros((16, 256), F32), jnp.zeros((16, 256), F32), jnp.zeros((1, 256), F32)))
    q_top = jnp.max(tops[0], axis=1, keepdims=True)
    k_top = jnp.max(tops[1], axis=1, keepdims=True)
    top2 = jnp.max(q_top * k_top) * (scale * scale)
    v_max = jnp.max(tops[2])
    small = ((top2 < 96.0 ** 2) & (v_max < 2.0 ** 20)) | ((top2 < 108.0 ** 2) & (v_max < 2.0 ** 8))

    @pl.when(small)
    def _():
        rh = lax.broadcasted_iota(jnp.int32, (128, Q_TILE), 0) // head_dim
        n_kc = n_pos // K_CHUNK

        def heads(b, carry):
            b0 = pl.multiple_of(b * 128, 128)
            tiles = [(j, t * Q_TILE) for j in range(per_blk) for t in range(n_pos // Q_TILE)]
            steps = [(tile, c) for tile in tiles for c in range(n_kc)]
            masked = {}

            def score(step):
                tile, c = step
                if tile not in masked:
                    j, q0 = tile
                    masked[tile] = jnp.where(rh == j, q_buf[pl.ds(b0, 128), q0:q0 + Q_TILE], 0)
                return _dot(k_buf[c * K_CHUNK:(c + 1) * K_CHUNK, pl.ds(b0, 128)], masked[tile])

            pending = [score(s) for s in steps[:AHEAD]]
            tot = out = None
            for n, ((j, q0), c) in enumerate(steps):
                if n + AHEAD < len(steps):
                    pending.append(score(steps[n + AHEAD]))
                p = jnp.exp2(pending.pop(0) * scale)
                h0 = pl.multiple_of(b0 + j * head_dim, head_dim)
                part = jnp.sum(p.reshape(K_CHUNK // 8, 8, Q_TILE), axis=0)
                pv = _dot(v_buf[pl.ds(h0, head_dim), c * K_CHUNK:(c + 1) * K_CHUNK], p.astype(BF16))
                tot, out = (part, pv) if c == 0 else (tot + part, out + pv)
                if c == n_kc - 1:
                    res = out / jnp.sum(tot, axis=0, keepdims=True)
                    ot_buf[pl.ds(h0, head_dim), q0:q0 + Q_TILE] = res.astype(BF16)
            return carry

        lax.fori_loop(0, n_ch // 128, heads, 0)

    @pl.when(jnp.logical_not(small))
    def _():
        rh = lax.broadcasted_iota(jnp.int32, (128, 256), 0) // head_dim
        n_tiles = n_pos // 256

        def tile(i, carry):
            h = i // n_tiles
            q0 = pl.multiple_of((i % n_tiles) * 256, 256)
            b0 = pl.multiple_of((h // per_blk) * 128, 128)
            h0 = pl.multiple_of(h * head_dim, head_dim)
            qm = jnp.where(rh == h % per_blk, q_buf[pl.ds(b0, 128), pl.ds(q0, 256)], 0)
            s = _dot(k_buf[:, pl.ds(b0, 128)], qm)
            p = jnp.exp2((s - jnp.max(s, axis=0, keepdims=True)) * scale)
            o = _dot(v_buf[pl.ds(h0, head_dim), :], p.astype(BF16))
            ot_buf[pl.ds(h0, head_dim), pl.ds(q0, 256)] = (o / jnp.sum(p, axis=0, keepdims=True)).astype(BF16)
            return carry

        lax.fori_loop(0, n_heads * n_tiles, tile, 0)

    def out_proj(i, carry):
        r0 = pl.multiple_of(i * 256, 256)
        acc = _dot(ot_buf[:, pl.ds(r0, 256)], proj_ref[3], ((0,), (0,)))
        o_ref[0, pl.ds(r0, 256), :] = (x_ref[0, pl.ds(r0, 256), :].astype(F32) + acc).astype(BF16)
        return carry

    lax.fori_loop(0, n_pos // 256, out_proj, 0)


VMEM_LIMIT = 60 * 1024 * 1024


def _res_scratch(hh, ww, n_ch, n_batch, n_temb, n_img, n_dev):
    return [
        pltpu.VMEM((n_img, hh, ww, n_ch), BF16),
        pltpu.VMEM((2, 9 * n_ch, n_ch), BF16),
        pltpu.VMEM((n_temb, n_ch), BF16),
        pltpu.VMEM(((hh + 2) * ww, 3 * n_ch), BF16),
        pltpu.VMEM((hh * ww, n_ch), BF16),
        pltpu.VMEM((n_batch, n_ch), F32),
        pltpu.VMEM((n_ch, n_ch), BF16),
        pltpu.SemaphoreType.DMA((3,)),
        pltpu.SemaphoreType.DMA((n_img, n_dev)),
        pltpu.SemaphoreType.DMA((n_img, n_dev)),
        pltpu.SemaphoreType.DMA((n_img,)),
    ]


def solution(mesh):
    n_row, n_col = mesh.shape['row'], mesh.shape['col']
    n_dev = n_row * n_col
    vmem, hbm = pl.BlockSpec(memory_space=pltpu.VMEM), pl.BlockSpec(memory_space=pl.ANY)

    def run_stage(latent, t_emb, res_norm, res_conv, res_temb, attn_norm, attn_proj):
        n_batch, bh, bw, n_ch = latent.shape
        hh, ww = bh * n_row, bw * n_col
        n_pos, n_img = hh * ww, n_batch // n_dev
        proj = jnp.transpose(attn_proj, (0, 1, 3, 2)).reshape(4, n_ch, n_ch)
        conv_w = res_conv.reshape(2, 2, 9 * n_ch, n_ch)
        scratch = _res_scratch(hh, ww, n_ch, n_batch, t_emb.shape[1], n_img, n_dev)

        x1 = pl.pallas_call(
            functools.partial(_first_kernel, n_row, n_col),
            out_shape=jax.ShapeDtypeStruct((n_img, n_pos, n_ch), BF16),
            in_specs=[hbm, vmem, vmem, hbm, hbm],
            out_specs=vmem,
            scratch_shapes=scratch,
            compiler_params=pltpu.CompilerParams(collective_id=0, has_side_effects=True, vmem_limit_bytes=VMEM_LIMIT),
        )(latent, t_emb, res_norm, conv_w, res_temb)

        def whole(a):
            return pl.BlockSpec(a.shape, lambda i, nd=a.ndim: (0,) * nd, pipeline_mode=pl.Buffered(1))

        img_spec = pl.BlockSpec((1, n_pos, n_ch), lambda i: (i, 0, 0))
        x2 = pl.pallas_call(
            _attn_kernel,
            grid=(n_img,),
            out_shape=jax.ShapeDtypeStruct((n_img, n_pos, n_ch), BF16),
            in_specs=[img_spec, whole(attn_norm), whole(proj)],
            out_specs=img_spec,
            scratch_shapes=[
                pltpu.VMEM((n_ch, n_ch), BF16),
                pltpu.VMEM((n_pos, n_ch), BF16),
                pltpu.VMEM((n_ch, n_pos), BF16),
                pltpu.VMEM((n_ch, n_pos), BF16),
                pltpu.VMEM((n_ch, n_pos), BF16),
            ],
            compiler_params=pltpu.CompilerParams(dimension_semantics=("arbitrary",), vmem_limit_bytes=VMEM_LIMIT),
        )(x1, attn_norm, proj)

        return pl.pallas_call(
            functools.partial(_last_kernel, n_row, n_col),
            out_shape=jax.ShapeDtypeStruct(latent.shape, BF16),
            in_specs=[vmem, vmem, vmem, hbm, hbm],
            out_specs=hbm,
            scratch_shapes=scratch,
            compiler_params=pltpu.CompilerParams(collective_id=1, has_side_effects=True, vmem_limit_bytes=VMEM_LIMIT),
        )(x2, t_emb, res_norm, conv_w, res_temb)

    spec_x = P('dp', 'row', 'col', None)
    return jax.shard_map(run_stage, mesh=mesh, in_specs=(spec_x, P('dp', None), P(), P(), P(), P(), P()), out_specs=spec_x, check_vma=False)
```

```python
import functools

import jax
import jax.numpy as jnp
from jax import lax
from jax.experimental import pallas as pl
from jax.experimental.pallas import tpu as pltpu
from jax.sharding import PartitionSpec as P

MESH = pl.DeviceIdType.MESH
GROUPS = 32
EPS = 1e-5
LOG2E = 1.4426950408889634
F32 = jnp.float32
BF16 = jnp.bfloat16
Q_TILE = 512
K_CHUNK = 256
AHEAD = 2
N_CHUNKS = 2


def _me_and_peers(n_row, n_col):
    me_r, me_c = lax.axis_index('row'), lax.axis_index('col')
    peers = []
    for k in range(1, n_row * n_col):
        peers.append((lax.rem(me_r + k // n_col, n_row), lax.rem(me_c + k % n_col, n_col)))
    return me_r, me_c, peers


def _barrier(peers):
    sem = pltpu.get_barrier_semaphore()
    for r, c in peers:
        pl.semaphore_signal(sem, inc=1, device_id={'row': r, 'col': c}, device_id_type=MESH)
    pl.semaphore_wait(sem, len(peers))


def _dot(a, b, dims=((1,), (0,))):
    return lax.dot_general(a, b, (dims, ((), ())), preferred_element_type=F32)


def _chan_sums(v):
    return jnp.sum(v, axis=0, keepdims=True), jnp.sum(v * v, axis=0, keepdims=True)


def _group_matrix(n_ch):
    per = n_ch // GROUPS
    gi = lax.broadcasted_iota(jnp.int32, (n_ch, n_ch), 0) // per
    gj = lax.broadcasted_iota(jnp.int32, (n_ch, n_ch), 1) // per
    return jnp.where(gi == gj, 1.0, 0.0).astype(BF16)


def _moments(s1, s2, grp, count):
    n_ch = s1.shape[1]
    st = jnp.concatenate([s1, s2, jnp.zeros((6, n_ch), F32)], axis=0)
    hi = st.astype(BF16)
    r1 = st - hi.astype(F32)
    mid = r1.astype(BF16)
    lo = (r1 - mid.astype(F32)).astype(BF16)
    tot = (_dot(lo, grp) + _dot(mid, grp)) + _dot(hi, grp)
    mean = tot[0:1] / count
    var = tot[1:2] / count - mean * mean
    return mean, lax.rsqrt(var + EPS)


def _zero_sums(n_ch):
    return jnp.zeros((1, n_ch), F32), jnp.zeros((1, n_ch), F32)


class _ResBlock:
    def __init__(self, hh, ww, n_ch, rnorm_ref, w_t, act, hid, temb_s, grp_s):
        self.hh, self.ww, self.n_ch = hh, ww, n_ch
        self.rnorm_ref, self.w_t, self.act, self.hid = rnorm_ref, w_t, act, hid
        self.temb_s, self.grp_s = temb_s, grp_s
        self.rows = hh // N_CHUNKS
        self.count = float(hh * ww * (n_ch // GROUPS))

    def setup(self, temb_ref, wtemb_ref):
        te = temb_ref[...].astype(F32)
        t_act = (te * jax.nn.sigmoid(te)).astype(BF16)
        self.temb_s[...] = _dot(t_act, wtemb_ref[...])
        self.grp_s[...] = _group_matrix(self.n_ch)
        zeros = jnp.zeros((self.ww, self.act.shape[1]), BF16)
        self.act[0:self.ww, :] = zeros
        self.act[(self.hh + 1) * self.ww:(self.hh + 2) * self.ww, :] = zeros

    def conv(self, j, src, sums, epilogue):
        ww, n_ch, act = self.ww, self.n_ch, self.act
        mean, inv = _moments(*sums, self.grp_s[...], self.count)
        a_mul = inv * self.rnorm_ref[j, 0:1].astype(F32)
        b_add = self.rnorm_ref[j, 1:2].astype(F32)
        col = lax.broadcasted_iota(jnp.int32, (ww, 1), 0)

        def fill(i):
            u = (src(i, 1).astype(F32) - mean) * a_mul + b_add
            a = u * (0.5 * jnp.tanh(0.5 * u) + 0.5)
            left = jnp.where(col == 0, 0.0, pltpu.roll(a, 1, 0))
            right = jnp.where(col == ww - 1, 0.0, pltpu.roll(a, ww - 1, 0))
            d0 = (i + 1) * ww
            act[d0:d0 + ww, 0:n_ch] = left.astype(BF16)
            act[d0:d0 + ww, n_ch:2 * n_ch] = a.astype(BF16)
            act[d0:d0 + ww, 2 * n_ch:3 * n_ch] = right.astype(BF16)

        filled, s1, s2 = 0, *_zero_sums(n_ch)
        for k in range(N_CHUNKS):
            need = min(self.hh, (k + 1) * self.rows + 1)
            for i in range(filled, need):
                fill(i)
            filled = need
            r0, n = k * self.rows * ww, self.rows * ww
            lhs = jnp.concatenate([act[r0 + dy * ww:r0 + dy * ww + n, :] for dy in range(3)], axis=1)
            out = epilogue(k, _dot(self.w_t[j], lhs, ((1,), (1,))).T)
            d1, d2 = _chan_sums(out.astype(F32))
            s1, s2 = s1 + d1, s2 + d2
        return s1, s2

    def run(self, src, sums, img, wait_weight, dst):
        hid, rows = self.hid, self.rows
        t_row = self.temb_s[pl.ds(img, 1), :]

        def shape4(v):
            return v.reshape(rows, self.ww, self.n_ch)

        def first(k, acc):
            out = (acc + t_row).astype(BF16)
            hid[k * rows:(k + 1) * rows] = shape4(out)
            return out

        def second(k, acc):
            out = (src(k * rows, rows).astype(F32) + acc).astype(BF16)
            dst(k, shape4(out))
            return out

        wait_weight(0)
        sums = self.conv(0, src, sums, first)
        wait_weight(1)
        return self.conv(1, lambda i, n: hid[i:i + n].reshape(n * self.ww, self.n_ch), sums, second)


def _first_kernel(n_row, n_col, lat_ref, temb_ref, rnorm_ref, conv_hbm, wtemb_hbm, o_ref, sums_ref, next_w,
                  xv, wconv, w_t, wtemb, act, hid, temb_s, grp_s, wsem, send_sem, recv_sem, loc_sem):
    me_r, me_c, peers = _me_and_peers(n_row, n_col)
    me = me_r * n_col + me_c
    n_img, hh, ww, n_ch = xv.shape
    bh, bw = hh // n_row, ww // n_col
    weights = [pltpu.make_async_copy(conv_hbm.at[i // 2, i % 2], wconv.at[i], wsem.at[i]) for i in range(4)]
    temb_copy = pltpu.make_async_copy(wtemb_hbm.at[0], wtemb, wsem.at[4])
    pass_on = pltpu.make_async_copy(w_t.at[pl.ds(2, 2)], next_w, wsem.at[5])

    def place(s):
        return xv.at[s, pl.ds(me_r * bh, bh), pl.ds(pl.multiple_of(me_c * bw, bw), bw), :]

    def copy(s, k):
        r, c = peers[k]
        return pltpu.make_async_remote_copy(
            lat_ref.at[(r * n_col + c) * n_img + s], place(s), send_sem.at[s, k], recv_sem.at[s, k],
            device_id={'row': r, 'col': c}, device_id_type=MESH)

    def own(s):
        return pltpu.make_async_copy(lat_ref.at[me * n_img + s], place(s), loc_sem.at[s])

    _barrier(peers)
    for s in range(n_img):
        for k in range(len(peers)):
            copy(s, k).start()
        own(s).start()
    for w in [temb_copy, *weights]:
        w.start()

    blk = _ResBlock(hh, ww, n_ch, rnorm_ref.at[0], w_t, act, hid, temb_s, grp_s)
    temb_copy.wait()
    blk.setup(temb_ref, wtemb)
    for w in weights:
        w.wait()

    def turn(i, carry):
        t0 = pl.multiple_of(i * n_ch, n_ch)
        for j in range(4):
            w_t[j, :, pl.ds(t0, n_ch)] = wconv[j, pl.ds(t0, n_ch), :].T
        return carry

    lax.fori_loop(0, 9, turn, 0)
    pass_on.start()

    def image(s, carry):
        for k in range(len(peers)):
            copy(s, k).wait_recv()
        own(s).wait()

        def src(i, n):
            return xv[s, pl.ds(i, n)].reshape(n * ww, n_ch)

        def in_sums(i, sums):
            d1, d2 = _chan_sums(src(i * 4, 4).astype(F32))
            return sums[0] + d1, sums[1] + d2

        def dst(k, v):
            o_ref[s, k * blk.rows:(k + 1) * blk.rows] = v

        sums = lax.fori_loop(0, hh // 4, in_sums, _zero_sums(n_ch))
        s1, s2 = blk.run(src, sums, me * n_img + s, lambda j: None, dst)
        sums_ref[s, 0:1] = s1
        sums_ref[s, 1:2] = s2
        return carry

    lax.fori_loop(0, n_img, image, 0)
    pass_on.wait()
    for s in range(n_img):
        for k in range(len(peers)):
            copy(s, k).wait_send()


def _last_kernel(n_row, n_col, x_ref, sums_ref, temb_ref, rnorm_ref, w_hbm, wtemb_hbm, o_ref,
                 yv, w_t, wtemb, act, hid, temb_s, grp_s, wsem, send_sem, recv_sem, loc_sem):
    me_r, me_c, peers = _me_and_peers(n_row, n_col)
    me = me_r * n_col + me_c
    n_img, hh, ww, n_ch = yv.shape
    bh, bw = hh // n_row, ww // n_col
    weights = [pltpu.make_async_copy(w_hbm.at[i], w_t.at[i], wsem.at[i]) for i in range(2)]
    temb_copy = pltpu.make_async_copy(wtemb_hbm.at[1], wtemb, wsem.at[2])
    for w in [temb_copy, *weights]:
        w.start()
    blk = _ResBlock(hh, ww, n_ch, rnorm_ref.at[1], w_t, act, hid, temb_s, grp_s)
    temb_copy.wait()
    blk.setup(temb_ref, wtemb)
    _barrier(peers)

    def block(s, k, c):
        return yv.at[s, pl.ds(k * bh, bh), pl.ds(pl.multiple_of(c * bw, bw), bw), :]

    def rel(k, c):
        return lax.rem(k - me_r + n_row, n_row) * n_col + lax.rem(c - me_c + n_col, n_col)

    def copy(s, k, c):
        return pltpu.make_async_remote_copy(
            block(s, k, c), o_ref.at[me * n_img + s], send_sem.at[s, rel(k, c)], recv_sem.at[s, rel(k, c)],
            device_id={'row': k, 'col': c}, device_id_type=MESH)

    def own(s):
        return pltpu.make_async_copy(block(s, me_r, me_c), o_ref.at[me * n_img + s], loc_sem.at[s])

    def image(s, carry):
        def src(i, n):
            return x_ref[s, pl.ds(i, n)].reshape(n * ww, n_ch)

        def dst(k, v):
            yv[s, k * blk.rows:(k + 1) * blk.rows] = v
            per = blk.rows // bh
            for d in range(per * n_col):
                kk = k * per + d // n_col
                c = lax.rem(me_c + 1 + d, n_col)
                remote = (kk != me_r) | (c != me_c)

                @pl.when(remote)
                def _():
                    copy(s, kk, c).start()

                @pl.when(jnp.logical_not(remote))
                def _():
                    own(s).start()

        def wait_weight(j):
            @pl.when(s == 0)
            def _():
                weights[j].wait()

        blk.run(src, (sums_ref[s, 0:1], sums_ref[s, 1:2]), me * n_img + s, wait_weight, dst)
        return carry

    lax.fori_loop(0, n_img, image, 0)
    for s in range(n_img):
        for r, c in peers:
            copy(s, r, c).wait()
        own(s).wait()


def _attn_kernel(x_ref, sums_ref, anorm_ref, proj_ref, o_ref, osums_ref, grp_s, k_buf, q_buf, v_buf, ot_buf):
    n_pos, n_ch = x_ref.shape[1:]
    count = float(n_pos * (n_ch // GROUPS))
    head_dim = 32
    n_heads = n_ch // head_dim
    per_blk = 128 // head_dim
    scale = LOG2E * head_dim ** -0.5

    @pl.when(pl.program_id(0) == 0)
    def _():
        grp_s[...] = _group_matrix(n_ch)

    sums = sums_ref[0, 0:1], sums_ref[0, 1:2]
    mean, inv = _moments(*sums, grp_s[...], count)
    a_mul = inv * anorm_ref[0:1].astype(F32)
    b_add = anorm_ref[1:2].astype(F32)
    head_rows = jnp.where(lax.broadcasted_iota(jnp.int32, (16, n_ch), 0)
                          == lax.broadcasted_iota(jnp.int32, (16, n_ch), 1) // head_dim, 1.0, 0.0).astype(BF16)

    def project(i, tops):
        r0 = pl.multiple_of(i * 256, 256)
        g = ((x_ref[0, pl.ds(r0, 256), :].astype(F32) - mean) * a_mul + b_add).astype(BF16)
        q = _dot(proj_ref[0], g, ((1,), (1,))).astype(BF16)
        v = _dot(proj_ref[2], g, ((1,), (1,))).astype(BF16)
        k = _dot(g, proj_ref[1], ((1,), (1,))).astype(BF16)
        q_buf[:, pl.ds(r0, 256)] = q
        v_buf[:, pl.ds(r0, 256)] = v
        k_buf[pl.ds(r0, 256), :] = k
        q2 = _dot(head_rows, (q.astype(F32) * q.astype(F32)).astype(BF16))
        k2 = _dot(head_rows, (k.astype(F32) * k.astype(F32)).astype(BF16), ((1,), (1,)))
        v_top = jnp.max(jnp.abs(v.astype(F32)), axis=0, keepdims=True)
        return jnp.maximum(tops[0], q2), jnp.maximum(tops[1], k2), jnp.maximum(tops[2], v_top)

    tops = lax.fori_loop(0, n_pos // 256, project,
                         (jnp.zeros((16, 256), F32), jnp.zeros((16, 256), F32), jnp.zeros((1, 256), F32)))
    q_top = jnp.max(tops[0], axis=1, keepdims=True)
    k_top = jnp.max(tops[1], axis=1, keepdims=True)
    top2 = jnp.max(q_top * k_top) * (scale * scale)
    v_max = jnp.max(tops[2])
    small = ((top2 < 96.0 ** 2) & (v_max < 2.0 ** 20)) | ((top2 < 108.0 ** 2) & (v_max < 2.0 ** 8))

    @pl.when(small)
    def _():
        rh = lax.broadcasted_iota(jnp.int32, (128, Q_TILE), 0) // head_dim
        n_kc = n_pos // K_CHUNK

        def heads(b, carry):
            b0 = pl.multiple_of(b * 128, 128)
            tiles = [(j, t * Q_TILE) for j in range(per_blk) for t in range(n_pos // Q_TILE)]
            steps = [(tile, c) for tile in tiles for c in range(n_kc)]
            masked = {}

            def score(step):
                tile, c = step
                if tile not in masked:
                    j, q0 = tile
                    masked[tile] = jnp.where(rh == j, q_buf[pl.ds(b0, 128), q0:q0 + Q_TILE], 0)
                return _dot(k_buf[c * K_CHUNK:(c + 1) * K_CHUNK, pl.ds(b0, 128)], masked[tile])

            pending = [score(s) for s in steps[:AHEAD]]
            tot = out = None
            for n, ((j, q0), c) in enumerate(steps):
                if n + AHEAD < len(steps):
                    pending.append(score(steps[n + AHEAD]))
                p = jnp.exp2(pending.pop(0) * scale)
                h0 = pl.multiple_of(b0 + j * head_dim, head_dim)
                part = jnp.sum(p.reshape(K_CHUNK // 8, 8, Q_TILE), axis=0)
                pv = _dot(v_buf[pl.ds(h0, head_dim), c * K_CHUNK:(c + 1) * K_CHUNK], p.astype(BF16))
                tot, out = (part, pv) if c == 0 else (tot + part, out + pv)
                if c == n_kc - 1:
                    res = out / jnp.sum(tot, axis=0, keepdims=True)
                    ot_buf[pl.ds(h0, head_dim), q0:q0 + Q_TILE] = res.astype(BF16)
            return carry

        lax.fori_loop(0, n_ch // 128, heads, 0)

    @pl.when(jnp.logical_not(small))
    def _():
        rh = lax.broadcasted_iota(jnp.int32, (128, 256), 0) // head_dim
        n_tiles = n_pos // 256

        def tile(i, carry):
            h = i // n_tiles
            q0 = pl.multiple_of((i % n_tiles) * 256, 256)
            b0 = pl.multiple_of((h // per_blk) * 128, 128)
            h0 = pl.multiple_of(h * head_dim, head_dim)
            qm = jnp.where(rh == h % per_blk, q_buf[pl.ds(b0, 128), pl.ds(q0, 256)], 0)
            s = _dot(k_buf[:, pl.ds(b0, 128)], qm)
            p = jnp.exp2((s - jnp.max(s, axis=0, keepdims=True)) * scale)
            o = _dot(v_buf[pl.ds(h0, head_dim), :], p.astype(BF16))
            ot_buf[pl.ds(h0, head_dim), pl.ds(q0, 256)] = (o / jnp.sum(p, axis=0, keepdims=True)).astype(BF16)
            return carry

        lax.fori_loop(0, n_heads * n_tiles, tile, 0)

    def out_proj(i, sums):
        r0 = pl.multiple_of(i * 256, 256)
        acc = _dot(ot_buf[:, pl.ds(r0, 256)], proj_ref[3], ((0,), (0,)))
        out = (x_ref[0, pl.ds(r0, 256), :].astype(F32) + acc).astype(BF16)
        o_ref[0, pl.ds(r0, 256), :] = out
        d1, d2 = _chan_sums(out.astype(F32))
        return sums[0] + d1, sums[1] + d2

    s1, s2 = lax.fori_loop(0, n_pos // 256, out_proj, _zero_sums(n_ch))
    osums_ref[0, 0:1] = s1
    osums_ref[0, 1:2] = s2


VMEM_LIMIT = 60 * 1024 * 1024


def solution(mesh):
    n_row, n_col = mesh.shape['row'], mesh.shape['col']
    n_dev = n_row * n_col
    vmem, hbm = pl.BlockSpec(memory_space=pltpu.VMEM), pl.BlockSpec(memory_space=pl.ANY)

    def run_stage(latent, t_emb, res_norm, res_conv, res_temb, attn_norm, attn_proj):
        n_batch, bh, bw, n_ch = latent.shape
        hh, ww = bh * n_row, bw * n_col
        n_pos, n_img = hh * ww, n_batch // n_dev
        proj = jnp.transpose(attn_proj, (0, 1, 3, 2)).reshape(4, n_ch, n_ch)
        conv_w = res_conv.reshape(2, 2, 9 * n_ch, n_ch)
        sums_shape = jax.ShapeDtypeStruct((n_img, 8, n_ch), F32)
        images = pltpu.VMEM((n_img, hh, ww, n_ch), BF16)
        work = [
            pltpu.VMEM((t_emb.shape[1], n_ch), BF16),
            pltpu.VMEM(((hh + 2) * ww, 3 * n_ch), BF16),
            pltpu.VMEM((hh, ww, n_ch), BF16),
            pltpu.VMEM((n_batch, n_ch), F32),
            pltpu.VMEM((n_ch, n_ch), BF16),
            pltpu.SemaphoreType.DMA((6,)),
            pltpu.SemaphoreType.DMA((n_img, n_dev)),
            pltpu.SemaphoreType.DMA((n_img, n_dev)),
            pltpu.SemaphoreType.DMA((n_img,)),
        ]

        x1, sums1, next_w = pl.pallas_call(
            functools.partial(_first_kernel, n_row, n_col),
            out_shape=[jax.ShapeDtypeStruct((n_img, hh, ww, n_ch), BF16), sums_shape,
                       jax.ShapeDtypeStruct((2, n_ch, 9 * n_ch), BF16)],
            in_specs=[hbm, vmem, vmem, hbm, hbm],
            out_specs=[vmem, vmem, hbm],
            scratch_shapes=[images, pltpu.VMEM((4, 9 * n_ch, n_ch), BF16), pltpu.VMEM((4, n_ch, 9 * n_ch), BF16), *work],
            compiler_params=pltpu.CompilerParams(collective_id=0, has_side_effects=True, vmem_limit_bytes=VMEM_LIMIT),
        )(latent, t_emb, res_norm, conv_w, res_temb)

        def whole(a):
            return pl.BlockSpec(a.shape, lambda i, nd=a.ndim: (0,) * nd, pipeline_mode=pl.Buffered(1))

        img_spec = pl.BlockSpec((1, n_pos, n_ch), lambda i: (i, 0, 0))
        sums_spec = pl.BlockSpec((1, 8, n_ch), lambda i: (i, 0, 0))
        x2, sums2 = pl.pallas_call(
            _attn_kernel,
            grid=(n_img,),
            out_shape=[jax.ShapeDtypeStruct((n_img, n_pos, n_ch), BF16), sums_shape],
            in_specs=[img_spec, sums_spec, whole(attn_norm), whole(proj)],
            out_specs=[img_spec, sums_spec],
            scratch_shapes=[
                pltpu.VMEM((n_ch, n_ch), BF16),
                pltpu.VMEM((n_pos, n_ch), BF16),
                pltpu.VMEM((n_ch, n_pos), BF16),
                pltpu.VMEM((n_ch, n_pos), BF16),
                pltpu.VMEM((n_ch, n_pos), BF16),
            ],
            compiler_params=pltpu.CompilerParams(dimension_semantics=("arbitrary",), vmem_limit_bytes=VMEM_LIMIT),
        )(x1.reshape(n_img, n_pos, n_ch), sums1, attn_norm, proj)

        return pl.pallas_call(
            functools.partial(_last_kernel, n_row, n_col),
            out_shape=jax.ShapeDtypeStruct(latent.shape, BF16),
            in_specs=[vmem, vmem, vmem, vmem, hbm, hbm],
            out_specs=hbm,
            scratch_shapes=[images, pltpu.VMEM((2, n_ch, 9 * n_ch), BF16), *work],
            compiler_params=pltpu.CompilerParams(collective_id=1, has_side_effects=True, vmem_limit_bytes=VMEM_LIMIT),
        )(x2.reshape(n_img, hh, ww, n_ch), sums2, t_emb, res_norm, next_w, res_temb)

    spec_x = P('dp', 'row', 'col', None)
    return jax.shard_map(run_stage, mesh=mesh, in_specs=(spec_x, P('dp', None), P(), P(), P(), P(), P()), out_specs=spec_x, check_vma=False)
```

```python
import functools

import jax
import jax.numpy as jnp
from jax import lax
from jax.experimental import pallas as pl
from jax.experimental.pallas import tpu as pltpu
from jax.sharding import PartitionSpec as P

MESH = pl.DeviceIdType.MESH
GROUPS = 32
EPS = 1e-5
LOG2E = 1.4426950408889634
F32 = jnp.float32
BF16 = jnp.bfloat16
Q_TILE = 512
K_CHUNK = 256
AHEAD = 2
CHUNK = 768
LAST_CHUNK = 512
PROJ_TILE = 512


def _me_and_peers(n_row, n_col):
    me_r, me_c = lax.axis_index('row'), lax.axis_index('col')
    peers = []
    for k in range(1, n_row * n_col):
        peers.append((lax.rem(me_r + k // n_col, n_row), lax.rem(me_c + k % n_col, n_col)))
    return me_r, me_c, peers


def _barrier(peers):
    sem = pltpu.get_barrier_semaphore()
    for r, c in peers:
        pl.semaphore_signal(sem, inc=1, device_id={'row': r, 'col': c}, device_id_type=MESH)
    pl.semaphore_wait(sem, len(peers))


def _dot(a, b, dims=((1,), (0,))):
    return lax.dot_general(a, b, (dims, ((), ())), preferred_element_type=F32)


def _chan_sums(v):
    return jnp.sum(v, axis=0, keepdims=True), jnp.sum(v * v, axis=0, keepdims=True)


def _group_matrix(n_ch):
    per = n_ch // GROUPS
    gi = lax.broadcasted_iota(jnp.int32, (n_ch, n_ch), 0) // per
    gj = lax.broadcasted_iota(jnp.int32, (n_ch, n_ch), 1) // per
    return jnp.where(gi == gj, 1.0, 0.0).astype(BF16)


def _moments(s1, s2, grp, count):
    n_ch = s1.shape[1]
    st = jnp.concatenate([s1, s2, jnp.zeros((6, n_ch), F32)], axis=0)
    hi = st.astype(BF16)
    r1 = st - hi.astype(F32)
    mid = r1.astype(BF16)
    lo = (r1 - mid.astype(F32)).astype(BF16)
    tot = (_dot(lo, grp) + _dot(mid, grp)) + _dot(hi, grp)
    mean = tot[0:1] / count
    var = tot[1:2] / count - mean * mean
    return mean, lax.rsqrt(var + EPS)


def _zero_sums(n_ch):
    return jnp.zeros((1, n_ch), F32), jnp.zeros((1, n_ch), F32)


class _ResBlock:
    def __init__(self, hh, ww, n_ch, rnorm_ref, w_t, act, hid, temb_s, grp_s, sums_s):
        self.hh, self.ww, self.n_ch = hh, ww, n_ch
        self.rnorm_ref, self.w_t, self.act, self.hid = rnorm_ref, w_t, act, hid
        self.temb_s, self.grp_s, self.sums_s = temb_s, grp_s, sums_s
        self.count = float(hh * ww * (n_ch // GROUPS))

    def setup(self, temb_ref, wtemb_ref):
        te = temb_ref[...].astype(F32)
        t_act = (te * jax.nn.sigmoid(te)).astype(BF16)
        self.temb_s[...] = _dot(t_act, wtemb_ref[...])
        self.grp_s[...] = _group_matrix(self.n_ch)
        zeros = jnp.zeros((self.ww, self.act.shape[1]), BF16)
        self.act[0:self.ww, :] = zeros
        self.act[(self.hh + 1) * self.ww:(self.hh + 2) * self.ww, :] = zeros

    def conv(self, j, src, sums, chunk, epilogue):
        ww, n_ch, act = self.ww, self.n_ch, self.act
        mean, inv = _moments(*sums, self.grp_s[...], self.count)
        a_mul = inv * self.rnorm_ref[j, 0:1].astype(F32)
        b_add = self.rnorm_ref[j, 1:2].astype(F32)
        col = lax.broadcasted_iota(jnp.int32, (ww, 1), 0)

        def fill(i):
            u = (src(i * ww, ww).astype(F32) - mean) * a_mul + b_add
            a = u * (0.5 * jnp.tanh(0.5 * u) + 0.5)
            left = jnp.where(col == 0, 0.0, pltpu.roll(a, 1, 0))
            right = jnp.where(col == ww - 1, 0.0, pltpu.roll(a, ww - 1, 0))
            d0 = (i + 1) * ww
            act[d0:d0 + ww, 0:n_ch] = left.astype(BF16)
            act[d0:d0 + ww, n_ch:2 * n_ch] = a.astype(BF16)
            act[d0:d0 + ww, 2 * n_ch:3 * n_ch] = right.astype(BF16)

        def need(n):
            return min(self.hh, -(-(n + ww) // ww))

        n_pos = self.hh * ww
        for i in range(need(chunk)):
            fill(i)
        s1, s2 = _zero_sums(n_ch)
        for r0 in range(0, n_pos, chunk):
            lhs = jnp.concatenate([act[r0 + dy * ww:r0 + dy * ww + chunk, :] for dy in range(3)], axis=1)
            acc = _dot(self.w_t[j], lhs, ((1,), (1,)))
            for i in range(need(r0 + chunk), need(min(n_pos, r0 + 2 * chunk))):
                fill(i)
            out = epilogue(r0, acc.T)
            d1, d2 = _chan_sums(out.astype(F32))
            s1, s2 = s1 + d1, s2 + d2
        self.sums_s[0:1] = s1
        self.sums_s[1:2] = s2

    def run(self, src, sums, img, last_chunk, dst):
        hid, sums_s = self.hid, self.sums_s
        t_row = self.temb_s[pl.ds(img, 1), :]

        def first(r0, acc):
            out = (acc + t_row).astype(BF16)
            hid[r0:r0 + out.shape[0]] = out
            return out

        def second(r0, acc):
            out = (src(r0, acc.shape[0]).astype(F32) + acc).astype(BF16)
            dst(r0, out)
            return out

        self.conv(0, src, sums, CHUNK, first)

        @pl.when(img >= 0)
        def _():
            self.conv(1, lambda r0, n: hid[r0:r0 + n], (sums_s[0:1], sums_s[1:2]), last_chunk, second)


def _first_kernel(n_row, n_col, lat_ref, temb_hbm, rnorm_hbm, conv_hbm, wtemb_hbm, o_ref, sums_ref, next_w,
                  xv, wconv, w_t, temb_v, rnorm_v, wtemb, act, hid, temb_s, grp_s, sums_s, wsem, send_sem, recv_sem, loc_sem):
    me_r, me_c, peers = _me_and_peers(n_row, n_col)
    me = me_r * n_col + me_c
    n_img, hh, ww, n_ch = xv.shape
    bh, bw = hh // n_row, ww // n_col
    weights = [pltpu.make_async_copy(conv_hbm.at[i // 2, i % 2], wconv.at[i], wsem.at[i]) for i in range(4)]
    small = [
        pltpu.make_async_copy(wtemb_hbm.at[0], wtemb, wsem.at[4]),
        pltpu.make_async_copy(temb_hbm, temb_v, wsem.at[5]),
        pltpu.make_async_copy(rnorm_hbm, rnorm_v, wsem.at[6]),
    ]

    def place(s):
        return xv.at[s, pl.ds(me_r * bh, bh), pl.ds(pl.multiple_of(me_c * bw, bw), bw), :]

    def copy(s, k):
        r, c = peers[k]
        return pltpu.make_async_remote_copy(
            lat_ref.at[(r * n_col + c) * n_img + s], place(s), send_sem.at[s, k], recv_sem.at[s, k],
            device_id={'row': r, 'col': c}, device_id_type=MESH)

    def own(s):
        return pltpu.make_async_copy(lat_ref.at[me * n_img + s], place(s), loc_sem.at[s])

    _barrier(peers)
    for s in range(n_img):
        for k in range(len(peers)):
            copy(s, k).start()
        own(s).start()
    for w in [*small, *weights]:
        w.start()

    blk = _ResBlock(hh, ww, n_ch, rnorm_v.at[0], w_t, act, hid, temb_s, grp_s, sums_s)
    for w in small:
        w.wait()
    blk.setup(temb_v, wtemb)
    for w in weights:
        w.wait()

    def turn(i, carry):
        t0 = pl.multiple_of(i * n_ch, n_ch)
        for j in range(4):
            out = w_t.at[j] if j < 2 else next_w.at[j - 2]
            out[:, pl.ds(t0, n_ch)] = wconv[j, pl.ds(t0, n_ch), :].T
        return carry

    lax.fori_loop(0, 9, turn, 0)

    def image(s, carry):
        for k in range(len(peers)):
            copy(s, k).wait_recv()
        own(s).wait()

        def src(r0, n):
            return xv[s, pl.ds(r0 // ww, n // ww)].reshape(n, n_ch)

        def in_sums(i, sums):
            d1, d2 = _chan_sums(src(i * 4 * ww, 4 * ww).astype(F32))
            return sums[0] + d1, sums[1] + d2

        def dst(r0, v):
            o_ref[s, r0:r0 + v.shape[0]] = v

        sums = lax.fori_loop(0, hh // 4, in_sums, _zero_sums(n_ch))
        blk.run(src, sums, me * n_img + s, CHUNK, dst)
        sums_ref[s] = sums_s[...]
        return carry

    lax.fori_loop(0, n_img, image, 0)
    for s in range(n_img):
        for k in range(len(peers)):
            copy(s, k).wait_send()


def _last_kernel(n_row, n_col, x_ref, sums_ref, temb_ref, rnorm_ref, w_t, wtemb_ref, o_ref,
                 yv, act, hid, temb_s, grp_s, sums_s, send_sem, recv_sem, loc_sem):
    me_r, me_c, peers = _me_and_peers(n_row, n_col)
    me = me_r * n_col + me_c
    n_img, hh, ww, n_ch = yv.shape
    bh, bw = hh // n_row, ww // n_col
    blk = _ResBlock(hh, ww, n_ch, rnorm_ref.at[1], w_t, act, hid, temb_s, grp_s, sums_s)
    blk.setup(temb_ref, wtemb_ref.at[1])
    _barrier(peers)

    def block(s, k, c):
        return yv.at[s, pl.ds(k * bh, bh), pl.ds(pl.multiple_of(c * bw, bw), bw), :]

    def rel(k, c):
        return lax.rem(k - me_r + n_row, n_row) * n_col + lax.rem(c - me_c + n_col, n_col)

    def copy(s, k, c):
        return pltpu.make_async_remote_copy(
            block(s, k, c), o_ref.at[me * n_img + s], send_sem.at[s, rel(k, c)], recv_sem.at[s, rel(k, c)],
            device_id={'row': k, 'col': c}, device_id_type=MESH)

    def own(s):
        return pltpu.make_async_copy(block(s, me_r, me_c), o_ref.at[me * n_img + s], loc_sem.at[s])

    def image(s, carry):
        def src(r0, n):
            return x_ref[s, r0:r0 + n]

        def dst(r0, v):
            end = r0 + v.shape[0]
            while r0 < end:
                n = min(end, (r0 // ww + 1) * ww) - r0
                yv[s, r0 // ww, r0 % ww:r0 % ww + n] = v[v.shape[0] - (end - r0):v.shape[0] - (end - r0) + n]
                r0 += n
            for k in range((end - v.shape[0]) // (bh * ww), end // (bh * ww)):
                for d in range(n_col):
                    c = lax.rem(me_c + 1 + d, n_col)
                    remote = (k != me_r) | (c != me_c)

                    @pl.when(remote)
                    def _():
                        copy(s, k, c).start()

                    @pl.when(jnp.logical_not(remote))
                    def _():
                        own(s).start()

        blk.run(src, (sums_ref[s, 0:1], sums_ref[s, 1:2]), me * n_img + s, LAST_CHUNK, dst)
        return carry

    lax.fori_loop(0, n_img, image, 0)
    for s in range(n_img):
        for r, c in peers:
            copy(s, r, c).wait()
        own(s).wait()


def _attn_kernel(x_ref, sums_ref, anorm_ref, proj_ref, o_ref, osums_ref, grp_s, k_buf, q_buf, v_buf, ot_buf):
    n_img, n_pos, n_ch = x_ref.shape
    count = float(n_pos * (n_ch // GROUPS))
    head_dim = 32
    n_heads = n_ch // head_dim
    per_blk = 128 // head_dim
    scale = LOG2E * head_dim ** -0.5

    grp_s[...] = _group_matrix(n_ch)

    def image(img, carry_img):
        sums = sums_ref[img, 0:1], sums_ref[img, 1:2]
        mean, inv = _moments(*sums, grp_s[...], count)
        a_mul = inv * anorm_ref[0:1].astype(F32)
        b_add = anorm_ref[1:2].astype(F32)
        head_rows = jnp.where(lax.broadcasted_iota(jnp.int32, (16, n_ch), 0)
                              == lax.broadcasted_iota(jnp.int32, (16, n_ch), 1) // head_dim, 1.0, 0.0).astype(BF16)

        q_top = jnp.zeros((n_heads, PROJ_TILE), F32)
        k_top = jnp.zeros((16, PROJ_TILE), F32)
        v_top = jnp.zeros((1, PROJ_TILE), F32)
        last_k = None
        for r0 in [*range(0, n_pos, PROJ_TILE), None]:
            if r0 is not None:
                tile = slice(r0, r0 + PROJ_TILE)
                g = ((x_ref[img, tile].astype(F32) - mean) * a_mul + b_add).astype(BF16)
                k = _dot(g, proj_ref[1], ((1,), (1,))).astype(BF16)
                q = _dot(proj_ref[0], g, ((1,), (1,))).astype(BF16)
                v = _dot(proj_ref[2], g, ((1,), (1,))).astype(BF16)
                k_buf[tile, :] = k
                q_buf[:, tile] = q
                v_buf[:, tile] = v
                q = q.astype(F32)
                q_top = jnp.maximum(q_top, jnp.sum((q * q).reshape(n_heads, head_dim, PROJ_TILE), axis=1))
                v_top = jnp.maximum(v_top, jnp.max(jnp.abs(v.astype(F32)), axis=0, keepdims=True))
            if last_k is not None:
                k2 = last_k.astype(F32) * last_k.astype(F32)
                k_top = jnp.maximum(k_top, _dot(head_rows, k2.astype(BF16), ((1,), (1,))))
            last_k = k

        q_top = jnp.max(q_top, axis=1, keepdims=True)
        k_top = jnp.max(k_top, axis=1, keepdims=True)[:n_heads]
        top2 = jnp.max(q_top * k_top) * (scale * scale)
        v_max = jnp.max(v_top)
        small = ((top2 < 96.0 ** 2) & (v_max < 2.0 ** 20)) | ((top2 < 108.0 ** 2) & (v_max < 2.0 ** 8))

        @pl.when(small)
        def _():
            rh = lax.broadcasted_iota(jnp.int32, (128, Q_TILE), 0) // head_dim
            n_kc = n_pos // K_CHUNK

            def heads(b, carry):
                b0 = pl.multiple_of(b * 128, 128)
                tiles = [(j, t * Q_TILE) for j in range(per_blk) for t in range(n_pos // Q_TILE)]
                steps = [(tile, c) for tile in tiles for c in range(n_kc)]
                masked = {}

                def score(step):
                    tile, c = step
                    if tile not in masked:
                        j, q0 = tile
                        masked[tile] = jnp.where(rh == j, q_buf[pl.ds(b0, 128), q0:q0 + Q_TILE], 0)
                    return _dot(k_buf[c * K_CHUNK:(c + 1) * K_CHUNK, pl.ds(b0, 128)], masked[tile])

                pending = [score(s) for s in steps[:AHEAD]]
                tot = out = None
                for n, ((j, q0), c) in enumerate(steps):
                    if n + AHEAD < len(steps):
                        pending.append(score(steps[n + AHEAD]))
                    p = jnp.exp2(pending.pop(0) * scale)
                    h0 = pl.multiple_of(b0 + j * head_dim, head_dim)
                    part = jnp.sum(p.reshape(K_CHUNK // 8, 8, Q_TILE), axis=0)
                    pv = _dot(v_buf[pl.ds(h0, head_dim), c * K_CHUNK:(c + 1) * K_CHUNK], p.astype(BF16))
                    tot, out = (part, pv) if c == 0 else (tot + part, out + pv)
                    if c == n_kc - 1:
                        res = out / jnp.sum(tot, axis=0, keepdims=True)
                        ot_buf[pl.ds(h0, head_dim), q0:q0 + Q_TILE] = res.astype(BF16)
                return carry

            lax.fori_loop(0, n_ch // 128, heads, 0)

        @pl.when(jnp.logical_not(small))
        def _():
            rh = lax.broadcasted_iota(jnp.int32, (128, 256), 0) // head_dim
            n_tiles = n_pos // 256

            def tile(i, carry):
                h = i // n_tiles
                q0 = pl.multiple_of((i % n_tiles) * 256, 256)
                b0 = pl.multiple_of((h // per_blk) * 128, 128)
                h0 = pl.multiple_of(h * head_dim, head_dim)
                qm = jnp.where(rh == h % per_blk, q_buf[pl.ds(b0, 128), pl.ds(q0, 256)], 0)
                s = _dot(k_buf[:, pl.ds(b0, 128)], qm)
                p = jnp.exp2((s - jnp.max(s, axis=0, keepdims=True)) * scale)
                o = _dot(v_buf[pl.ds(h0, head_dim), :], p.astype(BF16))
                ot_buf[pl.ds(h0, head_dim), pl.ds(q0, 256)] = (o / jnp.sum(p, axis=0, keepdims=True)).astype(BF16)
                return carry

            lax.fori_loop(0, n_heads * n_tiles, tile, 0)

        s1, s2 = _zero_sums(n_ch)
        for r0 in range(0, n_pos, PROJ_TILE):
            tile = slice(r0, r0 + PROJ_TILE)
            acc = _dot(ot_buf[:, tile], proj_ref[3], ((0,), (0,)))
            out = (x_ref[img, tile].astype(F32) + acc).astype(BF16)
            o_ref[img, tile] = out
            d1, d2 = _chan_sums(out.astype(F32))
            s1, s2 = s1 + d1, s2 + d2
        osums_ref[img, 0:1] = s1
        osums_ref[img, 1:2] = s2
        return carry_img

    lax.fori_loop(0, n_img, image, 0)


VMEM_LIMIT = 60 * 1024 * 1024


def solution(mesh):
    n_row, n_col = mesh.shape['row'], mesh.shape['col']
    n_dev = n_row * n_col
    vmem, hbm = pl.BlockSpec(memory_space=pltpu.VMEM), pl.BlockSpec(memory_space=pltpu.HBM)

    def run_stage(latent, t_emb, res_norm, res_conv, res_temb, attn_norm, attn_proj):
        n_batch, bh, bw, n_ch = latent.shape
        hh, ww = bh * n_row, bw * n_col
        n_pos, n_img = hh * ww, n_batch // n_dev
        proj = jnp.transpose(attn_proj, (0, 1, 3, 2)).reshape(4, n_ch, n_ch)
        conv_w = res_conv.reshape(2, 2, 9 * n_ch, n_ch)
        sums_shape = jax.ShapeDtypeStruct((n_img, 8, n_ch), F32)
        images = pltpu.VMEM((n_img, hh, ww, n_ch), BF16)
        work = [
            pltpu.VMEM(((hh + 2) * ww, 3 * n_ch), BF16),
            pltpu.VMEM((n_pos, n_ch), BF16),
            pltpu.VMEM((n_batch, n_ch), F32),
            pltpu.VMEM((n_ch, n_ch), BF16),
            pltpu.VMEM((8, n_ch), F32),
        ]
        remote = [pltpu.SemaphoreType.DMA((n_img, n_dev)), pltpu.SemaphoreType.DMA((n_img, n_dev)),
                  pltpu.SemaphoreType.DMA((n_img,))]

        def resident(shape, dtype=BF16):
            return pltpu.VMEM(shape, dtype)

        x1, sums1, next_w = pl.pallas_call(
            functools.partial(_first_kernel, n_row, n_col),
            out_shape=[resident((n_img, n_pos, n_ch)), resident((n_img, 8, n_ch), F32), resident((2, n_ch, 9 * n_ch))],
            in_specs=[hbm] * 5,
            out_specs=[vmem, vmem, vmem],
            scratch_shapes=[
                images, pltpu.VMEM((4, 9 * n_ch, n_ch), BF16), pltpu.VMEM((2, n_ch, 9 * n_ch), BF16),
                pltpu.VMEM(t_emb.shape, BF16), pltpu.VMEM(res_norm.shape, BF16), pltpu.VMEM(res_temb.shape[1:], BF16),
                *work, pltpu.SemaphoreType.DMA((7,)), *remote,
            ],
            compiler_params=pltpu.CompilerParams(collective_id=0, has_side_effects=True, vmem_limit_bytes=42 << 20),
        )(*(pltpu.with_memory_space_constraint(a, pltpu.HBM) for a in (latent, t_emb, res_norm, conv_w, res_temb)))

        x2, sums2 = pl.pallas_call(
            _attn_kernel,
            out_shape=[resident((n_img, n_pos, n_ch)), resident((n_img, 8, n_ch), F32)],
            in_specs=[vmem, vmem, vmem, vmem],
            out_specs=[vmem, vmem],
            scratch_shapes=[
                pltpu.VMEM((n_ch, n_ch), BF16),
                pltpu.VMEM((n_pos, n_ch), BF16),
                pltpu.VMEM((n_ch, n_pos), BF16),
                pltpu.VMEM((n_ch, n_pos), BF16),
                pltpu.VMEM((n_ch, n_pos), BF16),
            ],
            compiler_params=pltpu.CompilerParams(vmem_limit_bytes=24 << 20),
        )(x1, sums1, attn_norm, proj)

        return pl.pallas_call(
            functools.partial(_last_kernel, n_row, n_col),
            out_shape=resident(latent.shape),
            in_specs=[vmem] * 6,
            out_specs=vmem,
            scratch_shapes=[images, *work, *remote],
            compiler_params=pltpu.CompilerParams(collective_id=1, has_side_effects=True, vmem_limit_bytes=24 << 20),
        )(x2, sums2, t_emb, res_norm, next_w, res_temb)

    spec_x = P('dp', 'row', 'col', None)
    return jax.shard_map(run_stage, mesh=mesh, in_specs=(spec_x, P('dp', None), P(), P(), P(), P(), P()), out_specs=spec_x, check_vma=False)
```

```python
import functools

import jax
import jax.numpy as jnp
from jax import lax
from jax.experimental import pallas as pl
from jax.experimental.pallas import tpu as pltpu
from jax.sharding import PartitionSpec as P

MESH = pl.DeviceIdType.MESH
GROUPS = 32
EPS = 1e-5
LOG2E = 1.4426950408889634
F32 = jnp.float32
BF16 = jnp.bfloat16
Q_TILE = 512
K_CHUNK = 256
AHEAD = 2
CHUNK = 768
LAST_CHUNK = 512
PROJ_TILE = 512


def _me_and_peers(n_row, n_col):
    me_r, me_c = lax.axis_index('row'), lax.axis_index('col')
    peers = []
    for k in range(1, n_row * n_col):
        peers.append((lax.rem(me_r + k // n_col, n_row), lax.rem(me_c + k % n_col, n_col)))
    return me_r, me_c, peers


def _barrier(peers):
    sem = pltpu.get_barrier_semaphore()
    for r, c in peers:
        pl.semaphore_signal(sem, inc=1, device_id={'row': r, 'col': c}, device_id_type=MESH)
    pl.semaphore_wait(sem, len(peers))


def _dot(a, b, dims=((1,), (0,))):
    return lax.dot_general(a, b, (dims, ((), ())), preferred_element_type=F32)


def _chan_sums(v):
    return jnp.sum(v, axis=0, keepdims=True), jnp.sum(v * v, axis=0, keepdims=True)


def _group_matrix(n_ch):
    per = n_ch // GROUPS
    gi = lax.broadcasted_iota(jnp.int32, (n_ch, n_ch), 0) // per
    gj = lax.broadcasted_iota(jnp.int32, (n_ch, n_ch), 1) // per
    return jnp.where(gi == gj, 1.0, 0.0).astype(BF16)


def _moments(s1, s2, grp, count):
    n_ch = s1.shape[1]
    st = jnp.concatenate([s1, s2, jnp.zeros((6, n_ch), F32)], axis=0)
    hi = st.astype(BF16)
    r1 = st - hi.astype(F32)
    mid = r1.astype(BF16)
    lo = (r1 - mid.astype(F32)).astype(BF16)
    parts = _dot(jnp.concatenate([hi.astype(F32), mid.astype(F32), lo.astype(F32)], axis=0).astype(BF16), grp)
    tot = (parts[16:24] + parts[8:16]) + parts[0:8]
    mean = tot[0:1] / count
    var = tot[1:2] / count - mean * mean
    return mean, lax.rsqrt(var + EPS)


def _zero_sums(n_ch):
    return jnp.zeros((1, n_ch), F32), jnp.zeros((1, n_ch), F32)


class _ResBlock:
    def __init__(self, hh, ww, n_ch, rnorm_ref, w_t, act, hid, temb_s, grp_s, sums_s):
        self.hh, self.ww, self.n_ch = hh, ww, n_ch
        self.rnorm_ref, self.w_t, self.act, self.hid = rnorm_ref, w_t, act, hid
        self.temb_s, self.grp_s, self.sums_s = temb_s, grp_s, sums_s
        self.count = float(hh * ww * (n_ch // GROUPS))

    def setup(self, temb_ref, wtemb_ref):
        te = temb_ref[...].astype(F32)
        t_act = (te * jax.nn.sigmoid(te)).astype(BF16)
        self.temb_s[...] = _dot(t_act, wtemb_ref[...])
        self.grp_s[...] = _group_matrix(self.n_ch)
        zeros = jnp.zeros((self.ww, self.act.shape[1]), BF16)
        self.act[0:self.ww, :] = zeros
        self.act[(self.hh + 1) * self.ww:(self.hh + 2) * self.ww, :] = zeros

    def conv(self, j, src, sums, chunk, epilogue, backward=False):
        ww, n_ch, act = self.ww, self.n_ch, self.act
        mean, inv = _moments(*sums, self.grp_s[...], self.count)
        a_mul = inv * self.rnorm_ref[j, 0:1].astype(F32)
        b_add = self.rnorm_ref[j, 1:2].astype(F32)
        col = lax.broadcasted_iota(jnp.int32, (ww, 1), 0)

        def fill(i):
            u = (src(i * ww, ww).astype(F32) - mean) * a_mul + b_add
            a = u * (0.5 * jnp.tanh(0.5 * u) + 0.5)
            left = jnp.where(col == 0, 0.0, pltpu.roll(a, 1, 0))
            right = jnp.where(col == ww - 1, 0.0, pltpu.roll(a, ww - 1, 0))
            d0 = (i + 1) * ww
            act[d0:d0 + ww, 0:n_ch] = left.astype(BF16)
            act[d0:d0 + ww, n_ch:2 * n_ch] = a.astype(BF16)
            act[d0:d0 + ww, 2 * n_ch:3 * n_ch] = right.astype(BF16)

        n_pos, filled = self.hh * ww, set()

        def fill_for(r0):
            for i in range(max(0, r0 // ww - 1), min(self.hh, (r0 + chunk - 1) // ww + 2)):
                if i not in filled:
                    filled.add(i)
                    fill(i)

        starts = list(range(0, n_pos, chunk))[::-1 if backward else 1]
        fill_for(starts[0])
        s1, s2 = _zero_sums(n_ch)
        for at, r0 in enumerate(starts):
            lhs = jnp.concatenate([act[r0 + dy * ww:r0 + dy * ww + chunk, :] for dy in range(3)], axis=1)
            acc = _dot(self.w_t[j], lhs, ((1,), (1,)))
            for ahead in starts[at + 1:at + 2]:
                fill_for(ahead)
            out = epilogue(r0, acc.T)
            d1, d2 = _chan_sums(out.astype(F32))
            s1, s2 = s1 + d1, s2 + d2
        self.sums_s[0:1] = s1
        self.sums_s[1:2] = s2

    def run(self, src, sums, img, last_chunk, dst, backward=None):
        hid, sums_s = self.hid, self.sums_s
        t_row = self.temb_s[pl.ds(img, 1), :]

        def first(r0, acc):
            out = (acc + t_row).astype(BF16)
            hid[r0:r0 + out.shape[0]] = out
            return out

        def second(r0, acc):
            out = (src(r0, acc.shape[0]).astype(F32) + acc).astype(BF16)
            dst(r0, out)
            return out

        self.conv(0, src, sums, CHUNK, first)

        def last(order):
            self.conv(1, lambda r0, n: hid[r0:r0 + n], (sums_s[0:1], sums_s[1:2]), last_chunk, second, order)

        if backward is None:
            pl.when(img >= 0)(lambda: last(False))
        else:
            pl.when(backward)(lambda: last(True))
            pl.when(jnp.logical_not(backward))(lambda: last(False))


def _first_kernel(n_row, n_col, lat_ref, temb_hbm, rnorm_hbm, conv_hbm, wtemb_hbm, o_ref, sums_ref, next_w,
                  xv, wconv, w_t, temb_v, rnorm_v, wtemb, act, hid, temb_s, grp_s, sums_s, wsem, send_sem, recv_sem, loc_sem):
    me_r, me_c, peers = _me_and_peers(n_row, n_col)
    me = me_r * n_col + me_c
    n_img, hh, ww, n_ch = xv.shape
    bh, bw = hh // n_row, ww // n_col
    weights = [pltpu.make_async_copy(conv_hbm.at[i // 2, i % 2], wconv.at[i], wsem.at[i]) for i in range(4)]
    small = [
        pltpu.make_async_copy(wtemb_hbm.at[0], wtemb, wsem.at[4]),
        pltpu.make_async_copy(temb_hbm, temb_v, wsem.at[5]),
        pltpu.make_async_copy(rnorm_hbm, rnorm_v, wsem.at[6]),
    ]

    def place(s):
        return xv.at[s, pl.ds(me_r * bh, bh), pl.ds(pl.multiple_of(me_c * bw, bw), bw), :]

    def copy(s, k):
        r, c = peers[k]
        return pltpu.make_async_remote_copy(
            lat_ref.at[(r * n_col + c) * n_img + s], place(s), send_sem.at[s, k], recv_sem.at[s, k],
            device_id={'row': r, 'col': c}, device_id_type=MESH)

    def own(s):
        return pltpu.make_async_copy(lat_ref.at[me * n_img + s], place(s), loc_sem.at[s])

    _barrier(peers)
    for s in range(n_img):
        for k in range(len(peers)):
            copy(s, k).start()
        own(s).start()
    for w in [*small, *weights]:
        w.start()

    blk = _ResBlock(hh, ww, n_ch, rnorm_v.at[0], w_t, act, hid, temb_s, grp_s, sums_s)
    for w in small:
        w.wait()
    blk.setup(temb_v, wtemb)
    for w in weights:
        w.wait()

    def turn(i, carry):
        t0 = pl.multiple_of(i * n_ch, n_ch)
        for j in range(4):
            out = w_t.at[j] if j < 2 else next_w.at[j - 2]
            out[:, pl.ds(t0, n_ch)] = wconv[j, pl.ds(t0, n_ch), :].T
        return carry

    lax.fori_loop(0, 9, turn, 0)

    def image(s, carry):
        for k in range(len(peers)):
            copy(s, k).wait_recv()
        own(s).wait()

        def src(r0, n):
            return xv[s, pl.ds(r0 // ww, n // ww)].reshape(n, n_ch)

        def in_sums(i, sums):
            d1, d2 = _chan_sums(src(i * 4 * ww, 4 * ww).astype(F32))
            return sums[0] + d1, sums[1] + d2

        def dst(r0, v):
            o_ref[s, r0:r0 + v.shape[0]] = v

        sums = lax.fori_loop(0, hh // 4, in_sums, _zero_sums(n_ch))
        blk.run(src, sums, me * n_img + s, CHUNK, dst)
        sums_ref[s] = sums_s[...]
        return carry

    lax.fori_loop(0, n_img, image, 0)
    for s in range(n_img):
        for k in range(len(peers)):
            copy(s, k).wait_send()


def _last_kernel(n_row, n_col, x_ref, sums_ref, temb_ref, rnorm_ref, w_t, wtemb_ref, o_ref,
                 yv, act, hid, temb_s, grp_s, sums_s, send_sem, recv_sem, loc_sem):
    me_r, me_c, peers = _me_and_peers(n_row, n_col)
    me = me_r * n_col + me_c
    n_img, hh, ww, n_ch = yv.shape
    bh, bw = hh // n_row, ww // n_col
    blk = _ResBlock(hh, ww, n_ch, rnorm_ref.at[1], w_t, act, hid, temb_s, grp_s, sums_s)
    blk.setup(temb_ref, wtemb_ref.at[1])
    _barrier(peers)

    def block(s, k, c):
        return yv.at[s, pl.ds(k * bh, bh), pl.ds(pl.multiple_of(c * bw, bw), bw), :]

    def rel(k, c):
        return lax.rem(k - me_r + n_row, n_row) * n_col + lax.rem(c - me_c + n_col, n_col)

    def copy(s, k, c):
        return pltpu.make_async_remote_copy(
            block(s, k, c), o_ref.at[me * n_img + s], send_sem.at[s, rel(k, c)], recv_sem.at[s, rel(k, c)],
            device_id={'row': k, 'col': c}, device_id_type=MESH)

    def own(s):
        return pltpu.make_async_copy(block(s, me_r, me_c), o_ref.at[me * n_img + s], loc_sem.at[s])

    def image(s, carry):
        def src(r0, n):
            return x_ref[s, r0:r0 + n]

        def ready(r0, end):
            size, blocks = bh * ww, []
            for k in range(n_row):
                if k * size < end and (k + 1) * size > r0:
                    done.setdefault(k, set()).update(range(max(r0, k * size), min(end, (k + 1) * size)))
                    if len(done[k]) == size:
                        done.pop(k)
                        blocks.append(k)
            return blocks

        done = {}

        def dst(r0, v):
            end, at = r0 + v.shape[0], r0
            while at < end:
                n = min(end, (at // ww + 1) * ww) - at
                yv[s, at // ww, at % ww:at % ww + n] = v[at - r0:at - r0 + n]
                at += n
            for k in ready(r0, end):
                for d in range(n_col):
                    c = lax.rem(me_c + 1 + d, n_col)
                    remote = (k != me_r) | (c != me_c)

                    @pl.when(remote)
                    def _():
                        copy(s, k, c).start()

                    @pl.when(jnp.logical_not(remote))
                    def _():
                        own(s).start()

        blk.run(src, (sums_ref[s, 0:1], sums_ref[s, 1:2]), me * n_img + s, LAST_CHUNK, dst, me_r < n_row // 2)
        return carry

    lax.fori_loop(0, n_img, image, 0)
    for s in range(n_img):
        for r, c in peers:
            copy(s, r, c).wait()
        own(s).wait()


def _attn_kernel(x_ref, sums_ref, anorm_ref, proj_ref, o_ref, osums_ref, grp_s, k_buf, q_buf, v_buf, ot_buf):
    n_img, n_pos, n_ch = x_ref.shape
    count = float(n_pos * (n_ch // GROUPS))
    head_dim = 32
    n_heads = n_ch // head_dim
    per_blk = 128 // head_dim
    scale = LOG2E * head_dim ** -0.5

    grp_s[...] = _group_matrix(n_ch)

    def image(img, carry_img):
        sums = sums_ref[img, 0:1], sums_ref[img, 1:2]
        mean, inv = _moments(*sums, grp_s[...], count)
        a_mul = inv * anorm_ref[0:1].astype(F32)
        b_add = anorm_ref[1:2].astype(F32)
        head_rows = jnp.where(lax.broadcasted_iota(jnp.int32, (16, n_ch), 0)
                              == lax.broadcasted_iota(jnp.int32, (16, n_ch), 1) // head_dim, 1.0, 0.0).astype(BF16)

        q_top = jnp.zeros((n_heads, PROJ_TILE), F32)
        k_top = jnp.zeros((16, PROJ_TILE), F32)
        v_top = jnp.zeros((1, PROJ_TILE), F32)
        last_k = None
        for r0 in [*range(0, n_pos, PROJ_TILE), None]:
            if r0 is not None:
                tile = slice(r0, r0 + PROJ_TILE)
                g = ((x_ref[img, tile].astype(F32) - mean) * a_mul + b_add).astype(BF16)
                k = _dot(g, proj_ref[1], ((1,), (1,))).astype(BF16)
                q = _dot(proj_ref[0], g, ((1,), (1,))).astype(BF16)
                v = _dot(proj_ref[2], g, ((1,), (1,))).astype(BF16)
                k_buf[tile, :] = k
                q_buf[:, tile] = q
                v_buf[:, tile] = v
                q = q.astype(F32)
                q_top = jnp.maximum(q_top, jnp.sum((q * q).reshape(n_heads, head_dim, PROJ_TILE), axis=1))
                v_top = jnp.maximum(v_top, jnp.max(jnp.abs(v.astype(F32)), axis=0, keepdims=True))
            if last_k is not None:
                k2 = last_k.astype(F32) * last_k.astype(F32)
                k_top = jnp.maximum(k_top, _dot(head_rows, k2.astype(BF16), ((1,), (1,))))
            last_k = k

        q_top = jnp.max(q_top, axis=1, keepdims=True)
        k_top = jnp.max(k_top, axis=1, keepdims=True)[:n_heads]
        top2 = jnp.max(q_top * k_top) * (scale * scale)
        v_max = jnp.max(v_top)
        small = ((top2 < 96.0 ** 2) & (v_max < 2.0 ** 20)) | ((top2 < 108.0 ** 2) & (v_max < 2.0 ** 8))

        @pl.when(small)
        def _():
            rh = lax.broadcasted_iota(jnp.int32, (128, Q_TILE), 0) // head_dim
            n_kc = n_pos // K_CHUNK

            def heads(b, carry):
                b0 = pl.multiple_of(b * 128, 128)
                tiles = [(j, t * Q_TILE) for j in range(per_blk) for t in range(n_pos // Q_TILE)]
                steps = [(tile, c) for tile in tiles for c in range(n_kc)]
                masked = {}

                def score(step):
                    tile, c = step
                    if tile not in masked:
                        j, q0 = tile
                        masked[tile] = jnp.where(rh == j, q_buf[pl.ds(b0, 128), q0:q0 + Q_TILE], 0)
                    return _dot(k_buf[c * K_CHUNK:(c + 1) * K_CHUNK, pl.ds(b0, 128)], masked[tile])

                pending = [score(s) for s in steps[:AHEAD]]
                tot = out = None
                for n, ((j, q0), c) in enumerate(steps):
                    if n + AHEAD < len(steps):
                        pending.append(score(steps[n + AHEAD]))
                    p = jnp.exp2(pending.pop(0) * scale)
                    h0 = pl.multiple_of(b0 + j * head_dim, head_dim)
                    part = jnp.sum(p.reshape(K_CHUNK // 8, 8, Q_TILE), axis=0)
                    pv = _dot(v_buf[pl.ds(h0, head_dim), c * K_CHUNK:(c + 1) * K_CHUNK], p.astype(BF16))
                    tot, out = (part, pv) if c == 0 else (tot + part, out + pv)
                    if c == n_kc - 1:
                        res = out / jnp.sum(tot, axis=0, keepdims=True)
                        ot_buf[pl.ds(h0, head_dim), q0:q0 + Q_TILE] = res.astype(BF16)
                return carry

            lax.fori_loop(0, n_ch // 128, heads, 0)

        @pl.when(jnp.logical_not(small))
        def _():
            rh = lax.broadcasted_iota(jnp.int32, (128, 256), 0) // head_dim
            n_tiles = n_pos // 256

            def tile(i, carry):
                h = i // n_tiles
                q0 = pl.multiple_of((i % n_tiles) * 256, 256)
                b0 = pl.multiple_of((h // per_blk) * 128, 128)
                h0 = pl.multiple_of(h * head_dim, head_dim)
                qm = jnp.where(rh == h % per_blk, q_buf[pl.ds(b0, 128), pl.ds(q0, 256)], 0)
                s = _dot(k_buf[:, pl.ds(b0, 128)], qm)
                p = jnp.exp2((s - jnp.max(s, axis=0, keepdims=True)) * scale)
                o = _dot(v_buf[pl.ds(h0, head_dim), :], p.astype(BF16))
                ot_buf[pl.ds(h0, head_dim), pl.ds(q0, 256)] = (o / jnp.sum(p, axis=0, keepdims=True)).astype(BF16)
                return carry

            lax.fori_loop(0, n_heads * n_tiles, tile, 0)

        s1, s2 = _zero_sums(n_ch)
        for r0 in range(0, n_pos, PROJ_TILE):
            tile = slice(r0, r0 + PROJ_TILE)
            acc = _dot(ot_buf[:, tile], proj_ref[3], ((0,), (0,)))
            out = (x_ref[img, tile].astype(F32) + acc).astype(BF16)
            o_ref[img, tile] = out
            d1, d2 = _chan_sums(out.astype(F32))
            s1, s2 = s1 + d1, s2 + d2
        osums_ref[img, 0:1] = s1
        osums_ref[img, 1:2] = s2
        return carry_img

    lax.fori_loop(0, n_img, image, 0)


VMEM_LIMIT = 60 * 1024 * 1024


def solution(mesh):
    n_row, n_col = mesh.shape['row'], mesh.shape['col']
    n_dev = n_row * n_col
    vmem, hbm = pl.BlockSpec(memory_space=pltpu.VMEM), pl.BlockSpec(memory_space=pltpu.HBM)

    def run_stage(latent, t_emb, res_norm, res_conv, res_temb, attn_norm, attn_proj):
        n_batch, bh, bw, n_ch = latent.shape
        hh, ww = bh * n_row, bw * n_col
        n_pos, n_img = hh * ww, n_batch // n_dev
        proj = jnp.transpose(attn_proj, (0, 1, 3, 2)).reshape(4, n_ch, n_ch)
        conv_w = res_conv.reshape(2, 2, 9 * n_ch, n_ch)
        sums_shape = jax.ShapeDtypeStruct((n_img, 8, n_ch), F32)
        images = pltpu.VMEM((n_img, hh, ww, n_ch), BF16)
        work = [
            pltpu.VMEM(((hh + 2) * ww, 3 * n_ch), BF16),
            pltpu.VMEM((n_pos, n_ch), BF16),
            pltpu.VMEM((n_batch, n_ch), F32),
            pltpu.VMEM((n_ch, n_ch), BF16),
            pltpu.VMEM((8, n_ch), F32),
        ]
        remote = [pltpu.SemaphoreType.DMA((n_img, n_dev)), pltpu.SemaphoreType.DMA((n_img, n_dev)),
                  pltpu.SemaphoreType.DMA((n_img,))]

        def resident(shape, dtype=BF16):
            return pltpu.VMEM(shape, dtype)

        x1, sums1, next_w = pl.pallas_call(
            functools.partial(_first_kernel, n_row, n_col),
            out_shape=[resident((n_img, n_pos, n_ch)), resident((n_img, 8, n_ch), F32), resident((2, n_ch, 9 * n_ch))],
            in_specs=[hbm] * 5,
            out_specs=[vmem, vmem, vmem],
            scratch_shapes=[
                images, pltpu.VMEM((4, 9 * n_ch, n_ch), BF16), pltpu.VMEM((2, n_ch, 9 * n_ch), BF16),
                pltpu.VMEM(t_emb.shape, BF16), pltpu.VMEM(res_norm.shape, BF16), pltpu.VMEM(res_temb.shape[1:], BF16),
                *work, pltpu.SemaphoreType.DMA((7,)), *remote,
            ],
            compiler_params=pltpu.CompilerParams(collective_id=0, has_side_effects=True, vmem_limit_bytes=42 << 20),
        )(*(pltpu.with_memory_space_constraint(a, pltpu.HBM) for a in (latent, t_emb, res_norm, conv_w, res_temb)))

        x2, sums2 = pl.pallas_call(
            _attn_kernel,
            out_shape=[resident((n_img, n_pos, n_ch)), resident((n_img, 8, n_ch), F32)],
            in_specs=[vmem, vmem, vmem, vmem],
            out_specs=[vmem, vmem],
            scratch_shapes=[
                pltpu.VMEM((n_ch, n_ch), BF16),
                pltpu.VMEM((n_pos, n_ch), BF16),
                pltpu.VMEM((n_ch, n_pos), BF16),
                pltpu.VMEM((n_ch, n_pos), BF16),
                pltpu.VMEM((n_ch, n_pos), BF16),
            ],
            compiler_params=pltpu.CompilerParams(vmem_limit_bytes=24 << 20),
        )(x1, sums1, attn_norm, proj)

        return pl.pallas_call(
            functools.partial(_last_kernel, n_row, n_col),
            out_shape=resident(latent.shape),
            in_specs=[vmem] * 6,
            out_specs=vmem,
            scratch_shapes=[images, *work, *remote],
            compiler_params=pltpu.CompilerParams(collective_id=1, has_side_effects=True, vmem_limit_bytes=24 << 20),
        )(x2, sums2, t_emb, res_norm, next_w, res_temb)

    spec_x = P('dp', 'row', 'col', None)
    return jax.shard_map(run_stage, mesh=mesh, in_specs=(spec_x, P('dp', None), P(), P(), P(), P(), P()), out_specs=spec_x, check_vma=False)
```

```python
import functools

import jax
import jax.numpy as jnp
from jax import lax
from jax.experimental import pallas as pl
from jax.experimental.pallas import tpu as pltpu
from jax.sharding import PartitionSpec as P

MESH = pl.DeviceIdType.MESH
GROUPS = 32
EPS = 1e-5
LOG2E = 1.4426950408889634
F32 = jnp.float32
BF16 = jnp.bfloat16
Q_TILE = 512
K_CHUNK = 256
AHEAD = 2
CHUNK = 768
LAST_CHUNK = 512
PROJ_TILE = 512


def _me_and_peers(n_row, n_col):
    me_r, me_c = lax.axis_index('row'), lax.axis_index('col')
    half = n_row // 2

    def other(r, far, core):
        r = lax.rem(r + far * half, n_row)
        return r // half * half + lax.rem(lax.rem(r, half) + core, half)

    order = [(f, k, c) for f, c in ((1, 1), (1, 0), (0, 1), (0, 0)) for k in range(half) if f or c or k]
    return me_r, me_c, [(other(me_r, f, k), lax.rem(me_c + c, n_col)) for f, k, c in order]


def _barrier(peers):
    sem = pltpu.get_barrier_semaphore()
    for r, c in peers:
        pl.semaphore_signal(sem, inc=1, device_id={'row': r, 'col': c}, device_id_type=MESH)
    pl.semaphore_wait(sem, len(peers))


def _dot(a, b, dims=((1,), (0,))):
    return lax.dot_general(a, b, (dims, ((), ())), preferred_element_type=F32)


def _chan_sums(v):
    return jnp.sum(v, axis=0, keepdims=True), jnp.sum(v * v, axis=0, keepdims=True)


def _group_matrix(n_ch):
    per = n_ch // GROUPS
    gi = lax.broadcasted_iota(jnp.int32, (n_ch, n_ch), 0) // per
    gj = lax.broadcasted_iota(jnp.int32, (n_ch, n_ch), 1) // per
    return jnp.where(gi == gj, 1.0, 0.0).astype(BF16)


def _moments(s1, s2, grp, count):
    n_ch = s1.shape[1]
    st = jnp.concatenate([s1, s2, jnp.zeros((6, n_ch), F32)], axis=0)
    hi = st.astype(BF16)
    r1 = st - hi.astype(F32)
    mid = r1.astype(BF16)
    lo = (r1 - mid.astype(F32)).astype(BF16)
    parts = _dot(jnp.concatenate([hi.astype(F32), mid.astype(F32), lo.astype(F32)], axis=0).astype(BF16), grp)
    tot = (parts[16:24] + parts[8:16]) + parts[0:8]
    mean = tot[0:1] / count
    var = tot[1:2] / count - mean * mean
    return mean, lax.rsqrt(var + EPS)


def _zero_sums(n_ch):
    return jnp.zeros((1, n_ch), F32), jnp.zeros((1, n_ch), F32)


class _ResBlock:
    def __init__(self, hh, ww, n_ch, rnorm_ref, w_t, act, hid, temb_s, grp_s, sums_s):
        self.hh, self.ww, self.n_ch = hh, ww, n_ch
        self.rnorm_ref, self.w_t, self.act, self.hid = rnorm_ref, w_t, act, hid
        self.temb_s, self.grp_s, self.sums_s = temb_s, grp_s, sums_s
        self.count = float(hh * ww * (n_ch // GROUPS))

    def setup(self, temb_ref, wtemb_ref):
        te = temb_ref[...].astype(F32)
        t_act = (te * jax.nn.sigmoid(te)).astype(BF16)
        self.temb_s[...] = _dot(t_act, wtemb_ref[...])
        self.grp_s[...] = _group_matrix(self.n_ch)
        zeros = jnp.zeros((self.ww, self.act.shape[1]), BF16)
        self.act[0:self.ww, :] = zeros
        self.act[(self.hh + 1) * self.ww:(self.hh + 2) * self.ww, :] = zeros

    def conv(self, j, src, sums, chunk, epilogue, backward=False):
        ww, n_ch, act = self.ww, self.n_ch, self.act
        mean, inv = _moments(*sums, self.grp_s[...], self.count)
        a_mul = inv * self.rnorm_ref[j, 0:1].astype(F32)
        half_b = 0.5 * (self.rnorm_ref[j, 1:2].astype(F32) - mean * a_mul)
        half_a = 0.5 * a_mul
        edge = jnp.zeros((1, n_ch), BF16)

        def fill(i):
            w = src(i * ww, ww).astype(F32) * half_a + half_b
            a = w * jnp.tanh(w) + w
            d0 = (i + 1) * ww
            act[d0:d0 + ww, 0:n_ch] = pltpu.roll(a, 1, 0).astype(BF16)
            act[d0:d0 + ww, n_ch:2 * n_ch] = a.astype(BF16)
            act[d0:d0 + ww, 2 * n_ch:3 * n_ch] = pltpu.roll(a, ww - 1, 0).astype(BF16)
            act[d0:d0 + 1, 0:n_ch] = edge
            act[d0 + ww - 1:d0 + ww, 2 * n_ch:3 * n_ch] = edge

        n_pos, filled = self.hh * ww, set()

        def fill_for(r0):
            for i in range(max(0, r0 // ww - 1), min(self.hh, (r0 + chunk - 1) // ww + 2)):
                if i not in filled:
                    filled.add(i)
                    fill(i)

        starts = list(range(0, n_pos, chunk))[::-1 if backward else 1]
        fill_for(starts[0])
        s1, s2 = _zero_sums(n_ch)
        for at, r0 in enumerate(starts):
            lhs = jnp.concatenate([act[r0 + dy * ww:r0 + dy * ww + chunk, :] for dy in range(3)], axis=1)
            acc = _dot(self.w_t[j], lhs, ((1,), (1,)))
            for ahead in starts[at + 1:at + 2]:
                fill_for(ahead)
            out = epilogue(r0, acc.T)
            d1, d2 = _chan_sums(out.astype(F32))
            s1, s2 = s1 + d1, s2 + d2
        self.sums_s[0:1] = s1
        self.sums_s[1:2] = s2

    def run(self, src, sums, img, last_chunk, dst, backward=None):
        hid, sums_s = self.hid, self.sums_s
        t_row = self.temb_s[pl.ds(img, 1), :]

        def first(r0, acc):
            out = (acc + t_row).astype(BF16)
            hid[r0:r0 + out.shape[0]] = out
            return out

        def second(r0, acc):
            out = (src(r0, acc.shape[0]).astype(F32) + acc).astype(BF16)
            dst(r0, out)
            return out

        self.conv(0, src, sums, CHUNK, first)

        def last(order):
            self.conv(1, lambda r0, n: hid[r0:r0 + n], (sums_s[0:1], sums_s[1:2]), last_chunk, second, order)

        if backward is None:
            pl.when(img >= 0)(lambda: last(False))
        else:
            pl.when(backward)(lambda: last(True))
            pl.when(jnp.logical_not(backward))(lambda: last(False))


def _first_kernel(n_row, n_col, lat_ref, temb_hbm, rnorm_hbm, conv_hbm, wtemb_hbm, o_ref, sums_ref, next_w,
                  xv, wconv, w_t, temb_v, rnorm_v, wtemb, act, hid, temb_s, grp_s, sums_s, wsem, send_sem, recv_sem, loc_sem):
    me_r, me_c, peers = _me_and_peers(n_row, n_col)
    me = me_r * n_col + me_c
    n_img, hh, ww, n_ch = xv.shape
    bh, bw = hh // n_row, ww // n_col
    weights = [pltpu.make_async_copy(conv_hbm.at[i // 2, i % 2], wconv.at[i], wsem.at[i]) for i in range(4)]
    small = [
        pltpu.make_async_copy(wtemb_hbm.at[0], wtemb, wsem.at[4]),
        pltpu.make_async_copy(temb_hbm, temb_v, wsem.at[5]),
        pltpu.make_async_copy(rnorm_hbm, rnorm_v, wsem.at[6]),
    ]

    def place(s):
        return xv.at[s, pl.ds(me_r * bh, bh), pl.ds(pl.multiple_of(me_c * bw, bw), bw), :]

    def copy(s, k):
        r, c = peers[k]
        return pltpu.make_async_remote_copy(
            lat_ref.at[(r * n_col + c) * n_img + s], place(s), send_sem.at[s, k], recv_sem.at[s, k],
            device_id={'row': r, 'col': c}, device_id_type=MESH)

    def own(s):
        return pltpu.make_async_copy(lat_ref.at[me * n_img + s], place(s), loc_sem.at[s])

    _barrier(peers)
    for s in range(n_img):
        for k in range(len(peers)):
            copy(s, k).start()
        own(s).start()
    for w in [*small, *weights]:
        w.start()

    blk = _ResBlock(hh, ww, n_ch, rnorm_v.at[0], w_t, act, hid, temb_s, grp_s, sums_s)
    for w in small:
        w.wait()
    blk.setup(temb_v, wtemb)
    for w in weights:
        w.wait()

    def turn(i, carry):
        t0 = pl.multiple_of(i * n_ch, n_ch)
        for j in range(4):
            out = w_t.at[j] if j < 2 else next_w.at[j - 2]
            out[:, pl.ds(t0, n_ch)] = wconv[j, pl.ds(t0, n_ch), :].T
        return carry

    lax.fori_loop(0, 9, turn, 0)

    def image(s, carry):
        for k in range(len(peers)):
            copy(s, k).wait_recv()
        own(s).wait()

        def src(r0, n):
            return xv[s, pl.ds(r0 // ww, n // ww)].reshape(n, n_ch)

        def in_sums(i, sums):
            d1, d2 = _chan_sums(src(i * 4 * ww, 4 * ww).astype(F32))
            return sums[0] + d1, sums[1] + d2

        def dst(r0, v):
            o_ref[s, r0:r0 + v.shape[0]] = v

        sums = lax.fori_loop(0, hh // 4, in_sums, _zero_sums(n_ch))
        blk.run(src, sums, me * n_img + s, CHUNK, dst)
        sums_ref[s] = sums_s[...]
        return carry

    lax.fori_loop(0, n_img, image, 0)
    for s in range(n_img):
        for k in range(len(peers)):
            copy(s, k).wait_send()


def _last_kernel(n_row, n_col, x_ref, sums_ref, temb_ref, rnorm_ref, w_t, wtemb_ref, o_ref,
                 yv, act, hid, temb_s, grp_s, sums_s, send_sem, recv_sem, loc_sem):
    me_r, me_c, peers = _me_and_peers(n_row, n_col)
    me = me_r * n_col + me_c
    n_img, hh, ww, n_ch = yv.shape
    bh, bw = hh // n_row, ww // n_col
    blk = _ResBlock(hh, ww, n_ch, rnorm_ref.at[1], w_t, act, hid, temb_s, grp_s, sums_s)
    blk.setup(temb_ref, wtemb_ref.at[1])
    _barrier(peers)

    def block(s, k, c):
        return yv.at[s, pl.ds(k * bh, bh), pl.ds(pl.multiple_of(c * bw, bw), bw), :]

    def rel(k, c):
        return lax.rem(k - me_r + n_row, n_row) * n_col + lax.rem(c - me_c + n_col, n_col)

    def copy(s, k, c):
        return pltpu.make_async_remote_copy(
            block(s, k, c), o_ref.at[me * n_img + s], send_sem.at[s, rel(k, c)], recv_sem.at[s, rel(k, c)],
            device_id={'row': k, 'col': c}, device_id_type=MESH)

    def own(s):
        return pltpu.make_async_copy(block(s, me_r, me_c), o_ref.at[me * n_img + s], loc_sem.at[s])

    def image(s, carry):
        def src(r0, n):
            return x_ref[s, r0:r0 + n]

        def ready(r0, end):
            size, blocks = bh * ww, []
            for k in range(n_row):
                if k * size < end and (k + 1) * size > r0:
                    done.setdefault(k, set()).update(range(max(r0, k * size), min(end, (k + 1) * size)))
                    if len(done[k]) == size:
                        done.pop(k)
                        blocks.append(k)
            return blocks

        done = {}

        def dst(r0, v):
            end, at = r0 + v.shape[0], r0
            while at < end:
                n = min(end, (at // ww + 1) * ww) - at
                yv[s, at // ww, at % ww:at % ww + n] = v[at - r0:at - r0 + n]
                at += n
            for k in ready(r0, end):
                for d in range(n_col):
                    c = lax.rem(me_c + 1 + d, n_col)
                    remote = (k != me_r) | (c != me_c)

                    @pl.when(remote)
                    def _():
                        copy(s, k, c).start()

                    @pl.when(jnp.logical_not(remote))
                    def _():
                        own(s).start()

        blk.run(src, (sums_ref[s, 0:1], sums_ref[s, 1:2]), me * n_img + s, LAST_CHUNK, dst, me_r < n_row // 2)
        return carry

    lax.fori_loop(0, n_img, image, 0)
    for s in range(n_img):
        for r, c in peers:
            copy(s, r, c).wait()
        own(s).wait()


def _attn_kernel(x_ref, sums_ref, anorm_ref, proj_ref, o_ref, osums_ref, grp_s, k_buf, q_buf, v_buf, ot_buf):
    n_img, n_pos, n_ch = x_ref.shape
    count = float(n_pos * (n_ch // GROUPS))
    head_dim = 32
    n_heads = n_ch // head_dim
    per_blk = 128 // head_dim
    scale = LOG2E * head_dim ** -0.5

    grp_s[...] = _group_matrix(n_ch)

    def image(img, carry_img):
        sums = sums_ref[img, 0:1], sums_ref[img, 1:2]
        mean, inv = _moments(*sums, grp_s[...], count)
        a_mul = inv * anorm_ref[0:1].astype(F32)
        b_add = anorm_ref[1:2].astype(F32)
        head_rows = jnp.where(lax.broadcasted_iota(jnp.int32, (16, n_ch), 0)
                              == lax.broadcasted_iota(jnp.int32, (16, n_ch), 1) // head_dim, 1.0, 0.0).astype(BF16)

        q_top = jnp.zeros((n_heads, PROJ_TILE), F32)
        k_top = jnp.zeros((16, PROJ_TILE), F32)
        v_top = jnp.zeros((1, PROJ_TILE), F32)
        last_k = None
        for r0 in [*range(0, n_pos, PROJ_TILE), None]:
            if r0 is not None:
                tile = slice(r0, r0 + PROJ_TILE)
                g = ((x_ref[img, tile].astype(F32) - mean) * a_mul + b_add).astype(BF16)
                k = _dot(g, proj_ref[1], ((1,), (1,)))
                q = _dot(proj_ref[0], g, ((1,), (1,))).astype(BF16)
                v = _dot(proj_ref[2], g, ((1,), (1,))).astype(BF16)
                for b0 in range(0, n_ch, 128):
                    for j in range(per_blk):
                        part = k[:, b0:b0 + 128]
                        part = part if j == 0 else pltpu.roll(part, 128 - j * head_dim, 1)
                        k_buf[j, tile, b0:b0 + 128] = part.astype(BF16)
                k = k.astype(BF16)
                q_buf[:, tile] = q
                v_buf[:, tile] = v
                q = q.astype(F32)
                q_top = jnp.maximum(q_top, jnp.sum((q * q).reshape(n_heads, head_dim, PROJ_TILE), axis=1))
                v_top = jnp.maximum(v_top, jnp.max(jnp.abs(v.astype(F32)), axis=0, keepdims=True))
            if last_k is not None:
                k2 = last_k.astype(F32) * last_k.astype(F32)
                k_top = jnp.maximum(k_top, _dot(head_rows, k2.astype(BF16), ((1,), (1,))))
            last_k = k

        q_top = jnp.max(q_top, axis=1, keepdims=True)
        k_top = jnp.max(k_top, axis=1, keepdims=True)[:n_heads]
        top2 = jnp.max(q_top * k_top) * (scale * scale)
        v_max = jnp.max(v_top)
        small = ((top2 < 96.0 ** 2) & (v_max < 2.0 ** 20)) | ((top2 < 108.0 ** 2) & (v_max < 2.0 ** 8))

        @pl.when(small)
        def _():
            n_kc = n_pos // K_CHUNK

            def heads(b, carry):
                b0 = pl.multiple_of(b * 128, 128)
                tiles = [(j, t * Q_TILE) for j in range(per_blk) for t in range(n_pos // Q_TILE)]
                steps = [(tile, c) for tile in tiles for c in range(n_kc)]

                def score(step):
                    (j, q0), c = step
                    h0 = pl.multiple_of(b0 + j * head_dim, head_dim)
                    keys = k_buf[j, c * K_CHUNK:(c + 1) * K_CHUNK, pl.ds(b0, 128)]
                    return _dot(keys[:, :head_dim], q_buf[pl.ds(h0, head_dim), q0:q0 + Q_TILE])

                pending = [score(s) for s in steps[:AHEAD]]
                tot = out = None
                for n, ((j, q0), c) in enumerate(steps):
                    if n + AHEAD < len(steps):
                        pending.append(score(steps[n + AHEAD]))
                    p = jnp.exp2(pending.pop(0) * scale)
                    h0 = pl.multiple_of(b0 + j * head_dim, head_dim)
                    part = jnp.sum(p.reshape(K_CHUNK // 8, 8, Q_TILE), axis=0)
                    pv = _dot(v_buf[pl.ds(h0, head_dim), c * K_CHUNK:(c + 1) * K_CHUNK], p.astype(BF16))
                    tot, out = (part, pv) if c == 0 else (tot + part, out + pv)
                    if c == n_kc - 1:
                        res = out / jnp.sum(tot, axis=0, keepdims=True)
                        ot_buf[pl.ds(h0, head_dim), q0:q0 + Q_TILE] = res.astype(BF16)
                return carry

            lax.fori_loop(0, n_ch // 128, heads, 0)

        @pl.when(jnp.logical_not(small))
        def _():
            rh = lax.broadcasted_iota(jnp.int32, (128, 256), 0) // head_dim
            n_tiles = n_pos // 256

            def tile(i, carry):
                h = i // n_tiles
                q0 = pl.multiple_of((i % n_tiles) * 256, 256)
                b0 = pl.multiple_of((h // per_blk) * 128, 128)
                h0 = pl.multiple_of(h * head_dim, head_dim)
                qm = jnp.where(rh == h % per_blk, q_buf[pl.ds(b0, 128), pl.ds(q0, 256)], 0)
                s = _dot(k_buf[0, :, pl.ds(b0, 128)], qm)
                p = jnp.exp2((s - jnp.max(s, axis=0, keepdims=True)) * scale)
                o = _dot(v_buf[pl.ds(h0, head_dim), :], p.astype(BF16))
                ot_buf[pl.ds(h0, head_dim), pl.ds(q0, 256)] = (o / jnp.sum(p, axis=0, keepdims=True)).astype(BF16)
                return carry

            lax.fori_loop(0, n_heads * n_tiles, tile, 0)

        s1, s2 = _zero_sums(n_ch)
        for r0 in range(0, n_pos, PROJ_TILE):
            tile = slice(r0, r0 + PROJ_TILE)
            acc = _dot(ot_buf[:, tile], proj_ref[3], ((0,), (0,)))
            out = (x_ref[img, tile].astype(F32) + acc).astype(BF16)
            o_ref[img, tile] = out
            d1, d2 = _chan_sums(out.astype(F32))
            s1, s2 = s1 + d1, s2 + d2
        osums_ref[img, 0:1] = s1
        osums_ref[img, 1:2] = s2
        return carry_img

    lax.fori_loop(0, n_img, image, 0)


VMEM_LIMIT = 60 * 1024 * 1024


def solution(mesh):
    n_row, n_col = mesh.shape['row'], mesh.shape['col']
    n_dev = n_row * n_col
    vmem, hbm = pl.BlockSpec(memory_space=pltpu.VMEM), pl.BlockSpec(memory_space=pltpu.HBM)

    def run_stage(latent, t_emb, res_norm, res_conv, res_temb, attn_norm, attn_proj):
        n_batch, bh, bw, n_ch = latent.shape
        hh, ww = bh * n_row, bw * n_col
        n_pos, n_img = hh * ww, n_batch // n_dev
        proj = jnp.transpose(attn_proj, (0, 1, 3, 2)).reshape(4, n_ch, n_ch)
        conv_w = res_conv.reshape(2, 2, 9 * n_ch, n_ch)
        sums_shape = jax.ShapeDtypeStruct((n_img, 8, n_ch), F32)
        images = pltpu.VMEM((n_img, hh, ww, n_ch), BF16)
        work = [
            pltpu.VMEM(((hh + 2) * ww, 3 * n_ch), BF16),
            pltpu.VMEM((n_pos, n_ch), BF16),
            pltpu.VMEM((n_batch, n_ch), F32),
            pltpu.VMEM((n_ch, n_ch), BF16),
            pltpu.VMEM((8, n_ch), F32),
        ]
        remote = [pltpu.SemaphoreType.DMA((n_img, n_dev)), pltpu.SemaphoreType.DMA((n_img, n_dev)),
                  pltpu.SemaphoreType.DMA((n_img,))]

        def resident(shape, dtype=BF16):
            return pltpu.VMEM(shape, dtype)

        x1, sums1, next_w = pl.pallas_call(
            functools.partial(_first_kernel, n_row, n_col),
            out_shape=[resident((n_img, n_pos, n_ch)), resident((n_img, 8, n_ch), F32), resident((2, n_ch, 9 * n_ch))],
            in_specs=[hbm] * 5,
            out_specs=[vmem, vmem, vmem],
            scratch_shapes=[
                images, pltpu.VMEM((4, 9 * n_ch, n_ch), BF16), pltpu.VMEM((2, n_ch, 9 * n_ch), BF16),
                pltpu.VMEM(t_emb.shape, BF16), pltpu.VMEM(res_norm.shape, BF16), pltpu.VMEM(res_temb.shape[1:], BF16),
                *work, pltpu.SemaphoreType.DMA((7,)), *remote,
            ],
            compiler_params=pltpu.CompilerParams(collective_id=0, has_side_effects=True, vmem_limit_bytes=42 << 20),
        )(*(pltpu.with_memory_space_constraint(a, pltpu.HBM) for a in (latent, t_emb, res_norm, conv_w, res_temb)))

        x2, sums2 = pl.pallas_call(
            _attn_kernel,
            out_shape=[resident((n_img, n_pos, n_ch)), resident((n_img, 8, n_ch), F32)],
            in_specs=[vmem, vmem, vmem, vmem],
            out_specs=[vmem, vmem],
            scratch_shapes=[
                pltpu.VMEM((n_ch, n_ch), BF16),
                pltpu.VMEM((4, n_pos, n_ch), BF16),
                pltpu.VMEM((n_ch, n_pos), BF16),
                pltpu.VMEM((n_ch, n_pos), BF16),
                pltpu.VMEM((n_ch, n_pos), BF16),
            ],
            compiler_params=pltpu.CompilerParams(vmem_limit_bytes=24 << 20),
        )(x1, sums1, attn_norm, proj)

        return pl.pallas_call(
            functools.partial(_last_kernel, n_row, n_col),
            out_shape=resident(latent.shape),
            in_specs=[vmem] * 6,
            out_specs=vmem,
            scratch_shapes=[images, *work, *remote],
            compiler_params=pltpu.CompilerParams(collective_id=1, has_side_effects=True, vmem_limit_bytes=24 << 20),
        )(x2, sums2, t_emb, res_norm, next_w, res_temb)

    spec_x = P('dp', 'row', 'col', None)
    return jax.shard_map(run_stage, mesh=mesh, in_specs=(spec_x, P('dp', None), P(), P(), P(), P(), P()), out_specs=spec_x, check_vma=False)
```

```python
import functools

import jax
import jax.numpy as jnp
from jax import lax
from jax.experimental import pallas as pl
from jax.experimental.pallas import tpu as pltpu
from jax.sharding import PartitionSpec as P

MESH = pl.DeviceIdType.MESH
GROUPS = 32
EPS = 1e-5
LOG2E = 1.4426950408889634
F32 = jnp.float32
BF16 = jnp.bfloat16
Q_TILE = 512
K_CHUNK = 256
AHEAD = 2
CHUNK = 768
LAST_CHUNK = 512
PROJ_TILE = 512


def _me_and_peers(n_row, n_col):
    me_r, me_c = lax.axis_index('row'), lax.axis_index('col')
    half = n_row // 2

    def other(r, far, core):
        r = lax.rem(r + far * half, n_row)
        return r // half * half + lax.rem(lax.rem(r, half) + core, half)

    order = [(f, k, c) for f, c in ((1, 1), (1, 0), (0, 1), (0, 0)) for k in range(half) if f or c or k]
    return me_r, me_c, [(other(me_r, f, k), lax.rem(me_c + c, n_col)) for f, k, c in order]


def _barrier(peers):
    sem = pltpu.get_barrier_semaphore()
    for r, c in peers:
        pl.semaphore_signal(sem, inc=1, device_id={'row': r, 'col': c}, device_id_type=MESH)
    pl.semaphore_wait(sem, len(peers))


def _dot(a, b, dims=((1,), (0,))):
    return lax.dot_general(a, b, (dims, ((), ())), preferred_element_type=F32)


def _chan_sums(v):
    return jnp.sum(v, axis=0, keepdims=True), jnp.sum(v * v, axis=0, keepdims=True)


def _group_matrix(n_ch):
    per = n_ch // GROUPS
    gi = lax.broadcasted_iota(jnp.int32, (n_ch, n_ch), 0) // per
    gj = lax.broadcasted_iota(jnp.int32, (n_ch, n_ch), 1) // per
    return jnp.where(gi == gj, 1.0, 0.0).astype(BF16)


def _moments(s1, s2, grp, count):
    n_ch = s1.shape[1]
    st = jnp.concatenate([s1, s2, jnp.zeros((6, n_ch), F32)], axis=0)
    hi = st.astype(BF16)
    r1 = st - hi.astype(F32)
    mid = r1.astype(BF16)
    lo = (r1 - mid.astype(F32)).astype(BF16)
    parts = _dot(jnp.concatenate([hi.astype(F32), mid.astype(F32), lo.astype(F32)], axis=0).astype(BF16), grp)
    tot = (parts[16:24] + parts[8:16]) + parts[0:8]
    mean = tot[0:1] / count
    var = tot[1:2] / count - mean * mean
    return mean, lax.rsqrt(var + EPS)


def _zero_sums(n_ch):
    return jnp.zeros((1, n_ch), F32), jnp.zeros((1, n_ch), F32)


class _ResBlock:
    def __init__(self, hh, ww, n_ch, rnorm_ref, w_t, act, hid, temb_s, grp_s, sums_s):
        self.hh, self.ww, self.n_ch = hh, ww, n_ch
        self.rnorm_ref, self.w_t, self.act, self.hid = rnorm_ref, w_t, act, hid
        self.temb_s, self.grp_s, self.sums_s = temb_s, grp_s, sums_s
        self.count = float(hh * ww * (n_ch // GROUPS))

    def clear_borders(self):
        zeros = jnp.zeros((self.ww, self.act.shape[1]), BF16)
        self.act[0:self.ww, :] = zeros
        self.act[(self.hh + 1) * self.ww:(self.hh + 2) * self.ww, :] = zeros

    def conv(self, j, src, sums, chunk, epilogue, backward=False):
        ww, n_ch, act = self.ww, self.n_ch, self.act
        mean, inv = _moments(*sums, self.grp_s[...], self.count)
        a_mul = inv * self.rnorm_ref[j, 0:1].astype(F32)
        half_b = 0.5 * (self.rnorm_ref[j, 1:2].astype(F32) - mean * a_mul)
        half_a = 0.5 * a_mul
        edge = jnp.zeros((1, n_ch), BF16)

        def fill(i):
            w = src(i * ww, ww).astype(F32) * half_a + half_b
            a = w * jnp.tanh(w) + w
            d0 = (i + 1) * ww
            act[d0:d0 + ww, 0:n_ch] = pltpu.roll(a, 1, 0).astype(BF16)
            act[d0:d0 + ww, n_ch:2 * n_ch] = a.astype(BF16)
            act[d0:d0 + ww, 2 * n_ch:3 * n_ch] = pltpu.roll(a, ww - 1, 0).astype(BF16)
            act[d0:d0 + 1, 0:n_ch] = edge
            act[d0 + ww - 1:d0 + ww, 2 * n_ch:3 * n_ch] = edge

        n_pos, filled = self.hh * ww, set()

        def fill_for(r0):
            for i in range(max(0, r0 // ww - 1), min(self.hh, (r0 + chunk - 1) // ww + 2)):
                if i not in filled:
                    filled.add(i)
                    fill(i)

        starts = list(range(0, n_pos, chunk))[::-1 if backward else 1]
        fill_for(starts[0])
        s1, s2 = _zero_sums(n_ch)
        for at, r0 in enumerate(starts):
            lhs = jnp.concatenate([act[r0 + dy * ww:r0 + dy * ww + chunk, :] for dy in range(3)], axis=1)
            acc = _dot(self.w_t[j], lhs, ((1,), (1,)))
            for ahead in starts[at + 1:at + 2]:
                fill_for(ahead)
            out = epilogue(r0, acc.T)
            d1, d2 = _chan_sums(out.astype(F32))
            s1, s2 = s1 + d1, s2 + d2
        self.sums_s[0:1] = s1
        self.sums_s[1:2] = s2

    def run(self, src, sums, img, last_chunk, dst, backward):
        hid, sums_s = self.hid, self.sums_s
        t_row = self.temb_s[pl.ds(img, 1), :]

        def first(r0, acc):
            out = (acc + t_row).astype(BF16)
            hid[r0:r0 + out.shape[0]] = out
            return out

        def second(r0, acc):
            out = (src(r0, acc.shape[0]).astype(F32) + acc).astype(BF16)
            dst(r0, out)
            return out

        self.conv(0, src, sums, CHUNK, first)

        def last(order):
            self.conv(1, lambda r0, n: hid[r0:r0 + n], (sums_s[0:1], sums_s[1:2]), last_chunk, second, order)

        pl.when(backward)(lambda: last(True))
        pl.when(jnp.logical_not(backward))(lambda: last(False))


HEAD_DIM = 32
LOGIT_SCALE = LOG2E * HEAD_DIM ** -0.5


def _project(src, n_pos, sums, grp, anorm_ref, proj_ref, k_buf, q_buf, v_buf, bound_ref):
    n_ch = proj_ref.shape[-1]
    n_heads = n_ch // HEAD_DIM
    mean, inv = _moments(*sums, grp, float(n_pos * (n_ch // GROUPS)))
    a_mul = inv * anorm_ref[0:1].astype(F32)
    b_add = anorm_ref[1:2].astype(F32)
    head_rows = jnp.where(lax.broadcasted_iota(jnp.int32, (16, n_ch), 0)
                          == lax.broadcasted_iota(jnp.int32, (16, n_ch), 1) // HEAD_DIM, 1.0, 0.0).astype(BF16)
    q_top = jnp.zeros((n_heads, PROJ_TILE), F32)
    k_top = jnp.zeros((16, PROJ_TILE), F32)
    v_top = jnp.zeros((1, PROJ_TILE), F32)
    last_k = None
    for r0 in [*range(0, n_pos, PROJ_TILE), None]:
        if r0 is not None:
            tile = slice(r0, r0 + PROJ_TILE)
            g = ((src(r0, PROJ_TILE).astype(F32) - mean) * a_mul + b_add).astype(BF16)
            k = _dot(g, proj_ref[1], ((1,), (1,)))
            q = _dot(proj_ref[0], g, ((1,), (1,))).astype(BF16)
            v = _dot(proj_ref[2], g, ((1,), (1,))).astype(BF16)
            for b0 in range(0, n_ch, 128):
                for j in range(128 // HEAD_DIM):
                    part = k[:, b0:b0 + 128]
                    part = part if j == 0 else pltpu.roll(part, 128 - j * HEAD_DIM, 1)
                    k_buf[j, tile, b0:b0 + 128] = part.astype(BF16)
            k = k.astype(BF16)
            q_buf[:, tile] = q
            v_buf[:, tile] = v
            q = q.astype(F32)
            q_top = jnp.maximum(q_top, jnp.sum((q * q).reshape(n_heads, HEAD_DIM, PROJ_TILE), axis=1))
            v_top = jnp.maximum(v_top, jnp.max(jnp.abs(v.astype(F32)), axis=0, keepdims=True))
        if last_k is not None:
            k2 = last_k.astype(F32) * last_k.astype(F32)
            k_top = jnp.maximum(k_top, _dot(head_rows, k2.astype(BF16), ((1,), (1,))))
        last_k = k
    q_top = jnp.max(q_top, axis=1, keepdims=True)
    k_top = jnp.max(k_top, axis=1, keepdims=True)[:n_heads]
    top2 = jnp.max(q_top * k_top, axis=0, keepdims=True) * (LOGIT_SCALE * LOGIT_SCALE)
    bound_ref[0:1] = jnp.broadcast_to(top2, (1, 128))
    bound_ref[1:2] = jnp.broadcast_to(jnp.max(v_top, axis=1, keepdims=True), (1, 128))


def _first_kernel(n_row, n_col, lat_ref, temb_hbm, rnorm_hbm, conv_hbm, wtemb_hbm, anorm_hbm, proj_hbm,
                  o_ref, sums_ref, next_w, next_temb, grp_ref, k_buf, q_buf, v_buf, bound_ref,
                  xv, wconv, w_t, temb_v, rnorm_v, wtemb, anorm_v, proj_v, act, temb_s, sums_s,
                  wsem, send_sem, recv_sem, loc_sem):
    me_r, me_c, peers = _me_and_peers(n_row, n_col)
    me = me_r * n_col + me_c
    n_img, hh, ww, n_ch = xv.shape
    n_pos = hh * ww
    bh, bw = hh // n_row, ww // n_col
    weights = [pltpu.make_async_copy(conv_hbm.at[i // 2, i % 2], wconv.at[i], wsem.at[i]) for i in range(4)]
    small = [pltpu.make_async_copy(a, b, wsem.at[4 + i]) for i, (a, b) in enumerate([
        (wtemb_hbm, wtemb), (temb_hbm, temb_v), (rnorm_hbm, rnorm_v), (anorm_hbm, anorm_v), (proj_hbm, proj_v)])]

    def place(s):
        return xv.at[s, pl.ds(me_r * bh, bh), pl.ds(pl.multiple_of(me_c * bw, bw), bw), :]

    def copy(s, k):
        r, c = peers[k]
        return pltpu.make_async_remote_copy(
            lat_ref.at[(r * n_col + c) * n_img + s], place(s), send_sem.at[s, k], recv_sem.at[s, k],
            device_id={'row': r, 'col': c}, device_id_type=MESH)

    def own(s):
        return pltpu.make_async_copy(lat_ref.at[me * n_img + s], place(s), loc_sem.at[s])

    _barrier(peers)
    for s in range(n_img):
        for k in range(len(peers)):
            copy(s, k).start()
        own(s).start()
    for w in [*small, *weights]:
        w.start()

    blk = _ResBlock(hh, ww, n_ch, rnorm_v.at[0], w_t, act, None, temb_s, grp_ref, sums_s)
    blk.clear_borders()
    grp_ref[...] = _group_matrix(n_ch)
    for w in small:
        w.wait()
    te = temb_v[...].astype(F32)
    t_act = (te * jax.nn.sigmoid(te)).astype(BF16)
    temb_s[...] = _dot(t_act, wtemb[0])
    next_temb[...] = _dot(t_act, wtemb[1])
    for w in weights:
        w.wait()

    def turn(i, carry):
        t0 = pl.multiple_of(i * n_ch, n_ch)
        for j in range(4):
            out = w_t.at[j] if j < 2 else next_w.at[j - 2]
            out[:, pl.ds(t0, n_ch)] = wconv[j, pl.ds(t0, n_ch), :].T
        return carry

    lax.fori_loop(0, 9, turn, 0)

    def half_block(t, carry):
        s, j = t // 2, lax.rem(t, 2)

        @pl.when(t == 2)
        def _():
            _project(lambda r0, n: o_ref[0, r0:r0 + n], n_pos, (sums_ref[0, 0:1], sums_ref[0, 1:2]), grp_ref[...],
                     anorm_v, proj_v, k_buf, q_buf, v_buf, bound_ref)

        @pl.when(j == 0)
        def _():
            for k in range(len(peers)):
                copy(s, k).wait_recv()
            own(s).wait()

            def take(i, sums):
                v = xv[s, pl.ds(i * 4, 4)].reshape(4 * ww, n_ch)
                o_ref[s, pl.ds(pl.multiple_of(i * 4 * ww, 4 * ww), 4 * ww)] = v
                d1, d2 = _chan_sums(v.astype(F32))
                return sums[0] + d1, sums[1] + d2

            s1, s2 = lax.fori_loop(0, hh // 4, take, _zero_sums(n_ch))
            sums_s[0:1] = s1
            sums_s[1:2] = s2

        t_row = temb_s[pl.ds(me * n_img + s, 1), :]

        def epilogue(r0, acc):
            n = acc.shape[0]
            x = xv[s, r0 // ww:(r0 + n) // ww].reshape(n, n_ch).astype(F32)
            out = (acc + jnp.where(j == 0, t_row, x)).astype(BF16)
            o_ref[s, r0:r0 + n] = out
            return out

        blk.conv(j, lambda r0, n: o_ref[s, r0:r0 + n], (sums_s[0:1], sums_s[1:2]), CHUNK, epilogue)
        sums_ref[s] = sums_s[...]
        return carry

    lax.fori_loop(0, 2 * n_img, half_block, 0)
    for s in range(n_img):
        for k in range(len(peers)):
            copy(s, k).wait_send()


def _last_kernel(n_row, n_col, x_ref, sums_ref, rnorm_ref, w_t, temb_ref, grp_ref, o_ref,
                 yv, act, hid, sums_s, send_sem, recv_sem, loc_sem):
    me_r, me_c, peers = _me_and_peers(n_row, n_col)
    me = me_r * n_col + me_c
    n_img, hh, ww, n_ch = yv.shape
    bh, bw = hh // n_row, ww // n_col
    blk = _ResBlock(hh, ww, n_ch, rnorm_ref.at[1], w_t, act, hid, temb_ref, grp_ref, sums_s)
    blk.clear_borders()
    _barrier(peers)

    def block(s, k, c):
        return yv.at[s, pl.ds(k * bh, bh), pl.ds(pl.multiple_of(c * bw, bw), bw), :]

    def rel(k, c):
        return lax.rem(k - me_r + n_row, n_row) * n_col + lax.rem(c - me_c + n_col, n_col)

    def copy(s, k, c):
        return pltpu.make_async_remote_copy(
            block(s, k, c), o_ref.at[me * n_img + s], send_sem.at[s, rel(k, c)], recv_sem.at[s, rel(k, c)],
            device_id={'row': k, 'col': c}, device_id_type=MESH)

    def own(s):
        return pltpu.make_async_copy(block(s, me_r, me_c), o_ref.at[me * n_img + s], loc_sem.at[s])

    def image(s, carry):
        def src(r0, n):
            return x_ref[s, r0:r0 + n]

        def ready(r0, end):
            size, blocks = bh * ww, []
            for k in range(n_row):
                if k * size < end and (k + 1) * size > r0:
                    done.setdefault(k, set()).update(range(max(r0, k * size), min(end, (k + 1) * size)))
                    if len(done[k]) == size:
                        done.pop(k)
                        blocks.append(k)
            return blocks

        done = {}

        def dst(r0, v):
            end, at = r0 + v.shape[0], r0
            while at < end:
                n = min(end, (at // ww + 1) * ww) - at
                yv[s, at // ww, at % ww:at % ww + n] = v[at - r0:at - r0 + n]
                at += n
            for k in ready(r0, end):
                for d in range(n_col):
                    c = lax.rem(me_c + 1 + d, n_col)
                    remote = (k != me_r) | (c != me_c)

                    @pl.when(remote)
                    def _():
                        copy(s, k, c).start()

                    @pl.when(jnp.logical_not(remote))
                    def _():
                        own(s).start()

        blk.run(src, (sums_ref[s, 0:1], sums_ref[s, 1:2]), me * n_img + s, LAST_CHUNK, dst, me_r < n_row // 2)
        return carry

    lax.fori_loop(0, n_img, image, 0)
    for s in range(n_img):
        for r, c in peers:
            copy(s, r, c).wait()
        own(s).wait()


def _attn_kernel(x_ref, sums_ref, anorm_ref, proj_ref, grp_ref, k_in, q_in, v_in, bound_in,
                 o_ref, osums_ref, k_buf, q_buf, v_buf, bound_ref, ot_buf):
    n_img, n_pos, n_ch = x_ref.shape
    head_dim, scale = HEAD_DIM, LOGIT_SCALE
    n_heads = n_ch // head_dim
    per_blk = 128 // head_dim

    def image(img, carry_img):
        @pl.when(img > 0)
        def _():
            _project(lambda r0, n: x_ref[img, r0:r0 + n], n_pos, (sums_ref[img, 0:1], sums_ref[img, 1:2]),
                     grp_ref[...], anorm_ref, proj_ref, k_buf, q_buf, v_buf, bound_ref)

        top2, v_max = jnp.max(bound_ref[0:1]), jnp.max(bound_ref[1:2])
        small = ((top2 < 96.0 ** 2) & (v_max < 2.0 ** 20)) | ((top2 < 108.0 ** 2) & (v_max < 2.0 ** 8))

        @pl.when(small)
        def _():
            n_kc = n_pos // K_CHUNK

            def heads(b, carry):
                b0 = pl.multiple_of(b * 128, 128)
                tiles = [(j, t * Q_TILE) for j in range(per_blk) for t in range(n_pos // Q_TILE)]
                steps = [(tile, c) for tile in tiles for c in range(n_kc)]

                def score(step):
                    (j, q0), c = step
                    h0 = pl.multiple_of(b0 + j * head_dim, head_dim)
                    keys = k_buf[j, c * K_CHUNK:(c + 1) * K_CHUNK, pl.ds(b0, 128)]
                    return _dot(keys[:, :head_dim], q_buf[pl.ds(h0, head_dim), q0:q0 + Q_TILE])

                pending = [score(s) for s in steps[:AHEAD]]
                tot = out = None
                for n, ((j, q0), c) in enumerate(steps):
                    if n + AHEAD < len(steps):
                        pending.append(score(steps[n + AHEAD]))
                    p = jnp.exp2(pending.pop(0) * scale)
                    h0 = pl.multiple_of(b0 + j * head_dim, head_dim)
                    part = jnp.sum(p.reshape(K_CHUNK // 8, 8, Q_TILE), axis=0)
                    pv = _dot(v_buf[pl.ds(h0, head_dim), c * K_CHUNK:(c + 1) * K_CHUNK], p.astype(BF16))
                    tot, out = (part, pv) if c == 0 else (tot + part, out + pv)
                    if c == n_kc - 1:
                        res = out / jnp.sum(tot, axis=0, keepdims=True)
                        ot_buf[pl.ds(h0, head_dim), q0:q0 + Q_TILE] = res.astype(BF16)
                return carry

            lax.fori_loop(0, n_ch // 128, heads, 0)

        @pl.when(jnp.logical_not(small))
        def _():
            rh = lax.broadcasted_iota(jnp.int32, (128, 256), 0) // head_dim
            n_tiles = n_pos // 256

            def tile(i, carry):
                h = i // n_tiles
                q0 = pl.multiple_of((i % n_tiles) * 256, 256)
                b0 = pl.multiple_of((h // per_blk) * 128, 128)
                h0 = pl.multiple_of(h * head_dim, head_dim)
                qm = jnp.where(rh == h % per_blk, q_buf[pl.ds(b0, 128), pl.ds(q0, 256)], 0)
                s = _dot(k_buf[0, :, pl.ds(b0, 128)], qm)
                p = jnp.exp2((s - jnp.max(s, axis=0, keepdims=True)) * scale)
                o = _dot(v_buf[pl.ds(h0, head_dim), :], p.astype(BF16))
                ot_buf[pl.ds(h0, head_dim), pl.ds(q0, 256)] = (o / jnp.sum(p, axis=0, keepdims=True)).astype(BF16)
                return carry

            lax.fori_loop(0, n_heads * n_tiles, tile, 0)

        s1, s2 = _zero_sums(n_ch)
        for r0 in range(0, n_pos, PROJ_TILE):
            tile = slice(r0, r0 + PROJ_TILE)
            acc = _dot(ot_buf[:, tile], proj_ref[3], ((0,), (0,)))
            out = (x_ref[img, tile].astype(F32) + acc).astype(BF16)
            o_ref[img, tile] = out
            d1, d2 = _chan_sums(out.astype(F32))
            s1, s2 = s1 + d1, s2 + d2
        osums_ref[img, 0:1] = s1
        osums_ref[img, 1:2] = s2
        return carry_img

    lax.fori_loop(0, n_img, image, 0)


K1_LIMIT, K2_LIMIT, K3_LIMIT = 36, 16, 24


def solution(mesh):
    n_row, n_col = mesh.shape['row'], mesh.shape['col']
    n_dev = n_row * n_col
    vmem, hbm = pl.BlockSpec(memory_space=pltpu.VMEM), pl.BlockSpec(memory_space=pltpu.HBM)

    def run_stage(latent, t_emb, res_norm, res_conv, res_temb, attn_norm, attn_proj):
        n_batch, bh, bw, n_ch = latent.shape
        hh, ww = bh * n_row, bw * n_col
        n_pos, n_img = hh * ww, n_batch // n_dev
        proj = jnp.transpose(attn_proj, (0, 1, 3, 2)).reshape(4, n_ch, n_ch)
        conv_w = res_conv.reshape(2, 2, 9 * n_ch, n_ch)
        images = pltpu.VMEM((n_img, hh, ww, n_ch), BF16)
        act = pltpu.VMEM(((hh + 2) * ww, 3 * n_ch), BF16)
        chan_sums = pltpu.VMEM((8, n_ch), F32)
        remote = [pltpu.SemaphoreType.DMA((n_img, n_dev)), pltpu.SemaphoreType.DMA((n_img, n_dev)),
                  pltpu.SemaphoreType.DMA((n_img,))]
        x_out, sums_out = pltpu.VMEM((n_img, n_pos, n_ch), BF16), pltpu.VMEM((n_img, 8, n_ch), F32)
        qkv_out = [pltpu.VMEM((128 // HEAD_DIM, n_pos, n_ch), BF16), pltpu.VMEM((n_ch, n_pos), BF16),
                   pltpu.VMEM((n_ch, n_pos), BF16), pltpu.VMEM((8, 128), F32)]

        from_hbm = (latent, t_emb, res_norm, conv_w, res_temb, attn_norm, proj)
        x1, sums1, next_w, next_temb, grp, *qkv = pl.pallas_call(
            functools.partial(_first_kernel, n_row, n_col),
            out_shape=[x_out, sums_out, pltpu.VMEM((2, n_ch, 9 * n_ch), BF16), pltpu.VMEM((n_batch, n_ch), F32),
                       pltpu.VMEM((n_ch, n_ch), BF16), *qkv_out],
            in_specs=[hbm] * len(from_hbm),
            out_specs=[vmem] * 9,
            scratch_shapes=[
                images, pltpu.VMEM((4, 9 * n_ch, n_ch), BF16), pltpu.VMEM((2, n_ch, 9 * n_ch), BF16),
                *(pltpu.VMEM(a.shape, BF16) for a in (t_emb, res_norm, res_temb, attn_norm, proj)),
                act, pltpu.VMEM((n_batch, n_ch), F32), chan_sums, pltpu.SemaphoreType.DMA((9,)), *remote,
            ],
            compiler_params=pltpu.CompilerParams(collective_id=0, has_side_effects=True, vmem_limit_bytes=K1_LIMIT << 20),
        )(*(pltpu.with_memory_space_constraint(a, pltpu.HBM) for a in from_hbm))

        x2, sums2, *_ = pl.pallas_call(
            _attn_kernel,
            out_shape=[x_out, sums_out, *qkv_out],
            in_specs=[vmem] * 9,
            out_specs=[vmem] * 6,
            input_output_aliases={5: 2, 6: 3, 7: 4, 8: 5},
            scratch_shapes=[pltpu.VMEM((n_ch, n_pos), BF16)],
            compiler_params=pltpu.CompilerParams(vmem_limit_bytes=K2_LIMIT << 20),
        )(x1, sums1, attn_norm, proj, grp, *qkv)

        return pl.pallas_call(
            functools.partial(_last_kernel, n_row, n_col),
            out_shape=pltpu.VMEM(latent.shape, BF16),
            in_specs=[vmem] * 6,
            out_specs=vmem,
            scratch_shapes=[images, act, pltpu.VMEM((n_pos, n_ch), BF16), chan_sums, *remote],
            compiler_params=pltpu.CompilerParams(collective_id=1, has_side_effects=True, vmem_limit_bytes=K3_LIMIT << 20),
        )(x2, sums2, res_norm, next_w, next_temb, grp)

    spec_x = P('dp', 'row', 'col', None)
    return jax.shard_map(run_stage, mesh=mesh, in_specs=(spec_x, P('dp', None), P(), P(), P(), P(), P()), out_specs=spec_x, check_vma=False)
```

```python
import functools

import jax
import jax.numpy as jnp
from jax import lax
from jax.experimental import pallas as pl
from jax.experimental.pallas import tpu as pltpu
from jax.sharding import PartitionSpec as P

MESH = pl.DeviceIdType.MESH
GROUPS = 32
EPS = 1e-5
LOG2E = 1.4426950408889634
F32 = jnp.float32
BF16 = jnp.bfloat16
Q_TILE = 512
K_CHUNK = 256
AHEAD = 2
CHUNK = 768
LAST_CHUNK = 512
PROJ_TILE = 512


def _me_and_peers(n_row, n_col):
    me_r, me_c = lax.axis_index('row'), lax.axis_index('col')
    half = n_row // 2

    def other(r, far, core):
        r = lax.rem(r + far * half, n_row)
        return r // half * half + lax.rem(lax.rem(r, half) + core, half)

    order = [(f, k, c) for f, c in ((1, 1), (1, 0), (0, 1), (0, 0)) for k in range(half) if f or c or k]
    return me_r, me_c, [(other(me_r, f, k), lax.rem(me_c + c, n_col)) for f, k, c in order]


def _barrier(peers):
    sem = pltpu.get_barrier_semaphore()
    for r, c in peers:
        pl.semaphore_signal(sem, inc=1, device_id={'row': r, 'col': c}, device_id_type=MESH)
    pl.semaphore_wait(sem, len(peers))


def _dot(a, b, dims=((1,), (0,))):
    return lax.dot_general(a, b, (dims, ((), ())), preferred_element_type=F32)


def _chan_sums(v):
    return jnp.sum(v, axis=0, keepdims=True), jnp.sum(v * v, axis=0, keepdims=True)


def _group_matrix(n_ch):
    per = n_ch // GROUPS
    gi = lax.broadcasted_iota(jnp.int32, (n_ch, n_ch), 0) // per
    gj = lax.broadcasted_iota(jnp.int32, (n_ch, n_ch), 1) // per
    return jnp.where(gi == gj, 1.0, 0.0).astype(BF16)


def _moments(s1, s2, grp, count):
    n_ch = s1.shape[1]
    st = jnp.concatenate([s1, s2, jnp.zeros((6, n_ch), F32)], axis=0)
    hi = st.astype(BF16)
    r1 = st - hi.astype(F32)
    mid = r1.astype(BF16)
    lo = (r1 - mid.astype(F32)).astype(BF16)
    parts = _dot(jnp.concatenate([hi.astype(F32), mid.astype(F32), lo.astype(F32)], axis=0).astype(BF16), grp)
    tot = (parts[16:24] + parts[8:16]) + parts[0:8]
    mean = tot[0:1] / count
    var = tot[1:2] / count - mean * mean
    return mean, lax.rsqrt(var + EPS)


def _zero_sums(n_ch):
    return jnp.zeros((1, n_ch), F32), jnp.zeros((1, n_ch), F32)


class _ResBlock:
    def __init__(self, hh, ww, n_ch, rnorm_ref, w_t, act, hid, temb_s, grp_s, sums_s):
        self.hh, self.ww, self.n_ch = hh, ww, n_ch
        self.rnorm_ref, self.w_t, self.act, self.hid = rnorm_ref, w_t, act, hid
        self.temb_s, self.grp_s, self.sums_s = temb_s, grp_s, sums_s
        self.count = float(hh * ww * (n_ch // GROUPS))

    def clear_borders(self):
        zeros = jnp.zeros((self.ww, self.act.shape[1]), BF16)
        self.act[0:self.ww, :] = zeros
        self.act[(self.hh + 1) * self.ww:(self.hh + 2) * self.ww, :] = zeros

    def conv(self, j, src, sums, chunk, epilogue, backward=False):
        ww, n_ch, act = self.ww, self.n_ch, self.act
        mean, inv = _moments(*sums, self.grp_s[...], self.count)
        a_mul = inv * self.rnorm_ref[j, 0:1].astype(F32)
        half_b = 0.5 * (self.rnorm_ref[j, 1:2].astype(F32) - mean * a_mul)
        half_a = 0.5 * a_mul
        edge = jnp.zeros((1, n_ch), BF16)

        def fill(i):
            w = src(i * ww, ww).astype(F32) * half_a + half_b
            a = w * jnp.tanh(w) + w
            d0 = (i + 1) * ww
            act[d0:d0 + ww, 0:n_ch] = pltpu.roll(a, 1, 0).astype(BF16)
            act[d0:d0 + ww, n_ch:2 * n_ch] = a.astype(BF16)
            act[d0:d0 + ww, 2 * n_ch:3 * n_ch] = pltpu.roll(a, ww - 1, 0).astype(BF16)
            act[d0:d0 + 1, 0:n_ch] = edge
            act[d0 + ww - 1:d0 + ww, 2 * n_ch:3 * n_ch] = edge

        n_pos, filled = self.hh * ww, set()

        def fill_for(r0):
            for i in range(max(0, r0 // ww - 1), min(self.hh, (r0 + chunk - 1) // ww + 2)):
                if i not in filled:
                    filled.add(i)
                    fill(i)

        starts = list(range(0, n_pos, chunk))[::-1 if backward else 1]
        fill_for(starts[0])
        s1, s2 = _zero_sums(n_ch)
        for at, r0 in enumerate(starts):
            lhs = jnp.concatenate([act[r0 + dy * ww:r0 + dy * ww + chunk, :] for dy in range(3)], axis=1)
            acc = _dot(self.w_t[j], lhs, ((1,), (1,)))
            for ahead in starts[at + 1:at + 2]:
                fill_for(ahead)
            out = epilogue(r0, acc.T)
            d1, d2 = _chan_sums(out.astype(F32))
            s1, s2 = s1 + d1, s2 + d2
        self.sums_s[0:1] = s1
        self.sums_s[1:2] = s2

    def run(self, src, sums, img, last_chunk, dst, backward):
        hid, sums_s = self.hid, self.sums_s
        t_row = self.temb_s[pl.ds(img, 1), :]

        def first(r0, acc):
            out = (acc + t_row).astype(BF16)
            hid[r0:r0 + out.shape[0]] = out
            return out

        def second(r0, acc):
            out = (src(r0, acc.shape[0]).astype(F32) + acc).astype(BF16)
            dst(r0, out)
            return out

        self.conv(0, src, sums, CHUNK, first)

        def last(order):
            self.conv(1, lambda r0, n: hid[r0:r0 + n], (sums_s[0:1], sums_s[1:2]), last_chunk, second, order)

        pl.when(backward)(lambda: last(True))
        pl.when(jnp.logical_not(backward))(lambda: last(False))


HEAD_DIM = 32
LOGIT_SCALE = LOG2E * HEAD_DIM ** -0.5


def _project(src, n_pos, sums, grp, anorm_ref, proj_ref, k_buf, q_buf, v_buf, bound_ref):
    n_ch = proj_ref.shape[-1]
    n_heads = n_ch // HEAD_DIM
    mean, inv = _moments(*sums, grp, float(n_pos * (n_ch // GROUPS)))
    a_mul = inv * anorm_ref[0:1].astype(F32)
    b_add = anorm_ref[1:2].astype(F32)
    head_rows = jnp.where(lax.broadcasted_iota(jnp.int32, (16, n_ch), 0)
                          == lax.broadcasted_iota(jnp.int32, (16, n_ch), 1) // HEAD_DIM, 1.0, 0.0).astype(BF16)
    q_top = jnp.zeros((n_heads, PROJ_TILE), F32)
    k_top = jnp.zeros((16, PROJ_TILE), F32)
    v_top = jnp.zeros((1, PROJ_TILE), F32)
    last_k = None
    for r0 in [*range(0, n_pos, PROJ_TILE), None]:
        if r0 is not None:
            tile = slice(r0, r0 + PROJ_TILE)
            g = ((src(r0, PROJ_TILE).astype(F32) - mean) * a_mul + b_add).astype(BF16)
            k = _dot(g, proj_ref[1], ((1,), (1,)))
            q = _dot(proj_ref[0], g, ((1,), (1,))).astype(BF16)
            v = _dot(proj_ref[2], g, ((1,), (1,))).astype(BF16)
            for b0 in range(0, n_ch, 128):
                for j in range(128 // HEAD_DIM):
                    part = k[:, b0:b0 + 128]
                    part = part if j == 0 else pltpu.roll(part, 128 - j * HEAD_DIM, 1)
                    k_buf[j, tile, b0:b0 + 128] = part.astype(BF16)
            k = k.astype(BF16)
            q_buf[:, tile] = q
            v_buf[:, tile] = v
            q = q.astype(F32)
            q_top = jnp.maximum(q_top, jnp.sum((q * q).reshape(n_heads, HEAD_DIM, PROJ_TILE), axis=1))
            v_top = jnp.maximum(v_top, jnp.max(jnp.abs(v.astype(F32)), axis=0, keepdims=True))
        if last_k is not None:
            k2 = last_k.astype(F32) * last_k.astype(F32)
            k_top = jnp.maximum(k_top, _dot(head_rows, k2.astype(BF16), ((1,), (1,))))
        last_k = k
    q_top = jnp.max(q_top, axis=1, keepdims=True)
    k_top = jnp.max(k_top, axis=1, keepdims=True)[:n_heads]
    top2 = jnp.max(q_top * k_top, axis=0, keepdims=True) * (LOGIT_SCALE * LOGIT_SCALE)
    bound_ref[0:1] = jnp.broadcast_to(top2, (1, 128))
    bound_ref[1:2] = jnp.broadcast_to(jnp.max(v_top, axis=1, keepdims=True), (1, 128))


def _first_kernel(n_row, n_col, lat_ref, temb_hbm, rnorm_hbm, conv_hbm, wtemb_hbm, anorm_hbm, proj_hbm,
                  o_ref, sums_ref, next_w, next_temb, grp_ref, k_buf, q_buf, v_buf, bound_ref,
                  xv, wconv, w_t, temb_v, rnorm_v, wtemb, anorm_v, proj_v, act, temb_s, sums_s,
                  wsem, send_sem, recv_sem, loc_sem):
    me_r, me_c, peers = _me_and_peers(n_row, n_col)
    me = me_r * n_col + me_c
    n_img, hh, ww, n_ch = xv.shape
    n_pos = hh * ww
    bh, bw = hh // n_row, ww // n_col
    weights = [pltpu.make_async_copy(conv_hbm.at[i // 2, i % 2], wconv.at[i], wsem.at[i]) for i in range(4)]
    small = [pltpu.make_async_copy(a, b, wsem.at[4 + i]) for i, (a, b) in enumerate([
        (wtemb_hbm, wtemb), (temb_hbm, temb_v), (rnorm_hbm, rnorm_v), (anorm_hbm, anorm_v), (proj_hbm, proj_v)])]

    def place(s):
        return xv.at[s, pl.ds(me_r * bh, bh), pl.ds(pl.multiple_of(me_c * bw, bw), bw), :]

    def copy(s, k):
        r, c = peers[k]
        return pltpu.make_async_remote_copy(
            lat_ref.at[(r * n_col + c) * n_img + s], place(s), send_sem.at[s, k], recv_sem.at[s, k],
            device_id={'row': r, 'col': c}, device_id_type=MESH)

    def own(s):
        return pltpu.make_async_copy(lat_ref.at[me * n_img + s], place(s), loc_sem.at[s])

    _barrier(peers)
    for k in range(len(peers)):
        copy(0, k).start()
    for s in range(n_img):
        own(s).start()
    for w in [*small, *weights]:
        w.start()

    blk = _ResBlock(hh, ww, n_ch, rnorm_v.at[0], w_t, act, None, temb_s, grp_ref, sums_s)
    blk.clear_borders()
    grp_ref[...] = _group_matrix(n_ch)
    for w in small:
        w.wait()
    te = temb_v[...].astype(F32)
    t_act = (te * jax.nn.sigmoid(te)).astype(BF16)
    temb_s[...] = _dot(t_act, wtemb[0])
    next_temb[...] = _dot(t_act, wtemb[1])
    for w in weights:
        w.wait()

    def turn(i, carry):
        t0 = pl.multiple_of(i * n_ch, n_ch)
        for j in range(4):
            out = w_t.at[j] if j < 2 else next_w.at[j - 2]
            out[:, pl.ds(t0, n_ch)] = wconv[j, pl.ds(t0, n_ch), :].T
        return carry

    lax.fori_loop(0, 9, turn, 0)
    for s in range(1, n_img):
        for k in range(len(peers)):
            copy(s - 1, k).wait_send()
            copy(s, k).start()

    def half_block(t, carry):
        s, j = t // 2, lax.rem(t, 2)

        @pl.when(t == 2)
        def _():
            _project(lambda r0, n: o_ref[0, r0:r0 + n], n_pos, (sums_ref[0, 0:1], sums_ref[0, 1:2]), grp_ref[...],
                     anorm_v, proj_v, k_buf, q_buf, v_buf, bound_ref)

        @pl.when(j == 0)
        def _():
            for k in range(len(peers)):
                copy(s, k).wait_recv()
            own(s).wait()

            def take(i, sums):
                v = xv[s, pl.ds(i * 4, 4)].reshape(4 * ww, n_ch)
                o_ref[s, pl.ds(pl.multiple_of(i * 4 * ww, 4 * ww), 4 * ww)] = v
                d1, d2 = _chan_sums(v.astype(F32))
                return sums[0] + d1, sums[1] + d2

            s1, s2 = lax.fori_loop(0, hh // 4, take, _zero_sums(n_ch))
            sums_s[0:1] = s1
            sums_s[1:2] = s2

        t_row = temb_s[pl.ds(me * n_img + s, 1), :]

        def epilogue(r0, acc):
            n = acc.shape[0]
            x = xv[s, r0 // ww:(r0 + n) // ww].reshape(n, n_ch).astype(F32)
            out = (acc + jnp.where(j == 0, t_row, x)).astype(BF16)
            o_ref[s, r0:r0 + n] = out
            return out

        blk.conv(j, lambda r0, n: o_ref[s, r0:r0 + n], (sums_s[0:1], sums_s[1:2]), CHUNK, epilogue)
        sums_ref[s] = sums_s[...]
        return carry

    lax.fori_loop(0, 2 * n_img, half_block, 0)
    for k in range(len(peers)):
        copy(n_img - 1, k).wait_send()


def _last_kernel(n_row, n_col, x_ref, sums_ref, rnorm_ref, w_t, temb_ref, grp_ref, o_ref,
                 yv, act, hid, sums_s, send_sem, recv_sem, loc_sem):
    me_r, me_c, peers = _me_and_peers(n_row, n_col)
    me = me_r * n_col + me_c
    n_img, hh, ww, n_ch = yv.shape
    bh, bw = hh // n_row, ww // n_col
    blk = _ResBlock(hh, ww, n_ch, rnorm_ref.at[1], w_t, act, hid, temb_ref, grp_ref, sums_s)
    blk.clear_borders()
    _barrier(peers)

    def block(s, k, c):
        return yv.at[s, pl.ds(k * bh, bh), pl.ds(pl.multiple_of(c * bw, bw), bw), :]

    def rel(k, c):
        return lax.rem(k - me_r + n_row, n_row) * n_col + lax.rem(c - me_c + n_col, n_col)

    def copy(s, k, c):
        return pltpu.make_async_remote_copy(
            block(s, k, c), o_ref.at[me * n_img + s], send_sem.at[s, rel(k, c)], recv_sem.at[s, rel(k, c)],
            device_id={'row': k, 'col': c}, device_id_type=MESH)

    def own(s):
        return pltpu.make_async_copy(block(s, me_r, me_c), o_ref.at[me * n_img + s], loc_sem.at[s])

    def image(s, carry):
        def src(r0, n):
            return x_ref[s, r0:r0 + n]

        def ready(r0, end):
            size, blocks = bh * ww, []
            for k in range(n_row):
                if k * size < end and (k + 1) * size > r0:
                    done.setdefault(k, set()).update(range(max(r0, k * size), min(end, (k + 1) * size)))
                    if len(done[k]) == size:
                        done.pop(k)
                        blocks.append(k)
            return blocks

        done = {}

        def dst(r0, v):
            end, at = r0 + v.shape[0], r0
            while at < end:
                n = min(end, (at // ww + 1) * ww) - at
                yv[s, at // ww, at % ww:at % ww + n] = v[at - r0:at - r0 + n]
                at += n
            for k in ready(r0, end):
                for d in range(n_col):
                    c = lax.rem(me_c + 1 + d, n_col)
                    remote = (k != me_r) | (c != me_c)

                    @pl.when(remote)
                    def _():
                        copy(s, k, c).start()

                    @pl.when(jnp.logical_not(remote))
                    def _():
                        own(s).start()

        blk.run(src, (sums_ref[s, 0:1], sums_ref[s, 1:2]), me * n_img + s, LAST_CHUNK, dst, me_r < n_row // 2)
        return carry

    lax.fori_loop(0, n_img, image, 0)
    for s in range(n_img):
        for r, c in peers:
            copy(s, r, c).wait()
        own(s).wait()


def _attn_kernel(x_ref, sums_ref, anorm_ref, proj_ref, grp_ref, k_in, q_in, v_in, bound_in,
                 o_ref, osums_ref, k_buf, q_buf, v_buf, bound_ref, ot_buf):
    n_img, n_pos, n_ch = x_ref.shape
    head_dim, scale = HEAD_DIM, LOGIT_SCALE
    n_heads = n_ch // head_dim
    per_blk = 128 // head_dim

    def image(img, carry_img):
        @pl.when(img > 0)
        def _():
            _project(lambda r0, n: x_ref[img, r0:r0 + n], n_pos, (sums_ref[img, 0:1], sums_ref[img, 1:2]),
                     grp_ref[...], anorm_ref, proj_ref, k_buf, q_buf, v_buf, bound_ref)

        top2, v_max = jnp.max(bound_ref[0:1]), jnp.max(bound_ref[1:2])
        small = ((top2 < 96.0 ** 2) & (v_max < 2.0 ** 20)) | ((top2 < 108.0 ** 2) & (v_max < 2.0 ** 8))

        @pl.when(small)
        def _():
            n_kc = n_pos // K_CHUNK

            def heads(b, carry):
                b0 = pl.multiple_of(b * 128, 128)
                tiles = [(j, t * Q_TILE) for j in range(per_blk) for t in range(n_pos // Q_TILE)]
                steps = [(tile, c) for tile in tiles for c in range(n_kc)]

                def score(step):
                    (j, q0), c = step
                    h0 = pl.multiple_of(b0 + j * head_dim, head_dim)
                    keys = k_buf[j, c * K_CHUNK:(c + 1) * K_CHUNK, pl.ds(b0, 128)]
                    return _dot(keys[:, :head_dim], q_buf[pl.ds(h0, head_dim), q0:q0 + Q_TILE])

                pending = [score(s) for s in steps[:AHEAD]]
                tot = out = None
                for n, ((j, q0), c) in enumerate(steps):
                    if n + AHEAD < len(steps):
                        pending.append(score(steps[n + AHEAD]))
                    p = jnp.exp2(pending.pop(0) * scale)
                    h0 = pl.multiple_of(b0 + j * head_dim, head_dim)
                    part = jnp.sum(p.reshape(K_CHUNK // 8, 8, Q_TILE), axis=0)
                    pv = _dot(v_buf[pl.ds(h0, head_dim), c * K_CHUNK:(c + 1) * K_CHUNK], p.astype(BF16))
                    tot, out = (part, pv) if c == 0 else (tot + part, out + pv)
                    if c == n_kc - 1:
                        res = out / jnp.sum(tot, axis=0, keepdims=True)
                        ot_buf[pl.ds(h0, head_dim), q0:q0 + Q_TILE] = res.astype(BF16)
                return carry

            lax.fori_loop(0, n_ch // 128, heads, 0)

        @pl.when(jnp.logical_not(small))
        def _():
            rh = lax.broadcasted_iota(jnp.int32, (128, 256), 0) // head_dim
            n_tiles = n_pos // 256

            def tile(i, carry):
                h = i // n_tiles
                q0 = pl.multiple_of((i % n_tiles) * 256, 256)
                b0 = pl.multiple_of((h // per_blk) * 128, 128)
                h0 = pl.multiple_of(h * head_dim, head_dim)
                qm = jnp.where(rh == h % per_blk, q_buf[pl.ds(b0, 128), pl.ds(q0, 256)], 0)
                s = _dot(k_buf[0, :, pl.ds(b0, 128)], qm)
                p = jnp.exp2((s - jnp.max(s, axis=0, keepdims=True)) * scale)
                o = _dot(v_buf[pl.ds(h0, head_dim), :], p.astype(BF16))
                ot_buf[pl.ds(h0, head_dim), pl.ds(q0, 256)] = (o / jnp.sum(p, axis=0, keepdims=True)).astype(BF16)
                return carry

            lax.fori_loop(0, n_heads * n_tiles, tile, 0)

        s1, s2 = _zero_sums(n_ch)
        for r0 in range(0, n_pos, PROJ_TILE):
            tile = slice(r0, r0 + PROJ_TILE)
            acc = _dot(ot_buf[:, tile], proj_ref[3], ((0,), (0,)))
            out = (x_ref[img, tile].astype(F32) + acc).astype(BF16)
            o_ref[img, tile] = out
            d1, d2 = _chan_sums(out.astype(F32))
            s1, s2 = s1 + d1, s2 + d2
        osums_ref[img, 0:1] = s1
        osums_ref[img, 1:2] = s2
        return carry_img

    lax.fori_loop(0, n_img, image, 0)


K1_LIMIT, K2_LIMIT, K3_LIMIT = 36, 16, 24


def solution(mesh):
    n_row, n_col = mesh.shape['row'], mesh.shape['col']
    n_dev = n_row * n_col
    vmem, hbm = pl.BlockSpec(memory_space=pltpu.VMEM), pl.BlockSpec(memory_space=pltpu.HBM)

    def run_stage(latent, t_emb, res_norm, res_conv, res_temb, attn_norm, attn_proj):
        n_batch, bh, bw, n_ch = latent.shape
        hh, ww = bh * n_row, bw * n_col
        n_pos, n_img = hh * ww, n_batch // n_dev
        proj = jnp.transpose(attn_proj, (0, 1, 3, 2)).reshape(4, n_ch, n_ch)
        conv_w = res_conv.reshape(2, 2, 9 * n_ch, n_ch)
        images = pltpu.VMEM((n_img, hh, ww, n_ch), BF16)
        act = pltpu.VMEM(((hh + 2) * ww, 3 * n_ch), BF16)
        chan_sums = pltpu.VMEM((8, n_ch), F32)
        remote = [pltpu.SemaphoreType.DMA((n_img, n_dev)), pltpu.SemaphoreType.DMA((n_img, n_dev)),
                  pltpu.SemaphoreType.DMA((n_img,))]
        x_out, sums_out = pltpu.VMEM((n_img, n_pos, n_ch), BF16), pltpu.VMEM((n_img, 8, n_ch), F32)
        qkv_out = [pltpu.VMEM((128 // HEAD_DIM, n_pos, n_ch), BF16), pltpu.VMEM((n_ch, n_pos), BF16),
                   pltpu.VMEM((n_ch, n_pos), BF16), pltpu.VMEM((8, 128), F32)]

        from_hbm = (latent, t_emb, res_norm, conv_w, res_temb, attn_norm, proj)
        x1, sums1, next_w, next_temb, grp, *qkv = pl.pallas_call(
            functools.partial(_first_kernel, n_row, n_col),
            out_shape=[x_out, sums_out, pltpu.VMEM((2, n_ch, 9 * n_ch), BF16), pltpu.VMEM((n_batch, n_ch), F32),
                       pltpu.VMEM((n_ch, n_ch), BF16), *qkv_out],
            in_specs=[hbm] * len(from_hbm),
            out_specs=[vmem] * 9,
            scratch_shapes=[
                images, pltpu.VMEM((4, 9 * n_ch, n_ch), BF16), pltpu.VMEM((2, n_ch, 9 * n_ch), BF16),
                *(pltpu.VMEM(a.shape, BF16) for a in (t_emb, res_norm, res_temb, attn_norm, proj)),
                act, pltpu.VMEM((n_batch, n_ch), F32), chan_sums, pltpu.SemaphoreType.DMA((9,)), *remote,
            ],
            compiler_params=pltpu.CompilerParams(collective_id=0, has_side_effects=True, vmem_limit_bytes=K1_LIMIT << 20),
        )(*(pltpu.with_memory_space_constraint(a, pltpu.HBM) for a in from_hbm))

        x2, sums2, *_ = pl.pallas_call(
            _attn_kernel,
            out_shape=[x_out, sums_out, *qkv_out],
            in_specs=[vmem] * 9,
            out_specs=[vmem] * 6,
            input_output_aliases={5: 2, 6: 3, 7: 4, 8: 5},
            scratch_shapes=[pltpu.VMEM((n_ch, n_pos), BF16)],
            compiler_params=pltpu.CompilerParams(vmem_limit_bytes=K2_LIMIT << 20),
        )(x1, sums1, attn_norm, proj, grp, *qkv)

        return pl.pallas_call(
            functools.partial(_last_kernel, n_row, n_col),
            out_shape=pltpu.VMEM(latent.shape, BF16),
            in_specs=[vmem] * 6,
            out_specs=vmem,
            scratch_shapes=[images, act, pltpu.VMEM((n_pos, n_ch), BF16), chan_sums, *remote],
            compiler_params=pltpu.CompilerParams(collective_id=1, has_side_effects=True, vmem_limit_bytes=K3_LIMIT << 20),
        )(x2, sums2, res_norm, next_w, next_temb, grp)

    spec_x = P('dp', 'row', 'col', None)
    return jax.shard_map(run_stage, mesh=mesh, in_specs=(spec_x, P('dp', None), P(), P(), P(), P(), P()), out_specs=spec_x, check_vma=False)
```

```python
import functools

import jax
import jax.numpy as jnp
from jax import lax
from jax.experimental import pallas as pl
from jax.experimental.pallas import tpu as pltpu
from jax.sharding import PartitionSpec as P

MESH = pl.DeviceIdType.MESH
GROUPS = 32
EPS = 1e-5
LOG2E = 1.4426950408889634
F32 = jnp.float32
BF16 = jnp.bfloat16
Q_TILE = 512
K_CHUNK = 256
AHEAD = 2
CHUNK = 768
LAST_CHUNK = 512
PROJ_TILE = 512


def _me_and_peers(n_row, n_col):
    me_r, me_c = lax.axis_index('row'), lax.axis_index('col')
    half = n_row // 2

    def other(r, far, core):
        r = lax.rem(r + far * half, n_row)
        return r // half * half + lax.rem(lax.rem(r, half) + core, half)

    order = [(f, k, c) for f, c in ((1, 1), (1, 0), (0, 1), (0, 0)) for k in range(half) if f or c or k]
    return me_r, me_c, [(other(me_r, f, k), lax.rem(me_c + c, n_col)) for f, k, c in order]


def _signal_peers(peers):
    for r, c in peers:
        pl.semaphore_signal(pltpu.get_barrier_semaphore(), inc=1, device_id={'row': r, 'col': c}, device_id_type=MESH)


def _await_peers(peers):
    pl.semaphore_wait(pltpu.get_barrier_semaphore(), len(peers))


def _dot(a, b, dims=((1,), (0,))):
    return lax.dot_general(a, b, (dims, ((), ())), preferred_element_type=F32)


def _chan_sums(v):
    return jnp.sum(v, axis=0, keepdims=True), jnp.sum(v * v, axis=0, keepdims=True)


def _group_matrix(n_ch):
    per = n_ch // GROUPS
    gi = lax.broadcasted_iota(jnp.int32, (n_ch, n_ch), 0) // per
    gj = lax.broadcasted_iota(jnp.int32, (n_ch, n_ch), 1) // per
    return jnp.where(gi == gj, 1.0, 0.0).astype(BF16)


def _moments(s1, s2, grp, count):
    n_ch = s1.shape[1]
    st = jnp.concatenate([s1, s2, jnp.zeros((6, n_ch), F32)], axis=0)
    hi = st.astype(BF16)
    r1 = st - hi.astype(F32)
    mid = r1.astype(BF16)
    lo = (r1 - mid.astype(F32)).astype(BF16)
    parts = _dot(jnp.concatenate([hi.astype(F32), mid.astype(F32), lo.astype(F32)], axis=0).astype(BF16), grp)
    tot = (parts[16:24] + parts[8:16]) + parts[0:8]
    mean = tot[0:1] / count
    var = tot[1:2] / count - mean * mean
    return mean, lax.rsqrt(var + EPS)


def _zero_sums(n_ch):
    return jnp.zeros((1, n_ch), F32), jnp.zeros((1, n_ch), F32)


class _ResBlock:
    def __init__(self, hh, ww, n_ch, rnorm_ref, w_t, act, hid, temb_s, grp_s, sums_s):
        self.hh, self.ww, self.n_ch = hh, ww, n_ch
        self.rnorm_ref, self.w_t, self.act, self.hid = rnorm_ref, w_t, act, hid
        self.temb_s, self.grp_s, self.sums_s = temb_s, grp_s, sums_s
        self.count = float(hh * ww * (n_ch // GROUPS))

    def clear_borders(self):
        zeros = jnp.zeros((self.ww, self.act.shape[1]), BF16)
        self.act[0:self.ww, :] = zeros
        self.act[(self.hh + 1) * self.ww:(self.hh + 2) * self.ww, :] = zeros

    def conv(self, j, src, sums, chunk, epilogue, backward=False):
        ww, n_ch, act = self.ww, self.n_ch, self.act
        mean, inv = _moments(*sums, self.grp_s[...], self.count)
        a_mul = inv * self.rnorm_ref[j, 0:1].astype(F32)
        half_b = 0.5 * (self.rnorm_ref[j, 1:2].astype(F32) - mean * a_mul)
        half_a = 0.5 * a_mul
        edge = jnp.zeros((1, n_ch), BF16)

        def fill(i):
            w = src(i * ww, ww).astype(F32) * half_a + half_b
            a = w * jnp.tanh(w) + w
            d0 = (i + 1) * ww
            act[d0:d0 + ww, 0:n_ch] = pltpu.roll(a, 1, 0).astype(BF16)
            act[d0:d0 + ww, n_ch:2 * n_ch] = a.astype(BF16)
            act[d0:d0 + ww, 2 * n_ch:3 * n_ch] = pltpu.roll(a, ww - 1, 0).astype(BF16)
            act[d0:d0 + 1, 0:n_ch] = edge
            act[d0 + ww - 1:d0 + ww, 2 * n_ch:3 * n_ch] = edge

        n_pos, filled = self.hh * ww, set()

        def fill_for(r0):
            for i in range(max(0, r0 // ww - 1), min(self.hh, (r0 + chunk - 1) // ww + 2)):
                if i not in filled:
                    filled.add(i)
                    fill(i)

        starts = list(range(0, n_pos, chunk))[::-1 if backward else 1]
        fill_for(starts[0])
        s1, s2 = _zero_sums(n_ch)
        for at, r0 in enumerate(starts):
            lhs = jnp.concatenate([act[r0 + dy * ww:r0 + dy * ww + chunk, :] for dy in range(3)], axis=1)
            acc = _dot(self.w_t[j], lhs, ((1,), (1,)))
            for ahead in starts[at + 1:at + 2]:
                fill_for(ahead)
            out = epilogue(r0, acc.T)
            d1, d2 = _chan_sums(out.astype(F32))
            s1, s2 = s1 + d1, s2 + d2
        self.sums_s[0:1] = s1
        self.sums_s[1:2] = s2

    def run(self, src, sums, img, last_chunk, before_last, dst, backward):
        hid, sums_s = self.hid, self.sums_s
        t_row = self.temb_s[pl.ds(img, 1), :]

        def first(r0, acc):
            out = (acc + t_row).astype(BF16)
            hid[r0:r0 + out.shape[0]] = out
            return out

        def second(r0, acc):
            out = (src(r0, acc.shape[0]).astype(F32) + acc).astype(BF16)
            dst(r0, out)
            return out

        self.conv(0, src, sums, CHUNK, first)
        before_last()

        def last(order):
            self.conv(1, lambda r0, n: hid[r0:r0 + n], (sums_s[0:1], sums_s[1:2]), last_chunk, second, order)

        pl.when(backward)(lambda: last(True))
        pl.when(jnp.logical_not(backward))(lambda: last(False))


HEAD_DIM = 32
LOGIT_SCALE = LOG2E * HEAD_DIM ** -0.5


def _project(src, n_pos, sums, grp, anorm_ref, proj_ref, k_buf, q_buf, v_buf, bound_ref):
    n_ch = proj_ref.shape[-1]
    n_heads = n_ch // HEAD_DIM
    mean, inv = _moments(*sums, grp, float(n_pos * (n_ch // GROUPS)))
    a_mul = inv * anorm_ref[0:1].astype(F32)
    b_add = anorm_ref[1:2].astype(F32)
    head_rows = jnp.where(lax.broadcasted_iota(jnp.int32, (16, n_ch), 0)
                          == lax.broadcasted_iota(jnp.int32, (16, n_ch), 1) // HEAD_DIM, 1.0, 0.0).astype(BF16)
    q_top = jnp.zeros((n_heads, PROJ_TILE), F32)
    k_top = jnp.zeros((16, PROJ_TILE), F32)
    v_top = jnp.zeros((1, PROJ_TILE), F32)
    last_k = None
    for r0 in [*range(0, n_pos, PROJ_TILE), None]:
        if r0 is not None:
            tile = slice(r0, r0 + PROJ_TILE)
            g = ((src(r0, PROJ_TILE).astype(F32) - mean) * a_mul + b_add).astype(BF16)
            k = _dot(g, proj_ref[1], ((1,), (1,)))
            q = _dot(proj_ref[0], g, ((1,), (1,))).astype(BF16)
            v = _dot(proj_ref[2], g, ((1,), (1,))).astype(BF16)
            for b0 in range(0, n_ch, 128):
                for j in range(128 // HEAD_DIM):
                    part = k[:, b0:b0 + 128]
                    part = part if j == 0 else pltpu.roll(part, 128 - j * HEAD_DIM, 1)
                    k_buf[j, tile, b0:b0 + 128] = part.astype(BF16)
            k = k.astype(BF16)
            q_buf[:, tile] = q
            v_buf[:, tile] = v
            q = q.astype(F32)
            q_top = jnp.maximum(q_top, jnp.sum((q * q).reshape(n_heads, HEAD_DIM, PROJ_TILE), axis=1))
            v_top = jnp.maximum(v_top, jnp.max(jnp.abs(v.astype(F32)), axis=0, keepdims=True))
        if last_k is not None:
            k2 = last_k.astype(F32) * last_k.astype(F32)
            k_top = jnp.maximum(k_top, _dot(head_rows, k2.astype(BF16), ((1,), (1,))))
        last_k = k
    q_top = jnp.max(q_top, axis=1, keepdims=True)
    k_top = jnp.max(k_top, axis=1, keepdims=True)[:n_heads]
    top2 = jnp.max(q_top * k_top, axis=0, keepdims=True) * (LOGIT_SCALE * LOGIT_SCALE)
    bound_ref[0:1] = jnp.broadcast_to(top2, (1, 128))
    bound_ref[1:2] = jnp.broadcast_to(jnp.max(v_top, axis=1, keepdims=True), (1, 128))


def _out_project(x_ref, ot_ref, proj_ref, o_ref, sums_ref):
    n_pos, n_ch = x_ref.shape
    s1, s2 = _zero_sums(n_ch)
    for r0 in range(0, n_pos, PROJ_TILE):
        tile = slice(r0, r0 + PROJ_TILE)
        acc = _dot(ot_ref[:, tile], proj_ref[3], ((0,), (0,)))
        out = (x_ref[tile].astype(F32) + acc).astype(BF16)
        o_ref[tile] = out
        d1, d2 = _chan_sums(out.astype(F32))
        s1, s2 = s1 + d1, s2 + d2
    sums_ref[0:1] = s1
    sums_ref[1:2] = s2


def _first_kernel(n_row, n_col, lat_ref, temb_hbm, rnorm_hbm, conv_hbm, wtemb_hbm, anorm_hbm, proj_hbm,
                  o_ref, sums_ref, next_w, next_temb, grp_ref, k_buf, q_buf, v_buf, bound_ref,
                  xv, wconv, w_t, temb_v, rnorm_v, wtemb, anorm_v, proj_v, act, temb_s, sums_s,
                  wsem, send_sem, recv_sem, loc_sem):
    me_r, me_c, peers = _me_and_peers(n_row, n_col)
    me = me_r * n_col + me_c
    n_img, hh, ww, n_ch = xv.shape
    n_pos = hh * ww
    bh, bw = hh // n_row, ww // n_col
    weights = [pltpu.make_async_copy(conv_hbm.at[i // 2, i % 2], wconv.at[i], wsem.at[i]) for i in range(4)]
    small = [pltpu.make_async_copy(a, b, wsem.at[4 + i]) for i, (a, b) in enumerate([
        (wtemb_hbm, wtemb), (temb_hbm, temb_v), (rnorm_hbm, rnorm_v), (anorm_hbm, anorm_v), (proj_hbm, proj_v)])]

    def place(s):
        return xv.at[s, pl.ds(me_r * bh, bh), pl.ds(pl.multiple_of(me_c * bw, bw), bw), :]

    def copy(s, k):
        r, c = peers[k]
        return pltpu.make_async_remote_copy(
            lat_ref.at[(r * n_col + c) * n_img + s], place(s), send_sem.at[s, k], recv_sem.at[s, k],
            device_id={'row': r, 'col': c}, device_id_type=MESH)

    def own(s):
        return pltpu.make_async_copy(lat_ref.at[me * n_img + s], place(s), loc_sem.at[s])

    _signal_peers(peers)
    _await_peers(peers)
    for k in range(len(peers)):
        copy(0, k).start()
    for s in range(n_img):
        own(s).start()
    for w in [*small, *weights]:
        w.start()

    blk = _ResBlock(hh, ww, n_ch, rnorm_v.at[0], w_t, act, None, temb_s, grp_ref, sums_s)
    blk.clear_borders()
    grp_ref[...] = _group_matrix(n_ch)
    for w in small:
        w.wait()
    te = temb_v[...].astype(F32)
    t_act = (te * jax.nn.sigmoid(te)).astype(BF16)
    temb_s[...] = _dot(t_act, wtemb[0])
    next_temb[...] = _dot(t_act, wtemb[1])
    for w in weights:
        w.wait()

    def turn(i, carry):
        t0 = pl.multiple_of(i * n_ch, n_ch)
        for j in range(4):
            out = w_t.at[j] if j < 2 else next_w.at[j - 2]
            out[:, pl.ds(t0, n_ch)] = wconv[j, pl.ds(t0, n_ch), :].T
        return carry

    lax.fori_loop(0, 9, turn, 0)
    for s in range(1, n_img):
        for k in range(len(peers)):
            copy(s - 1, k).wait_send()
            copy(s, k).start()

    def half_block(t, carry):
        s, j = t // 2, lax.rem(t, 2)

        @pl.when(t == 2)
        def _():
            _project(lambda r0, n: o_ref[0, r0:r0 + n], n_pos, (sums_ref[0, 0:1], sums_ref[0, 1:2]), grp_ref[...],
                     anorm_v, proj_v, k_buf, q_buf, v_buf, bound_ref)

        @pl.when(j == 0)
        def _():
            for k in range(len(peers)):
                copy(s, k).wait_recv()
            own(s).wait()

            def take(i, sums):
                v = xv[s, pl.ds(i * 4, 4)].reshape(4 * ww, n_ch)
                o_ref[s, pl.ds(pl.multiple_of(i * 4 * ww, 4 * ww), 4 * ww)] = v
                d1, d2 = _chan_sums(v.astype(F32))
                return sums[0] + d1, sums[1] + d2

            s1, s2 = lax.fori_loop(0, hh // 4, take, _zero_sums(n_ch))
            sums_s[0:1] = s1
            sums_s[1:2] = s2

        t_row = temb_s[pl.ds(me * n_img + s, 1), :]

        def epilogue(r0, acc):
            n = acc.shape[0]
            x = xv[s, r0 // ww:(r0 + n) // ww].reshape(n, n_ch).astype(F32)
            out = (acc + jnp.where(j == 0, t_row, x)).astype(BF16)
            o_ref[s, r0:r0 + n] = out
            return out

        blk.conv(j, lambda r0, n: o_ref[s, r0:r0 + n], (sums_s[0:1], sums_s[1:2]), CHUNK, epilogue)
        sums_ref[s] = sums_s[...]
        return carry

    lax.fori_loop(0, 2 * n_img, half_block, 0)
    for k in range(len(peers)):
        copy(n_img - 1, k).wait_send()


def _last_kernel(n_row, n_col, x1_ref, ot_ref, proj_ref, x_in, sums_in, rnorm_ref, w_t, temb_ref, grp_ref,
                 o_ref, x_ref, sums_ref, yv, act, hid, sums_s, send_sem, recv_sem, loc_sem):
    me_r, me_c, peers = _me_and_peers(n_row, n_col)
    me = me_r * n_col + me_c
    n_img, hh, ww, n_ch = yv.shape
    bh, bw = hh // n_row, ww // n_col
    blk = _ResBlock(hh, ww, n_ch, rnorm_ref.at[1], w_t, act, hid, temb_ref, grp_ref, sums_s)
    _signal_peers(peers)
    blk.clear_borders()

    def block(s, k, c):
        return yv.at[s, pl.ds(k * bh, bh), pl.ds(pl.multiple_of(c * bw, bw), bw), :]

    def rel(k, c):
        return lax.rem(k - me_r + n_row, n_row) * n_col + lax.rem(c - me_c + n_col, n_col)

    def copy(s, k, c):
        return pltpu.make_async_remote_copy(
            block(s, k, c), o_ref.at[me * n_img + s], send_sem.at[s, rel(k, c)], recv_sem.at[s, rel(k, c)],
            device_id={'row': k, 'col': c}, device_id_type=MESH)

    def own(s):
        return pltpu.make_async_copy(block(s, me_r, me_c), o_ref.at[me * n_img + s], loc_sem.at[s])

    def image(s, carry):
        def src(r0, n):
            return x_ref[s, r0:r0 + n]

        def ready(r0, end):
            size, blocks = bh * ww, []
            for k in range(n_row):
                if k * size < end and (k + 1) * size > r0:
                    done.setdefault(k, set()).update(range(max(r0, k * size), min(end, (k + 1) * size)))
                    if len(done[k]) == size:
                        done.pop(k)
                        blocks.append(k)
            return blocks

        done = {}

        def dst(r0, v):
            end, at = r0 + v.shape[0], r0
            while at < end:
                n = min(end, (at // ww + 1) * ww) - at
                yv[s, at // ww, at % ww:at % ww + n] = v[at - r0:at - r0 + n]
                at += n
            for k in ready(r0, end):
                for d in range(n_col):
                    c = lax.rem(me_c + 1 + d, n_col)
                    remote = (k != me_r) | (c != me_c)

                    @pl.when(remote)
                    def _():
                        copy(s, k, c).start()

                    @pl.when(jnp.logical_not(remote))
                    def _():
                        own(s).start()

        def before_last():
            @pl.when(s == 0)
            def _():
                _await_peers(peers)

        @pl.when(s == n_img - 1)
        def _():
            _out_project(x1_ref.at[s], ot_ref, proj_ref, x_ref.at[s], sums_ref.at[s])

        blk.run(src, (sums_ref[s, 0:1], sums_ref[s, 1:2]), me * n_img + s, LAST_CHUNK, before_last, dst,
                me_r < n_row // 2)
        return carry

    lax.fori_loop(0, n_img, image, 0)
    for s in range(n_img):
        for r, c in peers:
            copy(s, r, c).wait()
        own(s).wait()


def _attn_kernel(x_ref, sums_ref, anorm_ref, proj_ref, grp_ref, k_in, q_in, v_in, bound_in,
                 o_ref, osums_ref, k_buf, q_buf, v_buf, bound_ref, ot_buf):
    n_img, n_pos, n_ch = x_ref.shape
    head_dim, scale = HEAD_DIM, LOGIT_SCALE
    n_heads = n_ch // head_dim
    per_blk = 128 // head_dim

    def image(img, carry_img):
        @pl.when(img > 0)
        def _():
            _project(lambda r0, n: x_ref[img, r0:r0 + n], n_pos, (sums_ref[img, 0:1], sums_ref[img, 1:2]),
                     grp_ref[...], anorm_ref, proj_ref, k_buf, q_buf, v_buf, bound_ref)

        top2, v_max = jnp.max(bound_ref[0:1]), jnp.max(bound_ref[1:2])
        small = ((top2 < 96.0 ** 2) & (v_max < 2.0 ** 20)) | ((top2 < 108.0 ** 2) & (v_max < 2.0 ** 8))

        @pl.when(small)
        def _():
            n_kc = n_pos // K_CHUNK

            def heads(b, carry):
                b0 = pl.multiple_of(b * 128, 128)
                tiles = [(j, t * Q_TILE) for j in range(per_blk) for t in range(n_pos // Q_TILE)]
                steps = [(tile, c) for tile in tiles for c in range(n_kc)]

                def score(step):
                    (j, q0), c = step
                    h0 = pl.multiple_of(b0 + j * head_dim, head_dim)
                    keys = k_buf[j, c * K_CHUNK:(c + 1) * K_CHUNK, pl.ds(b0, 128)]
                    return _dot(keys[:, :head_dim], q_buf[pl.ds(h0, head_dim), q0:q0 + Q_TILE])

                pending = [score(s) for s in steps[:AHEAD]]
                tot = out = None
                for n, ((j, q0), c) in enumerate(steps):
                    if n + AHEAD < len(steps):
                        pending.append(score(steps[n + AHEAD]))
                    p = jnp.exp2(pending.pop(0) * scale)
                    h0 = pl.multiple_of(b0 + j * head_dim, head_dim)
                    part = jnp.sum(p.reshape(K_CHUNK // 8, 8, Q_TILE), axis=0)
                    pv = _dot(v_buf[pl.ds(h0, head_dim), c * K_CHUNK:(c + 1) * K_CHUNK], p.astype(BF16))
                    tot, out = (part, pv) if c == 0 else (tot + part, out + pv)
                    if c == n_kc - 1:
                        res = out / jnp.sum(tot, axis=0, keepdims=True)
                        ot_buf[pl.ds(h0, head_dim), q0:q0 + Q_TILE] = res.astype(BF16)
                return carry

            lax.fori_loop(0, n_ch // 128, heads, 0)

        @pl.when(jnp.logical_not(small))
        def _():
            rh = lax.broadcasted_iota(jnp.int32, (128, 256), 0) // head_dim
            n_tiles = n_pos // 256

            def tile(i, carry):
                h = i // n_tiles
                q0 = pl.multiple_of((i % n_tiles) * 256, 256)
                b0 = pl.multiple_of((h // per_blk) * 128, 128)
                h0 = pl.multiple_of(h * head_dim, head_dim)
                qm = jnp.where(rh == h % per_blk, q_buf[pl.ds(b0, 128), pl.ds(q0, 256)], 0)
                s = _dot(k_buf[0, :, pl.ds(b0, 128)], qm)
                p = jnp.exp2((s - jnp.max(s, axis=0, keepdims=True)) * scale)
                o = _dot(v_buf[pl.ds(h0, head_dim), :], p.astype(BF16))
                ot_buf[pl.ds(h0, head_dim), pl.ds(q0, 256)] = (o / jnp.sum(p, axis=0, keepdims=True)).astype(BF16)
                return carry

            lax.fori_loop(0, n_heads * n_tiles, tile, 0)

        @pl.when(img < n_img - 1)
        def _():
            _out_project(x_ref.at[img], ot_buf, proj_ref, o_ref.at[img], osums_ref.at[img])

        return carry_img

    lax.fori_loop(0, n_img, image, 0)


K1_LIMIT, K2_LIMIT, K3_LIMIT = 36, 16, 24


def solution(mesh):
    n_row, n_col = mesh.shape['row'], mesh.shape['col']
    n_dev = n_row * n_col
    vmem, hbm = pl.BlockSpec(memory_space=pltpu.VMEM), pl.BlockSpec(memory_space=pltpu.HBM)

    def run_stage(latent, t_emb, res_norm, res_conv, res_temb, attn_norm, attn_proj):
        n_batch, bh, bw, n_ch = latent.shape
        hh, ww = bh * n_row, bw * n_col
        n_pos, n_img = hh * ww, n_batch // n_dev
        proj = jnp.transpose(attn_proj, (0, 1, 3, 2)).reshape(4, n_ch, n_ch)
        conv_w = res_conv.reshape(2, 2, 9 * n_ch, n_ch)
        images = pltpu.VMEM((n_img, hh, ww, n_ch), BF16)
        act = pltpu.VMEM(((hh + 2) * ww, 3 * n_ch), BF16)
        chan_sums = pltpu.VMEM((8, n_ch), F32)
        remote = [pltpu.SemaphoreType.DMA((n_img, n_dev)), pltpu.SemaphoreType.DMA((n_img, n_dev)),
                  pltpu.SemaphoreType.DMA((n_img,))]
        x_out, sums_out = pltpu.VMEM((n_img, n_pos, n_ch), BF16), pltpu.VMEM((n_img, 8, n_ch), F32)
        qkv_out = [pltpu.VMEM((128 // HEAD_DIM, n_pos, n_ch), BF16), pltpu.VMEM((n_ch, n_pos), BF16),
                   pltpu.VMEM((n_ch, n_pos), BF16), pltpu.VMEM((8, 128), F32)]

        from_hbm = (latent, t_emb, res_norm, conv_w, res_temb, attn_norm, proj)
        x1, sums1, next_w, next_temb, grp, *qkv = pl.pallas_call(
            functools.partial(_first_kernel, n_row, n_col),
            out_shape=[x_out, sums_out, pltpu.VMEM((2, n_ch, 9 * n_ch), BF16), pltpu.VMEM((n_batch, n_ch), F32),
                       pltpu.VMEM((n_ch, n_ch), BF16), *qkv_out],
            in_specs=[hbm] * len(from_hbm),
            out_specs=[vmem] * 9,
            scratch_shapes=[
                images, pltpu.VMEM((4, 9 * n_ch, n_ch), BF16), pltpu.VMEM((2, n_ch, 9 * n_ch), BF16),
                *(pltpu.VMEM(a.shape, BF16) for a in (t_emb, res_norm, res_temb, attn_norm, proj)),
                act, pltpu.VMEM((n_batch, n_ch), F32), chan_sums, pltpu.SemaphoreType.DMA((9,)), *remote,
            ],
            compiler_params=pltpu.CompilerParams(collective_id=0, has_side_effects=True, vmem_limit_bytes=K1_LIMIT << 20),
        )(*(pltpu.with_memory_space_constraint(a, pltpu.HBM) for a in from_hbm))

        x2, sums2, _, _, _, _, ot = pl.pallas_call(
            _attn_kernel,
            out_shape=[x_out, sums_out, *qkv_out, pltpu.VMEM((n_ch, n_pos), BF16)],
            in_specs=[vmem] * 9,
            out_specs=[vmem] * 7,
            input_output_aliases={5: 2, 6: 3, 7: 4, 8: 5},
            compiler_params=pltpu.CompilerParams(vmem_limit_bytes=K2_LIMIT << 20),
        )(x1, sums1, attn_norm, proj, grp, *qkv)

        return pl.pallas_call(
            functools.partial(_last_kernel, n_row, n_col),
            out_shape=[pltpu.VMEM(latent.shape, BF16), x_out, sums_out],
            in_specs=[vmem] * 9,
            out_specs=[vmem] * 3,
            input_output_aliases={3: 1, 4: 2},
            scratch_shapes=[images, act, pltpu.VMEM((n_pos, n_ch), BF16), chan_sums, *remote],
            compiler_params=pltpu.CompilerParams(collective_id=1, has_side_effects=True, vmem_limit_bytes=K3_LIMIT << 20),
        )(x1, ot, proj, x2, sums2, res_norm, next_w, next_temb, grp)[0]

    spec_x = P('dp', 'row', 'col', None)
    return jax.shard_map(run_stage, mesh=mesh, in_specs=(spec_x, P('dp', None), P(), P(), P(), P(), P()), out_specs=spec_x, check_vma=False)
```

```python
import functools

import jax
import jax.numpy as jnp
from jax import lax
from jax.experimental import pallas as pl
from jax.experimental.pallas import tpu as pltpu
from jax.sharding import PartitionSpec as P

MESH = pl.DeviceIdType.MESH
GROUPS = 32
EPS = 1e-5
LOG2E = 1.4426950408889634
F32 = jnp.float32
BF16 = jnp.bfloat16
Q_TILE = 512
K_CHUNK = 256
AHEAD = 2
CHUNK = 768
LAST_CHUNK = 512
PROJ_TILE = 256


def _me_and_peers(n_row, n_col):
    me_r, me_c = lax.axis_index('row'), lax.axis_index('col')
    half = n_row // 2

    def other(r, far, core):
        r = lax.rem(r + far * half, n_row)
        return r // half * half + lax.rem(lax.rem(r, half) + core, half)

    order = [(f, k, c) for f, c in ((1, 1), (1, 0), (0, 1), (0, 0)) for k in range(half) if f or c or k]
    return me_r, me_c, [(other(me_r, f, k), lax.rem(me_c + c, n_col)) for f, k, c in order]


def _signal_peers(peers):
    for r, c in peers:
        pl.semaphore_signal(pltpu.get_barrier_semaphore(), inc=1, device_id={'row': r, 'col': c}, device_id_type=MESH)


def _await_peers(peers):
    pl.semaphore_wait(pltpu.get_barrier_semaphore(), len(peers))


def _dot(a, b, dims=((1,), (0,))):
    return lax.dot_general(a, b, (dims, ((), ())), preferred_element_type=F32)


def _chan_sums(v):
    return jnp.sum(v, axis=0, keepdims=True), jnp.sum(v * v, axis=0, keepdims=True)


def _group_matrix(n_ch):
    per = n_ch // GROUPS
    gi = lax.broadcasted_iota(jnp.int32, (n_ch, n_ch), 0) // per
    gj = lax.broadcasted_iota(jnp.int32, (n_ch, n_ch), 1) // per
    return jnp.where(gi == gj, 1.0, 0.0).astype(BF16)


def _moments(s1, s2, grp, count):
    n_ch = s1.shape[1]
    st = jnp.concatenate([s1, s2, jnp.zeros((6, n_ch), F32)], axis=0)
    hi = st.astype(BF16)
    r1 = st - hi.astype(F32)
    mid = r1.astype(BF16)
    lo = (r1 - mid.astype(F32)).astype(BF16)
    parts = _dot(jnp.concatenate([hi.astype(F32), mid.astype(F32), lo.astype(F32)], axis=0).astype(BF16), grp)
    tot = (parts[16:24] + parts[8:16]) + parts[0:8]
    mean = tot[0:1] / count
    var = tot[1:2] / count - mean * mean
    return mean, lax.rsqrt(var + EPS)


def _zero_sums(n_ch):
    return jnp.zeros((1, n_ch), F32), jnp.zeros((1, n_ch), F32)


class _ResBlock:
    def __init__(self, hh, ww, n_ch, rnorm_ref, w_t, act, hid, temb_s, grp_s, sums_s):
        self.hh, self.ww, self.n_ch = hh, ww, n_ch
        self.rnorm_ref, self.w_t, self.act, self.hid = rnorm_ref, w_t, act, hid
        self.temb_s, self.grp_s, self.sums_s = temb_s, grp_s, sums_s
        self.count = float(hh * ww * (n_ch // GROUPS))

    def clear_borders(self):
        zeros = jnp.zeros((self.ww, self.act.shape[1]), BF16)
        self.act[0:self.ww, :] = zeros
        self.act[(self.hh + 1) * self.ww:(self.hh + 2) * self.ww, :] = zeros

    def conv(self, j, src, sums, chunk, epilogue, backward=False):
        ww, n_ch, act = self.ww, self.n_ch, self.act
        mean, inv = _moments(*sums, self.grp_s[...], self.count)
        a_mul = inv * self.rnorm_ref[j, 0:1].astype(F32)
        half_b = 0.5 * (self.rnorm_ref[j, 1:2].astype(F32) - mean * a_mul)
        half_a = 0.5 * a_mul
        edge = jnp.zeros((1, n_ch), BF16)

        def fill(i):
            w = src(i * ww, ww).astype(F32) * half_a + half_b
            a = w * jnp.tanh(w) + w
            d0 = (i + 1) * ww
            act[d0:d0 + ww, 0:n_ch] = pltpu.roll(a, 1, 0).astype(BF16)
            act[d0:d0 + ww, n_ch:2 * n_ch] = a.astype(BF16)
            act[d0:d0 + ww, 2 * n_ch:3 * n_ch] = pltpu.roll(a, ww - 1, 0).astype(BF16)
            act[d0:d0 + 1, 0:n_ch] = edge
            act[d0 + ww - 1:d0 + ww, 2 * n_ch:3 * n_ch] = edge

        n_pos, filled = self.hh * ww, set()

        def fill_for(r0):
            for i in range(max(0, r0 // ww - 1), min(self.hh, (r0 + chunk - 1) // ww + 2)):
                if i not in filled:
                    filled.add(i)
                    fill(i)

        starts = list(range(0, n_pos, chunk))[::-1 if backward else 1]
        fill_for(starts[0])
        s1, s2 = _zero_sums(n_ch)
        for at, r0 in enumerate(starts):
            lhs = jnp.concatenate([act[r0 + dy * ww:r0 + dy * ww + chunk, :] for dy in range(3)], axis=1)
            acc = _dot(self.w_t[j], lhs, ((1,), (1,)))
            for ahead in starts[at + 1:at + 2]:
                fill_for(ahead)
            out = epilogue(r0, acc.T)
            d1, d2 = _chan_sums(out.astype(F32))
            s1, s2 = s1 + d1, s2 + d2
        self.sums_s[0:1] = s1
        self.sums_s[1:2] = s2

    def run(self, src, sums, img, last_chunk, before_last, dst, backward):
        hid, sums_s = self.hid, self.sums_s
        t_row = self.temb_s[pl.ds(img, 1), :]

        def first(r0, acc):
            out = (acc + t_row).astype(BF16)
            hid[r0:r0 + out.shape[0]] = out
            return out

        def second(r0, acc):
            out = (src(r0, acc.shape[0]).astype(F32) + acc).astype(BF16)
            dst(r0, out)
            return out

        self.conv(0, src, sums, CHUNK, first)
        before_last()

        def last(order):
            self.conv(1, lambda r0, n: hid[r0:r0 + n], (sums_s[0:1], sums_s[1:2]), last_chunk, second, order)

        pl.when(backward)(lambda: last(True))
        pl.when(jnp.logical_not(backward))(lambda: last(False))


HEAD_DIM = 32
LOGIT_SCALE = LOG2E * HEAD_DIM ** -0.5


def _project(src, n_pos, sums, grp, anorm_ref, proj_ref, k_buf, q_buf, v_buf, bound_ref):
    n_ch = proj_ref.shape[-1]
    n_heads = n_ch // HEAD_DIM
    mean, inv = _moments(*sums, grp, float(n_pos * (n_ch // GROUPS)))
    a_mul = inv * anorm_ref[0:1].astype(F32)
    b_add = anorm_ref[1:2].astype(F32)
    head_rows = jnp.where(lax.broadcasted_iota(jnp.int32, (16, n_ch), 0)
                          == lax.broadcasted_iota(jnp.int32, (16, n_ch), 1) // HEAD_DIM, 1.0, 0.0).astype(BF16)
    q_top = jnp.zeros((n_heads, PROJ_TILE), F32)
    k_top = jnp.zeros((16, PROJ_TILE), F32)
    v_top = jnp.zeros((1, PROJ_TILE), F32)
    last_k = None
    for r0 in [*range(0, n_pos, PROJ_TILE), None]:
        if r0 is not None:
            tile = slice(r0, r0 + PROJ_TILE)
            g = ((src(r0, PROJ_TILE).astype(F32) - mean) * a_mul + b_add).astype(BF16)
            k = _dot(g, proj_ref[1], ((1,), (1,)))
            q = _dot(proj_ref[0], g, ((1,), (1,))).astype(BF16)
            v = _dot(proj_ref[2], g, ((1,), (1,))).astype(BF16)
            for b0 in range(0, n_ch, 128):
                for j in range(128 // HEAD_DIM):
                    part = k[:, b0:b0 + 128]
                    part = part if j == 0 else pltpu.roll(part, 128 - j * HEAD_DIM, 1)
                    k_buf[j, tile, b0:b0 + 128] = part.astype(BF16)
            k = k.astype(BF16)
            q_buf[:, tile] = q
            v_buf[:, tile] = v
            q = q.astype(F32)
            q_top = jnp.maximum(q_top, jnp.sum((q * q).reshape(n_heads, HEAD_DIM, PROJ_TILE), axis=1))
            v_top = jnp.maximum(v_top, jnp.max(jnp.abs(v.astype(F32)), axis=0, keepdims=True))
        if last_k is not None:
            k2 = last_k.astype(F32) * last_k.astype(F32)
            k_top = jnp.maximum(k_top, _dot(head_rows, k2.astype(BF16), ((1,), (1,))))
        last_k = k
    q_top = jnp.max(q_top, axis=1, keepdims=True)
    k_top = jnp.max(k_top, axis=1, keepdims=True)[:n_heads]
    top2 = jnp.max(q_top * k_top, axis=0, keepdims=True) * (LOGIT_SCALE * LOGIT_SCALE)
    bound_ref[0:1] = jnp.broadcast_to(top2, (1, 128))
    bound_ref[1:2] = jnp.broadcast_to(jnp.max(v_top, axis=1, keepdims=True), (1, 128))


def _out_project(x_ref, ot_ref, proj_ref, o_ref, sums_ref):
    n_pos, n_ch = x_ref.shape
    s1, s2 = _zero_sums(n_ch)
    for r0 in range(0, n_pos, PROJ_TILE):
        tile = slice(r0, r0 + PROJ_TILE)
        acc = _dot(ot_ref[:, tile], proj_ref[3], ((0,), (0,)))
        out = (x_ref[tile].astype(F32) + acc).astype(BF16)
        o_ref[tile] = out
        d1, d2 = _chan_sums(out.astype(F32))
        s1, s2 = s1 + d1, s2 + d2
    sums_ref[0:1] = s1
    sums_ref[1:2] = s2


def _first_kernel(n_row, n_col, lat_ref, temb_hbm, rnorm_hbm, conv_hbm, wtemb_hbm, anorm_hbm, proj_hbm,
                  o_ref, sums_ref, next_w, next_temb, grp_ref, k_buf, q_buf, v_buf, bound_ref,
                  xv, wconv, w_t, temb_v, rnorm_v, wtemb, anorm_v, proj_v, lat_v, part, parts, act, temb_s, sums_s,
                  wsem, send_sem, recv_sem, loc_sem, psend_sem, precv_sem):
    me_r, me_c, peers = _me_and_peers(n_row, n_col)
    me = me_r * n_col + me_c
    n_img, hh, ww, n_ch = xv.shape
    n_pos = hh * ww
    bh, bw = hh // n_row, ww // n_col
    weights = [pltpu.make_async_copy(conv_hbm.at[i // 2, i % 2], wconv.at[i], wsem.at[i]) for i in range(4)]
    small = [pltpu.make_async_copy(a, b, wsem.at[4 + i]) for i, (a, b) in enumerate([
        (wtemb_hbm, wtemb), (temb_hbm, temb_v), (rnorm_hbm, rnorm_v), (anorm_hbm, anorm_v), (proj_hbm, proj_v),
        (lat_ref, lat_v)])]

    def place(s):
        return xv.at[s, pl.ds(me_r * bh, bh), pl.ds(pl.multiple_of(me_c * bw, bw), bw), :]

    def copy(s, k):
        r, c = peers[k]
        return pltpu.make_async_remote_copy(
            lat_ref.at[(r * n_col + c) * n_img + s], place(s), send_sem.at[s, k], recv_sem.at[s, k],
            device_id={'row': r, 'col': c}, device_id_type=MESH)

    def part_copy(k):
        r, c = peers[k]
        return pltpu.make_async_remote_copy(
            part.at[pl.ds((r * n_col + c) * n_img, n_img)], parts.at[me], psend_sem.at[k], precv_sem.at[k],
            device_id={'row': r, 'col': c}, device_id_type=MESH)

    def own(s):
        return pltpu.make_async_copy(lat_ref.at[me * n_img + s], place(s), loc_sem.at[s])

    _signal_peers(peers)
    _await_peers(peers)
    for k in range(len(peers)):
        copy(0, k).start()
    for s in range(n_img):
        own(s).start()
    for w in [*small, *weights]:
        w.start()

    blk = _ResBlock(hh, ww, n_ch, rnorm_v.at[0], w_t, act, None, temb_s, grp_ref, sums_s)
    blk.clear_borders()
    grp_ref[...] = _group_matrix(n_ch)
    for w in small:
        w.wait()
    te = temb_v[...].astype(F32)
    t_act = (te * jax.nn.sigmoid(te)).astype(BF16)
    temb_s[...] = _dot(t_act, wtemb[0])
    next_temb[...] = _dot(t_act, wtemb[1])
    part[...] = jnp.zeros(part.shape, F32)

    def block_sums(i, carry):
        d1, d2 = _chan_sums(lat_v[i].reshape(bh * bw, n_ch).astype(F32))
        part[i, 0:1] = d1
        part[i, 1:2] = d2
        return carry

    lax.fori_loop(0, part.shape[0], block_sums, 0)
    parts[me] = part[pl.ds(me * n_img, n_img)]
    for w in weights:
        w.wait()

    def turn(i, carry):
        t0 = pl.multiple_of(i * n_ch, n_ch)
        for j in range(4):
            out = w_t.at[j] if j < 2 else next_w.at[j - 2]
            out[:, pl.ds(t0, n_ch)] = wconv[j, pl.ds(t0, n_ch), :].T
        return carry

    lax.fori_loop(0, 9, turn, 0)
    for k in range(len(peers)):
        part_copy(k).start()
    for s in range(1, n_img):
        for k in range(len(peers)):
            copy(s - 1, k).wait_send()
            copy(s, k).start()

    def half_block(t, carry):
        s, j = t // 2, lax.rem(t, 2)

        @pl.when(t == 2)
        def _():
            _project(lambda r0, n: o_ref[0, r0:r0 + n], n_pos, (sums_ref[0, 0:1], sums_ref[0, 1:2]), grp_ref[...],
                     anorm_v, proj_v, k_buf, q_buf, v_buf, bound_ref)

        @pl.when(j == 0)
        def _():
            for k in range(len(peers)):
                copy(s, k).wait_recv()
            own(s).wait()

            @pl.when(s == 0)
            def _():
                for k in range(len(peers)):
                    part_copy(k).wait_recv()

            tot = parts[0, s]
            for d in range(1, parts.shape[0]):
                tot = tot + parts[d, s]
            sums_s[...] = tot

        t_row = temb_s[pl.ds(me * n_img + s, 1), :]

        def epilogue(r0, acc):
            n = acc.shape[0]
            x = xv[s, r0 // ww:(r0 + n) // ww].reshape(n, n_ch).astype(F32)
            out = (acc + jnp.where(j == 0, t_row, x)).astype(BF16)
            o_ref[s, r0:r0 + n] = out
            return out

        def src(r0, n):
            return jnp.where(j == 0, xv[s, r0 // ww:(r0 + n) // ww].reshape(n, n_ch), o_ref[s, r0:r0 + n])

        blk.conv(j, src, (sums_s[0:1], sums_s[1:2]), CHUNK, epilogue)
        sums_ref[s] = sums_s[...]
        return carry

    lax.fori_loop(0, 2 * n_img, half_block, 0)
    for k in range(len(peers)):
        copy(n_img - 1, k).wait_send()
        part_copy(k).wait_send()


def _last_kernel(n_row, n_col, x1_ref, ot_ref, proj_ref, x_in, sums_in, rnorm_ref, w_t, temb_ref, grp_ref,
                 o_ref, x_ref, sums_ref, yv, act, hid, sums_s, send_sem, recv_sem, loc_sem):
    me_r, me_c, peers = _me_and_peers(n_row, n_col)
    me = me_r * n_col + me_c
    n_img, hh, ww, n_ch = yv.shape
    bh, bw = hh // n_row, ww // n_col
    blk = _ResBlock(hh, ww, n_ch, rnorm_ref.at[1], w_t, act, hid, temb_ref, grp_ref, sums_s)
    _signal_peers(peers)
    blk.clear_borders()

    def block(s, k, c):
        return yv.at[s, pl.ds(k * bh, bh), pl.ds(pl.multiple_of(c * bw, bw), bw), :]

    def rel(k, c):
        return lax.rem(k - me_r + n_row, n_row) * n_col + lax.rem(c - me_c + n_col, n_col)

    def copy(s, k, c):
        return pltpu.make_async_remote_copy(
            block(s, k, c), o_ref.at[me * n_img + s], send_sem.at[s, rel(k, c)], recv_sem.at[s, rel(k, c)],
            device_id={'row': k, 'col': c}, device_id_type=MESH)

    def own(s):
        return pltpu.make_async_copy(block(s, me_r, me_c), o_ref.at[me * n_img + s], loc_sem.at[s])

    def image(s, carry):
        def src(r0, n):
            return x_ref[s, r0:r0 + n]

        def ready(r0, end):
            size, blocks = bh * ww, []
            for k in range(n_row):
                if k * size < end and (k + 1) * size > r0:
                    done.setdefault(k, set()).update(range(max(r0, k * size), min(end, (k + 1) * size)))
                    if len(done[k]) == size:
                        done.pop(k)
                        blocks.append(k)
            return blocks

        done = {}

        def dst(r0, v):
            end, at = r0 + v.shape[0], r0
            while at < end:
                n = min(end, (at // ww + 1) * ww) - at
                yv[s, at // ww, at % ww:at % ww + n] = v[at - r0:at - r0 + n]
                at += n
            for k in ready(r0, end):
                for d in range(n_col):
                    c = lax.rem(me_c + 1 + d, n_col)
                    remote = (k != me_r) | (c != me_c)

                    @pl.when(remote)
                    def _():
                        copy(s, k, c).start()

                    @pl.when(jnp.logical_not(remote))
                    def _():
                        own(s).start()

        def before_last():
            @pl.when(s == 0)
            def _():
                _await_peers(peers)

        @pl.when(s == n_img - 1)
        def _():
            _out_project(x1_ref.at[s], ot_ref, proj_ref, x_ref.at[s], sums_ref.at[s])

        blk.run(src, (sums_ref[s, 0:1], sums_ref[s, 1:2]), me * n_img + s, LAST_CHUNK, before_last, dst,
                me_r < n_row // 2)
        return carry

    lax.fori_loop(0, n_img, image, 0)
    for s in range(n_img):
        for r, c in peers:
            copy(s, r, c).wait()
        own(s).wait()


def _attn_kernel(x_ref, sums_ref, anorm_ref, proj_ref, grp_ref, k_in, q_in, v_in, bound_in,
                 o_ref, osums_ref, k_buf, q_buf, v_buf, bound_ref, ot_buf):
    n_img, n_pos, n_ch = x_ref.shape
    head_dim, scale = HEAD_DIM, LOGIT_SCALE
    n_heads = n_ch // head_dim
    per_blk = 128 // head_dim

    def image(img, carry_img):
        @pl.when(img > 0)
        def _():
            _project(lambda r0, n: x_ref[img, r0:r0 + n], n_pos, (sums_ref[img, 0:1], sums_ref[img, 1:2]),
                     grp_ref[...], anorm_ref, proj_ref, k_buf, q_buf, v_buf, bound_ref)

        top2, v_max = jnp.max(bound_ref[0:1]), jnp.max(bound_ref[1:2])
        small = ((top2 < 96.0 ** 2) & (v_max < 2.0 ** 20)) | ((top2 < 108.0 ** 2) & (v_max < 2.0 ** 8))

        @pl.when(small)
        def _():
            n_kc = n_pos // K_CHUNK

            def heads(b, carry):
                b0 = pl.multiple_of(b * 128, 128)
                tiles = [(j, t * Q_TILE) for j in range(per_blk) for t in range(n_pos // Q_TILE)]
                steps = [(tile, c) for tile in tiles for c in range(n_kc)]

                def score(step):
                    (j, q0), c = step
                    h0 = pl.multiple_of(b0 + j * head_dim, head_dim)
                    keys = k_buf[j, c * K_CHUNK:(c + 1) * K_CHUNK, pl.ds(b0, 128)]
                    return _dot(keys[:, :head_dim], q_buf[pl.ds(h0, head_dim), q0:q0 + Q_TILE])

                pending = [score(s) for s in steps[:AHEAD]]
                tot = out = None
                for n, ((j, q0), c) in enumerate(steps):
                    if n + AHEAD < len(steps):
                        pending.append(score(steps[n + AHEAD]))
                    p = jnp.exp2(pending.pop(0) * scale)
                    h0 = pl.multiple_of(b0 + j * head_dim, head_dim)
                    part = jnp.sum(p.reshape(K_CHUNK // 8, 8, Q_TILE), axis=0)
                    pv = _dot(v_buf[pl.ds(h0, head_dim), c * K_CHUNK:(c + 1) * K_CHUNK], p.astype(BF16))
                    tot, out = (part, pv) if c == 0 else (tot + part, out + pv)
                    if c == n_kc - 1:
                        res = out / jnp.sum(tot, axis=0, keepdims=True)
                        ot_buf[pl.ds(h0, head_dim), q0:q0 + Q_TILE] = res.astype(BF16)
                return carry

            lax.fori_loop(0, n_ch // 128, heads, 0)

        @pl.when(jnp.logical_not(small))
        def _():
            rh = lax.broadcasted_iota(jnp.int32, (128, 256), 0) // head_dim
            n_tiles = n_pos // 256

            def tile(i, carry):
                h = i // n_tiles
                q0 = pl.multiple_of((i % n_tiles) * 256, 256)
                b0 = pl.multiple_of((h // per_blk) * 128, 128)
                h0 = pl.multiple_of(h * head_dim, head_dim)
                qm = jnp.where(rh == h % per_blk, q_buf[pl.ds(b0, 128), pl.ds(q0, 256)], 0)
                s = _dot(k_buf[0, :, pl.ds(b0, 128)], qm)
                p = jnp.exp2((s - jnp.max(s, axis=0, keepdims=True)) * scale)
                o = _dot(v_buf[pl.ds(h0, head_dim), :], p.astype(BF16))
                ot_buf[pl.ds(h0, head_dim), pl.ds(q0, 256)] = (o / jnp.sum(p, axis=0, keepdims=True)).astype(BF16)
                return carry

            lax.fori_loop(0, n_heads * n_tiles, tile, 0)

        @pl.when(img < n_img - 1)
        def _():
            _out_project(x_ref.at[img], ot_buf, proj_ref, o_ref.at[img], osums_ref.at[img])

        return carry_img

    lax.fori_loop(0, n_img, image, 0)


K1_LIMIT, K2_LIMIT, K3_LIMIT = 36, 16, 24


def solution(mesh):
    n_row, n_col = mesh.shape['row'], mesh.shape['col']
    n_dev = n_row * n_col
    vmem, hbm = pl.BlockSpec(memory_space=pltpu.VMEM), pl.BlockSpec(memory_space=pltpu.HBM)

    def run_stage(latent, t_emb, res_norm, res_conv, res_temb, attn_norm, attn_proj):
        n_batch, bh, bw, n_ch = latent.shape
        hh, ww = bh * n_row, bw * n_col
        n_pos, n_img = hh * ww, n_batch // n_dev
        proj = jnp.transpose(attn_proj, (0, 1, 3, 2)).reshape(4, n_ch, n_ch)
        conv_w = res_conv.reshape(2, 2, 9 * n_ch, n_ch)
        images = pltpu.VMEM((n_img, hh, ww, n_ch), BF16)
        act = pltpu.VMEM(((hh + 2) * ww, 3 * n_ch), BF16)
        chan_sums = pltpu.VMEM((8, n_ch), F32)
        remote = [pltpu.SemaphoreType.DMA((n_img, n_dev)), pltpu.SemaphoreType.DMA((n_img, n_dev)),
                  pltpu.SemaphoreType.DMA((n_img,))]
        x_out, sums_out = pltpu.VMEM((n_img, n_pos, n_ch), BF16), pltpu.VMEM((n_img, 8, n_ch), F32)
        qkv_out = [pltpu.VMEM((128 // HEAD_DIM, n_pos, n_ch), BF16), pltpu.VMEM((n_ch, n_pos), BF16),
                   pltpu.VMEM((n_ch, n_pos), BF16), pltpu.VMEM((8, 128), F32)]

        from_hbm = (latent, t_emb, res_norm, conv_w, res_temb, attn_norm, proj)
        x1, sums1, next_w, next_temb, grp, *qkv = pl.pallas_call(
            functools.partial(_first_kernel, n_row, n_col),
            out_shape=[x_out, sums_out, pltpu.VMEM((2, n_ch, 9 * n_ch), BF16), pltpu.VMEM((n_batch, n_ch), F32),
                       pltpu.VMEM((n_ch, n_ch), BF16), *qkv_out],
            in_specs=[hbm] * len(from_hbm),
            out_specs=[vmem] * 9,
            scratch_shapes=[
                images, pltpu.VMEM((4, 9 * n_ch, n_ch), BF16), pltpu.VMEM((2, n_ch, 9 * n_ch), BF16),
                *(pltpu.VMEM(a.shape, BF16) for a in (t_emb, res_norm, res_temb, attn_norm, proj)),
                pltpu.VMEM(latent.shape, BF16), pltpu.VMEM((n_batch, 8, n_ch), F32),
                pltpu.VMEM((n_dev, n_img, 8, n_ch), F32), act, pltpu.VMEM((n_batch, n_ch), F32), chan_sums,
                pltpu.SemaphoreType.DMA((10,)), *remote, pltpu.SemaphoreType.DMA((n_dev,)), pltpu.SemaphoreType.DMA((n_dev,)),
            ],
            compiler_params=pltpu.CompilerParams(collective_id=0, has_side_effects=True, vmem_limit_bytes=K1_LIMIT << 20),
        )(*(pltpu.with_memory_space_constraint(a, pltpu.HBM) for a in from_hbm))

        x2, sums2, _, _, _, _, ot = pl.pallas_call(
            _attn_kernel,
            out_shape=[x_out, sums_out, *qkv_out, pltpu.VMEM((n_ch, n_pos), BF16)],
            in_specs=[vmem] * 9,
            out_specs=[vmem] * 7,
            input_output_aliases={5: 2, 6: 3, 7: 4, 8: 5},
            compiler_params=pltpu.CompilerParams(vmem_limit_bytes=K2_LIMIT << 20),
        )(x1, sums1, attn_norm, proj, grp, *qkv)

        return pl.pallas_call(
            functools.partial(_last_kernel, n_row, n_col),
            out_shape=[pltpu.VMEM(latent.shape, BF16), x_out, sums_out],
            in_specs=[vmem] * 9,
            out_specs=[vmem] * 3,
            input_output_aliases={3: 1, 4: 2},
            scratch_shapes=[images, act, pltpu.VMEM((n_pos, n_ch), BF16), chan_sums, *remote],
            compiler_params=pltpu.CompilerParams(collective_id=1, has_side_effects=True, vmem_limit_bytes=K3_LIMIT << 20),
        )(x1, ot, proj, x2, sums2, res_norm, next_w, next_temb, grp)[0]

    spec_x = P('dp', 'row', 'col', None)
    return jax.shard_map(run_stage, mesh=mesh, in_specs=(spec_x, P('dp', None), P(), P(), P(), P(), P()), out_specs=spec_x, check_vma=False)
```

```python
import functools

import jax
import jax.numpy as jnp
from jax import lax
from jax.experimental import pallas as pl
from jax.experimental.pallas import tpu as pltpu
from jax.sharding import PartitionSpec as P

MESH = pl.DeviceIdType.MESH
GROUPS = 32
EPS = 1e-5
LOG2E = 1.4426950408889634
F32 = jnp.float32
BF16 = jnp.bfloat16
Q_TILE = 512
K_CHUNK = 256
AHEAD = 2
CHUNK = 768
LAST_CHUNK = 512
PROJ_TILE = 256


def _me_and_peers(n_row, n_col):
    me_r, me_c = lax.axis_index('row'), lax.axis_index('col')
    half = n_row // 2

    def other(r, far, core):
        r = lax.rem(r + far * half, n_row)
        return r // half * half + lax.rem(lax.rem(r, half) + core, half)

    order = [(f, k, c) for f, c in ((1, 1), (1, 0), (0, 1), (0, 0)) for k in range(half) if f or c or k]
    return me_r, me_c, [(other(me_r, f, k), lax.rem(me_c + c, n_col)) for f, k, c in order]


def _signal_peers(peers):
    for r, c in peers:
        pl.semaphore_signal(pltpu.get_barrier_semaphore(), inc=1, device_id={'row': r, 'col': c}, device_id_type=MESH)


def _await_peers(peers):
    pl.semaphore_wait(pltpu.get_barrier_semaphore(), len(peers))


def _dot(a, b, dims=((1,), (0,))):
    return lax.dot_general(a, b, (dims, ((), ())), preferred_element_type=F32)


def _chan_sums(v):
    return jnp.sum(v, axis=0, keepdims=True), jnp.sum(v * v, axis=0, keepdims=True)


def _group_matrix(n_ch):
    per = n_ch // GROUPS
    gi = lax.broadcasted_iota(jnp.int32, (n_ch, n_ch), 0) // per
    gj = lax.broadcasted_iota(jnp.int32, (n_ch, n_ch), 1) // per
    return jnp.where(gi == gj, 1.0, 0.0).astype(BF16)


def _moments(s1, s2, grp, count):
    n_ch = s1.shape[1]
    st = jnp.concatenate([s1, s2, jnp.zeros((6, n_ch), F32)], axis=0)
    hi = st.astype(BF16)
    r1 = st - hi.astype(F32)
    mid = r1.astype(BF16)
    lo = (r1 - mid.astype(F32)).astype(BF16)
    parts = _dot(jnp.concatenate([hi.astype(F32), mid.astype(F32), lo.astype(F32)], axis=0).astype(BF16), grp)
    tot = (parts[16:24] + parts[8:16]) + parts[0:8]
    mean = tot[0:1] / count
    var = tot[1:2] / count - mean * mean
    return mean, lax.rsqrt(var + EPS)


def _zero_sums(n_ch):
    return jnp.zeros((1, n_ch), F32), jnp.zeros((1, n_ch), F32)


class _ResBlock:
    def __init__(self, hh, ww, n_ch, rnorm_ref, w_t, act, hid, temb_s, grp_s, sums_s):
        self.hh, self.ww, self.n_ch = hh, ww, n_ch
        self.rnorm_ref, self.w_t, self.act, self.hid = rnorm_ref, w_t, act, hid
        self.temb_s, self.grp_s, self.sums_s = temb_s, grp_s, sums_s
        self.count = float(hh * ww * (n_ch // GROUPS))

    def clear_borders(self):
        zeros = jnp.zeros((self.ww, self.act.shape[1]), BF16)
        self.act[0:self.ww, :] = zeros
        self.act[(self.hh + 1) * self.ww:(self.hh + 2) * self.ww, :] = zeros

    def conv(self, j, src, sums, chunk, epilogue, backward=False):
        ww, n_ch, act = self.ww, self.n_ch, self.act
        mean, inv = _moments(*sums, self.grp_s[...], self.count)
        a_mul = inv * self.rnorm_ref[j, 0:1].astype(F32)
        half_b = 0.5 * (self.rnorm_ref[j, 1:2].astype(F32) - mean * a_mul)
        half_a = 0.5 * a_mul
        edge = jnp.zeros((1, n_ch), BF16)

        def fill(i):
            w = src(i * ww, ww).astype(F32) * half_a + half_b
            a = w * jnp.tanh(w) + w
            d0 = (i + 1) * ww
            act[d0:d0 + ww, 0:n_ch] = pltpu.roll(a, 1, 0).astype(BF16)
            act[d0:d0 + ww, n_ch:2 * n_ch] = a.astype(BF16)
            act[d0:d0 + ww, 2 * n_ch:3 * n_ch] = pltpu.roll(a, ww - 1, 0).astype(BF16)
            act[d0:d0 + 1, 0:n_ch] = edge
            act[d0 + ww - 1:d0 + ww, 2 * n_ch:3 * n_ch] = edge

        n_pos, filled = self.hh * ww, set()

        def fill_for(r0):
            for i in range(max(0, r0 // ww - 1), min(self.hh, (r0 + chunk - 1) // ww + 2)):
                if i not in filled:
                    filled.add(i)
                    fill(i)

        starts = list(range(0, n_pos, chunk))[::-1 if backward else 1]
        fill_for(starts[0])
        s1, s2 = _zero_sums(n_ch)
        for at, r0 in enumerate(starts):
            lhs = jnp.concatenate([act[r0 + dy * ww:r0 + dy * ww + chunk, :] for dy in range(3)], axis=1)
            acc = _dot(self.w_t[j], lhs, ((1,), (1,)))
            for ahead in starts[at + 1:at + 2]:
                fill_for(ahead)
            out = epilogue(r0, acc.T)
            d1, d2 = _chan_sums(out.astype(F32))
            s1, s2 = s1 + d1, s2 + d2
        self.sums_s[0:1] = s1
        self.sums_s[1:2] = s2

    def run(self, src, sums, img, last_chunk, before_last, dst, backward):
        hid, sums_s = self.hid, self.sums_s
        t_row = self.temb_s[pl.ds(img, 1), :]

        def first(r0, acc):
            out = (acc + t_row).astype(BF16)
            hid[r0:r0 + out.shape[0]] = out
            return out

        def second(r0, acc):
            out = (src(r0, acc.shape[0]).astype(F32) + acc).astype(BF16)
            dst(r0, out)
            return out

        self.conv(0, src, sums, CHUNK, first)
        before_last()

        def last(order):
            self.conv(1, lambda r0, n: hid[r0:r0 + n], (sums_s[0:1], sums_s[1:2]), last_chunk, second, order)

        pl.when(backward)(lambda: last(True))
        pl.when(jnp.logical_not(backward))(lambda: last(False))


HEAD_DIM = 32
LOGIT_SCALE = LOG2E * HEAD_DIM ** -0.5


def _project(src, n_pos, sums, grp, anorm_ref, proj_ref, k_buf, q_buf, v_buf, bound_ref):
    n_ch = proj_ref.shape[-1]
    n_heads = n_ch // HEAD_DIM
    mean, inv = _moments(*sums, grp, float(n_pos * (n_ch // GROUPS)))
    a_mul = inv * anorm_ref[0:1].astype(F32)
    b_add = anorm_ref[1:2].astype(F32)
    head_rows = jnp.where(lax.broadcasted_iota(jnp.int32, (16, n_ch), 0)
                          == lax.broadcasted_iota(jnp.int32, (16, n_ch), 1) // HEAD_DIM, 1.0, 0.0).astype(BF16)
    q_top = jnp.zeros((n_heads, PROJ_TILE), F32)
    k_top = jnp.zeros((16, PROJ_TILE), F32)
    v_top = jnp.zeros((1, PROJ_TILE), F32)
    last_k = None
    for r0 in [*range(0, n_pos, PROJ_TILE), None]:
        if r0 is not None:
            tile = slice(r0, r0 + PROJ_TILE)
            g = ((src(r0, PROJ_TILE).astype(F32) - mean) * a_mul + b_add).astype(BF16)
            k = _dot(g, proj_ref[1], ((1,), (1,)))
            q = _dot(proj_ref[0], g, ((1,), (1,))).astype(BF16)
            v = _dot(proj_ref[2], g, ((1,), (1,))).astype(BF16)
            for b0 in range(0, n_ch, 128):
                for j in range(128 // HEAD_DIM):
                    part = k[:, b0:b0 + 128]
                    part = part if j == 0 else pltpu.roll(part, 128 - j * HEAD_DIM, 1)
                    k_buf[j, tile, b0:b0 + 128] = part.astype(BF16)
            k = k.astype(BF16)
            q_buf[:, tile] = q
            v_buf[:, tile] = v
            q = q.astype(F32)
            q_top = jnp.maximum(q_top, jnp.sum((q * q).reshape(n_heads, HEAD_DIM, PROJ_TILE), axis=1))
            v_top = jnp.maximum(v_top, jnp.max(jnp.abs(v.astype(F32)), axis=0, keepdims=True))
        if last_k is not None:
            k2 = last_k.astype(F32) * last_k.astype(F32)
            k_top = jnp.maximum(k_top, _dot(head_rows, k2.astype(BF16), ((1,), (1,))))
        last_k = k
    q_top = jnp.max(q_top, axis=1, keepdims=True)
    k_top = jnp.max(k_top, axis=1, keepdims=True)[:n_heads]
    top2 = jnp.max(q_top * k_top, axis=0, keepdims=True) * (LOGIT_SCALE * LOGIT_SCALE)
    bound_ref[0:1] = jnp.broadcast_to(top2, (1, 128))
    bound_ref[1:2] = jnp.broadcast_to(jnp.max(v_top, axis=1, keepdims=True), (1, 128))


def _out_project(x_ref, ot_ref, proj_ref, o_ref, sums_ref):
    n_pos, n_ch = x_ref.shape
    s1, s2 = _zero_sums(n_ch)
    for r0 in range(0, n_pos, PROJ_TILE):
        tile = slice(r0, r0 + PROJ_TILE)
        acc = _dot(ot_ref[:, tile], proj_ref[3], ((0,), (0,)))
        out = (x_ref[tile].astype(F32) + acc).astype(BF16)
        o_ref[tile] = out
        d1, d2 = _chan_sums(out.astype(F32))
        s1, s2 = s1 + d1, s2 + d2
    sums_ref[0:1] = s1
    sums_ref[1:2] = s2


def _first_kernel(n_row, n_col, lat_ref, temb_hbm, rnorm_hbm, conv_hbm, wtemb_hbm, anorm_hbm, proj_hbm,
                  o_ref, sums_ref, next_w, next_temb, grp_ref, k_buf, q_buf, v_buf, bound_ref,
                  xv, wconv, w_t, temb_v, rnorm_v, wtemb, anorm_v, proj_v, act, temb_s, sums_s,
                  wsem, send_sem, recv_sem, loc_sem):
    me_r, me_c, peers = _me_and_peers(n_row, n_col)
    me = me_r * n_col + me_c
    n_img, hh, ww, n_ch = xv.shape
    n_pos = hh * ww
    bh, bw = hh // n_row, ww // n_col
    weights = [pltpu.make_async_copy(conv_hbm.at[i // 2, i % 2], wconv.at[i], wsem.at[i]) for i in range(4)]
    small = [pltpu.make_async_copy(a, b, wsem.at[4 + i]) for i, (a, b) in enumerate([
        (wtemb_hbm, wtemb), (temb_hbm, temb_v), (rnorm_hbm, rnorm_v), (anorm_hbm, anorm_v), (proj_hbm, proj_v)])]

    def place(s):
        return xv.at[s, pl.ds(me_r * bh, bh), pl.ds(pl.multiple_of(me_c * bw, bw), bw), :]

    def copy(s, k):
        r, c = peers[k]
        return pltpu.make_async_remote_copy(
            lat_ref.at[(r * n_col + c) * n_img + s], place(s), send_sem.at[s, k], recv_sem.at[s, k],
            device_id={'row': r, 'col': c}, device_id_type=MESH)

    def own(s):
        return pltpu.make_async_copy(lat_ref.at[me * n_img + s], place(s), loc_sem.at[s])

    _signal_peers(peers)
    _await_peers(peers)
    for k in range(len(peers)):
        copy(0, k).start()
    for s in range(n_img):
        own(s).start()
    for w in [*small, *weights]:
        w.start()

    blk = _ResBlock(hh, ww, n_ch, rnorm_v.at[0], w_t, act, None, temb_s, grp_ref, sums_s)
    blk.clear_borders()
    grp_ref[...] = _group_matrix(n_ch)
    for w in small:
        w.wait()
    te = temb_v[...].astype(F32)
    t_act = (te * jax.nn.sigmoid(te)).astype(BF16)
    temb_s[...] = _dot(t_act, wtemb[0])
    next_temb[...] = _dot(t_act, wtemb[1])
    for w in weights:
        w.wait()

    def turn(i, carry):
        t0 = pl.multiple_of(i * n_ch, n_ch)
        for j in range(4):
            out = w_t.at[j] if j < 2 else next_w.at[j - 2]
            out[:, pl.ds(t0, n_ch)] = wconv[j, pl.ds(t0, n_ch), :].T
        return carry

    lax.fori_loop(0, 9, turn, 0)
    for s in range(1, n_img):
        for k in range(len(peers)):
            copy(s - 1, k).wait_send()
            copy(s, k).start()

    def half_block(t, carry):
        s, j = t // 2, lax.rem(t, 2)

        @pl.when(t == 2)
        def _():
            _project(lambda r0, n: o_ref[0, r0:r0 + n], n_pos, (sums_ref[0, 0:1], sums_ref[0, 1:2]), grp_ref[...],
                     anorm_v, proj_v, k_buf, q_buf, v_buf, bound_ref)

        @pl.when(j == 0)
        def _():
            for k in range(len(peers)):
                copy(s, k).wait_recv()
            own(s).wait()

            def take(i, sums):
                v = xv[s, pl.ds(i * 4, 4)].reshape(4 * ww, n_ch)
                o_ref[s, pl.ds(pl.multiple_of(i * 4 * ww, 4 * ww), 4 * ww)] = v
                d1, d2 = _chan_sums(v.astype(F32))
                return sums[0] + d1, sums[1] + d2

            s1, s2 = lax.fori_loop(0, hh // 4, take, _zero_sums(n_ch))
            sums_s[0:1] = s1
            sums_s[1:2] = s2

        t_row = temb_s[pl.ds(me * n_img + s, 1), :]

        def epilogue(r0, acc):
            n = acc.shape[0]
            x = xv[s, r0 // ww:(r0 + n) // ww].reshape(n, n_ch).astype(F32)
            out = (acc + jnp.where(j == 0, t_row, x)).astype(BF16)
            o_ref[s, r0:r0 + n] = out
            return out

        blk.conv(j, lambda r0, n: o_ref[s, r0:r0 + n], (sums_s[0:1], sums_s[1:2]), CHUNK, epilogue)
        sums_ref[s] = sums_s[...]
        return carry

    lax.fori_loop(0, 2 * n_img, half_block, 0)
    for k in range(len(peers)):
        copy(n_img - 1, k).wait_send()


def _last_kernel(n_row, n_col, x1_ref, ot_ref, proj_ref, x_in, sums_in, rnorm_ref, w_t, temb_ref, grp_ref,
                 o_ref, x_ref, sums_ref, yv, act, hid, sums_s, send_sem, recv_sem, loc_sem):
    me_r, me_c, peers = _me_and_peers(n_row, n_col)
    me = me_r * n_col + me_c
    n_img, hh, ww, n_ch = yv.shape
    bh, bw = hh // n_row, ww // n_col
    blk = _ResBlock(hh, ww, n_ch, rnorm_ref.at[1], w_t, act, hid, temb_ref, grp_ref, sums_s)
    _signal_peers(peers)
    blk.clear_borders()

    def block(s, k, c):
        return yv.at[s, pl.ds(k * bh, bh), pl.ds(pl.multiple_of(c * bw, bw), bw), :]

    def rel(k, c):
        return lax.rem(k - me_r + n_row, n_row) * n_col + lax.rem(c - me_c + n_col, n_col)

    def copy(s, k, c):
        return pltpu.make_async_remote_copy(
            block(s, k, c), o_ref.at[me * n_img + s], send_sem.at[s, rel(k, c)], recv_sem.at[s, rel(k, c)],
            device_id={'row': k, 'col': c}, device_id_type=MESH)

    def own(s):
        return pltpu.make_async_copy(block(s, me_r, me_c), o_ref.at[me * n_img + s], loc_sem.at[s])

    def image(s, carry):
        def src(r0, n):
            return x_ref[s, r0:r0 + n]

        def ready(r0, end):
            size, blocks = bh * ww, []
            for k in range(n_row):
                if k * size < end and (k + 1) * size > r0:
                    done.setdefault(k, set()).update(range(max(r0, k * size), min(end, (k + 1) * size)))
                    if len(done[k]) == size:
                        done.pop(k)
                        blocks.append(k)
            return blocks

        done = {}

        def dst(r0, v):
            end, at = r0 + v.shape[0], r0
            while at < end:
                n = min(end, (at // ww + 1) * ww) - at
                yv[s, at // ww, at % ww:at % ww + n] = v[at - r0:at - r0 + n]
                at += n
            for k in ready(r0, end):
                for d in range(n_col):
                    c = lax.rem(me_c + 1 + d, n_col)
                    remote = (k != me_r) | (c != me_c)

                    @pl.when(remote)
                    def _():
                        copy(s, k, c).start()

                    @pl.when(jnp.logical_not(remote))
                    def _():
                        own(s).start()

        def before_last():
            @pl.when(s == 0)
            def _():
                _await_peers(peers)

        @pl.when(s == n_img - 1)
        def _():
            _out_project(x1_ref.at[s], ot_ref, proj_ref, x_ref.at[s], sums_ref.at[s])

        blk.run(src, (sums_ref[s, 0:1], sums_ref[s, 1:2]), me * n_img + s, LAST_CHUNK, before_last, dst,
                me_r < n_row // 2)
        return carry

    lax.fori_loop(0, n_img, image, 0)
    for s in range(n_img):
        for r, c in peers:
            copy(s, r, c).wait()
        own(s).wait()


def _attn_kernel(x_ref, sums_ref, anorm_ref, proj_ref, grp_ref, k_in, q_in, v_in, bound_in,
                 o_ref, osums_ref, k_buf, q_buf, v_buf, bound_ref, ot_buf):
    n_img, n_pos, n_ch = x_ref.shape
    head_dim, scale = HEAD_DIM, LOGIT_SCALE
    n_heads = n_ch // head_dim
    per_blk = 128 // head_dim

    def image(img, carry_img):
        @pl.when(img > 0)
        def _():
            _project(lambda r0, n: x_ref[img, r0:r0 + n], n_pos, (sums_ref[img, 0:1], sums_ref[img, 1:2]),
                     grp_ref[...], anorm_ref, proj_ref, k_buf, q_buf, v_buf, bound_ref)

        top2, v_max = jnp.max(bound_ref[0:1]), jnp.max(bound_ref[1:2])
        small = ((top2 < 96.0 ** 2) & (v_max < 2.0 ** 20)) | ((top2 < 108.0 ** 2) & (v_max < 2.0 ** 8))

        @pl.when(small)
        def _():
            n_kc = n_pos // K_CHUNK

            def heads(b, carry):
                b0 = pl.multiple_of(b * 128, 128)
                tiles = [(j, t * Q_TILE) for j in range(per_blk) for t in range(n_pos // Q_TILE)]
                steps = [(tile, c) for tile in tiles for c in range(n_kc)]

                def score(step):
                    (j, q0), c = step
                    h0 = pl.multiple_of(b0 + j * head_dim, head_dim)
                    keys = k_buf[j, c * K_CHUNK:(c + 1) * K_CHUNK, pl.ds(b0, 128)]
                    return _dot(keys[:, :head_dim], q_buf[pl.ds(h0, head_dim), q0:q0 + Q_TILE])

                pending = [score(s) for s in steps[:AHEAD]]
                tot = out = None
                for n, ((j, q0), c) in enumerate(steps):
                    if n + AHEAD < len(steps):
                        pending.append(score(steps[n + AHEAD]))
                    p = jnp.exp2(pending.pop(0) * scale)
                    h0 = pl.multiple_of(b0 + j * head_dim, head_dim)
                    part = jnp.sum(p.reshape(K_CHUNK // 8, 8, Q_TILE), axis=0)
                    pv = _dot(v_buf[pl.ds(h0, head_dim), c * K_CHUNK:(c + 1) * K_CHUNK], p.astype(BF16))
                    tot, out = (part, pv) if c == 0 else (tot + part, out + pv)
                    if c == n_kc - 1:
                        res = out / jnp.sum(tot, axis=0, keepdims=True)
                        ot_buf[pl.ds(h0, head_dim), q0:q0 + Q_TILE] = res.astype(BF16)
                return carry

            lax.fori_loop(0, n_ch // 128, heads, 0)

        @pl.when(jnp.logical_not(small))
        def _():
            rh = lax.broadcasted_iota(jnp.int32, (128, 256), 0) // head_dim
            n_tiles = n_pos // 256

            def tile(i, carry):
                h = i // n_tiles
                q0 = pl.multiple_of((i % n_tiles) * 256, 256)
                b0 = pl.multiple_of((h // per_blk) * 128, 128)
                h0 = pl.multiple_of(h * head_dim, head_dim)
                qm = jnp.where(rh == h % per_blk, q_buf[pl.ds(b0, 128), pl.ds(q0, 256)], 0)
                s = _dot(k_buf[0, :, pl.ds(b0, 128)], qm)
                p = jnp.exp2((s - jnp.max(s, axis=0, keepdims=True)) * scale)
                o = _dot(v_buf[pl.ds(h0, head_dim), :], p.astype(BF16))
                ot_buf[pl.ds(h0, head_dim), pl.ds(q0, 256)] = (o / jnp.sum(p, axis=0, keepdims=True)).astype(BF16)
                return carry

            lax.fori_loop(0, n_heads * n_tiles, tile, 0)

        @pl.when(img < n_img - 1)
        def _():
            _out_project(x_ref.at[img], ot_buf, proj_ref, o_ref.at[img], osums_ref.at[img])

        return carry_img

    lax.fori_loop(0, n_img, image, 0)


K1_LIMIT, K2_LIMIT, K3_LIMIT = 36, 16, 24


def solution(mesh):
    n_row, n_col = mesh.shape['row'], mesh.shape['col']
    n_dev = n_row * n_col
    vmem, hbm = pl.BlockSpec(memory_space=pltpu.VMEM), pl.BlockSpec(memory_space=pltpu.HBM)

    def run_stage(latent, t_emb, res_norm, res_conv, res_temb, attn_norm, attn_proj):
        n_batch, bh, bw, n_ch = latent.shape
        hh, ww = bh * n_row, bw * n_col
        n_pos, n_img = hh * ww, n_batch // n_dev
        proj = jnp.transpose(attn_proj, (0, 1, 3, 2)).reshape(4, n_ch, n_ch)
        conv_w = res_conv.reshape(2, 2, 9 * n_ch, n_ch)
        images = pltpu.VMEM((n_img, hh, ww, n_ch), BF16)
        act = pltpu.VMEM(((hh + 2) * ww, 3 * n_ch), BF16)
        chan_sums = pltpu.VMEM((8, n_ch), F32)
        remote = [pltpu.SemaphoreType.DMA((n_img, n_dev)), pltpu.SemaphoreType.DMA((n_img, n_dev)),
                  pltpu.SemaphoreType.DMA((n_img,))]
        x_out, sums_out = pltpu.VMEM((n_img, n_pos, n_ch), BF16), pltpu.VMEM((n_img, 8, n_ch), F32)
        qkv_out = [pltpu.VMEM((128 // HEAD_DIM, n_pos, n_ch), BF16), pltpu.VMEM((n_ch, n_pos), BF16),
                   pltpu.VMEM((n_ch, n_pos), BF16), pltpu.VMEM((8, 128), F32)]

        from_hbm = (latent, t_emb, res_norm, conv_w, res_temb, attn_norm, proj)
        x1, sums1, next_w, next_temb, grp, *qkv = pl.pallas_call(
            functools.partial(_first_kernel, n_row, n_col),
            out_shape=[x_out, sums_out, pltpu.VMEM((2, n_ch, 9 * n_ch), BF16), pltpu.VMEM((n_batch, n_ch), F32),
                       pltpu.VMEM((n_ch, n_ch), BF16), *qkv_out],
            in_specs=[hbm] * len(from_hbm),
            out_specs=[vmem] * 9,
            scratch_shapes=[
                images, pltpu.VMEM((4, 9 * n_ch, n_ch), BF16), pltpu.VMEM((2, n_ch, 9 * n_ch), BF16),
                *(pltpu.VMEM(a.shape, BF16) for a in (t_emb, res_norm, res_temb, attn_norm, proj)),
                act, pltpu.VMEM((n_batch, n_ch), F32), chan_sums, pltpu.SemaphoreType.DMA((9,)), *remote,
            ],
            compiler_params=pltpu.CompilerParams(collective_id=0, has_side_effects=True, vmem_limit_bytes=K1_LIMIT << 20),
        )(*(pltpu.with_memory_space_constraint(a, pltpu.HBM) for a in from_hbm))

        x2, sums2, _, _, _, _, ot = pl.pallas_call(
            _attn_kernel,
            out_shape=[x_out, sums_out, *qkv_out, pltpu.VMEM((n_ch, n_pos), BF16)],
            in_specs=[vmem] * 9,
            out_specs=[vmem] * 7,
            input_output_aliases={5: 2, 6: 3, 7: 4, 8: 5},
            compiler_params=pltpu.CompilerParams(vmem_limit_bytes=K2_LIMIT << 20),
        )(x1, sums1, attn_norm, proj, grp, *qkv)

        return pl.pallas_call(
            functools.partial(_last_kernel, n_row, n_col),
            out_shape=[pltpu.VMEM(latent.shape, BF16), x_out, sums_out],
            in_specs=[vmem] * 9,
            out_specs=[vmem] * 3,
            input_output_aliases={3: 1, 4: 2},
            scratch_shapes=[images, act, pltpu.VMEM((n_pos, n_ch), BF16), chan_sums, *remote],
            compiler_params=pltpu.CompilerParams(collective_id=1, has_side_effects=True, vmem_limit_bytes=K3_LIMIT << 20),
        )(x1, ot, proj, x2, sums2, res_norm, next_w, next_temb, grp)[0]

    spec_x = P('dp', 'row', 'col', None)
    return jax.shard_map(run_stage, mesh=mesh, in_specs=(spec_x, P('dp', None), P(), P(), P(), P(), P()), out_specs=spec_x, check_vma=False)
```

```python
import functools

import jax
import jax.numpy as jnp
from jax import lax
from jax.experimental import pallas as pl
from jax.experimental.pallas import tpu as pltpu
from jax.sharding import PartitionSpec as P

MESH = pl.DeviceIdType.MESH
GROUPS = 32
EPS = 1e-5
LOG2E = 1.4426950408889634
F32 = jnp.float32
BF16 = jnp.bfloat16
Q_TILE = 512
K_CHUNK = 128
AHEAD = 3
CHUNK = 768
LAST_CHUNK = 512
PROJ_TILE = 256


def _me_and_peers(n_row, n_col):
    me_r, me_c = lax.axis_index('row'), lax.axis_index('col')
    half = n_row // 2

    def other(r, far, core):
        r = lax.rem(r + far * half, n_row)
        return r // half * half + lax.rem(lax.rem(r, half) + core, half)

    order = [(f, k, c) for f, c in ((1, 1), (1, 0), (0, 1), (0, 0)) for k in range(half) if f or c or k]
    return me_r, me_c, [(other(me_r, f, k), lax.rem(me_c + c, n_col)) for f, k, c in order]


def _signal_peers(peers):
    for r, c in peers:
        pl.semaphore_signal(pltpu.get_barrier_semaphore(), inc=1, device_id={'row': r, 'col': c}, device_id_type=MESH)


def _await_peers(peers):
    pl.semaphore_wait(pltpu.get_barrier_semaphore(), len(peers))


def _dot(a, b, dims=((1,), (0,))):
    return lax.dot_general(a, b, (dims, ((), ())), preferred_element_type=F32)


def _chan_sums(v):
    return jnp.sum(v, axis=0, keepdims=True), jnp.sum(v * v, axis=0, keepdims=True)


def _group_matrix(n_ch):
    per = n_ch // GROUPS
    gi = lax.broadcasted_iota(jnp.int32, (n_ch, n_ch), 0) // per
    gj = lax.broadcasted_iota(jnp.int32, (n_ch, n_ch), 1) // per
    return jnp.where(gi == gj, 1.0, 0.0).astype(BF16)


def _moments(s1, s2, grp, count):
    n_ch = s1.shape[1]
    st = jnp.concatenate([s1, s2, jnp.zeros((6, n_ch), F32)], axis=0)
    hi = st.astype(BF16)
    r1 = st - hi.astype(F32)
    mid = r1.astype(BF16)
    lo = (r1 - mid.astype(F32)).astype(BF16)
    parts = _dot(jnp.concatenate([hi.astype(F32), mid.astype(F32), lo.astype(F32)], axis=0).astype(BF16), grp)
    tot = (parts[16:24] + parts[8:16]) + parts[0:8]
    mean = tot[0:1] / count
    var = tot[1:2] / count - mean * mean
    return mean, lax.rsqrt(var + EPS)


def _zero_sums(n_ch):
    return jnp.zeros((1, n_ch), F32), jnp.zeros((1, n_ch), F32)


class _ResBlock:
    def __init__(self, hh, ww, n_ch, rnorm_ref, w_t, act, hid, temb_s, grp_s, sums_s):
        self.hh, self.ww, self.n_ch = hh, ww, n_ch
        self.rnorm_ref, self.w_t, self.act, self.hid = rnorm_ref, w_t, act, hid
        self.temb_s, self.grp_s, self.sums_s = temb_s, grp_s, sums_s
        self.count = float(hh * ww * (n_ch // GROUPS))

    def clear_borders(self):
        zeros = jnp.zeros((self.ww, self.act.shape[1]), BF16)
        self.act[0:self.ww, :] = zeros
        self.act[(self.hh + 1) * self.ww:(self.hh + 2) * self.ww, :] = zeros

    def conv(self, j, src, sums, chunk, epilogue, backward=False):
        ww, n_ch, act = self.ww, self.n_ch, self.act
        mean, inv = _moments(*sums, self.grp_s[...], self.count)
        a_mul = inv * self.rnorm_ref[j, 0:1].astype(F32)
        half_b = 0.5 * (self.rnorm_ref[j, 1:2].astype(F32) - mean * a_mul)
        half_a = 0.5 * a_mul
        edge = jnp.zeros((1, n_ch), BF16)

        def fill(i):
            w = src(i * ww, ww).astype(F32) * half_a + half_b
            a = w * jnp.tanh(w) + w
            d0 = (i + 1) * ww
            act[d0:d0 + ww, 0:n_ch] = pltpu.roll(a, 1, 0).astype(BF16)
            act[d0:d0 + ww, n_ch:2 * n_ch] = a.astype(BF16)
            act[d0:d0 + ww, 2 * n_ch:3 * n_ch] = pltpu.roll(a, ww - 1, 0).astype(BF16)
            act[d0:d0 + 1, 0:n_ch] = edge
            act[d0 + ww - 1:d0 + ww, 2 * n_ch:3 * n_ch] = edge

        n_pos, filled = self.hh * ww, set()

        def fill_for(r0):
            for i in range(max(0, r0 // ww - 1), min(self.hh, (r0 + chunk - 1) // ww + 2)):
                if i not in filled:
                    filled.add(i)
                    fill(i)

        starts = list(range(0, n_pos, chunk))[::-1 if backward else 1]
        fill_for(starts[0])
        s1, s2 = _zero_sums(n_ch)
        for at, r0 in enumerate(starts):
            lhs = jnp.concatenate([act[r0 + dy * ww:r0 + dy * ww + chunk, :] for dy in range(3)], axis=1)
            acc = _dot(self.w_t[j], lhs, ((1,), (1,)))
            for ahead in starts[at + 1:at + 2]:
                fill_for(ahead)
            out = epilogue(r0, acc.T)
            d1, d2 = _chan_sums(out.astype(F32))
            s1, s2 = s1 + d1, s2 + d2
        self.sums_s[0:1] = s1
        self.sums_s[1:2] = s2

    def run(self, src, sums, img, last_chunk, before_last, dst, backward):
        hid, sums_s = self.hid, self.sums_s
        t_row = self.temb_s[pl.ds(img, 1), :]

        def first(r0, acc):
            out = (acc + t_row).astype(BF16)
            hid[r0:r0 + out.shape[0]] = out
            return out

        def second(r0, acc):
            out = (src(r0, acc.shape[0]).astype(F32) + acc).astype(BF16)
            dst(r0, out)
            return out

        self.conv(0, src, sums, CHUNK, first)
        before_last()

        def last(order):
            self.conv(1, lambda r0, n: hid[r0:r0 + n], (sums_s[0:1], sums_s[1:2]), last_chunk, second, order)

        pl.when(backward)(lambda: last(True))
        pl.when(jnp.logical_not(backward))(lambda: last(False))


HEAD_DIM = 32
LOGIT_SCALE = LOG2E * HEAD_DIM ** -0.5


def _project(src, n_pos, sums, grp, anorm_ref, proj_ref, k_buf, q_buf, v_buf, bound_ref):
    n_ch = proj_ref.shape[-1]
    n_heads = n_ch // HEAD_DIM
    mean, inv = _moments(*sums, grp, float(n_pos * (n_ch // GROUPS)))
    a_mul = inv * anorm_ref[0:1].astype(F32)
    b_add = anorm_ref[1:2].astype(F32)
    head_rows = jnp.where(lax.broadcasted_iota(jnp.int32, (16, n_ch), 0)
                          == lax.broadcasted_iota(jnp.int32, (16, n_ch), 1) // HEAD_DIM, 1.0, 0.0).astype(BF16)
    q_top = jnp.zeros((n_heads, PROJ_TILE), F32)
    k_top = jnp.zeros((16, PROJ_TILE), F32)
    v_top = jnp.zeros((1, PROJ_TILE), F32)
    last_k = None
    for r0 in [*range(0, n_pos, PROJ_TILE), None]:
        if r0 is not None:
            tile = slice(r0, r0 + PROJ_TILE)
            g = ((src(r0, PROJ_TILE).astype(F32) - mean) * a_mul + b_add).astype(BF16)
            k = _dot(g, proj_ref[1], ((1,), (1,)))
            q = _dot(proj_ref[0], g, ((1,), (1,))).astype(BF16)
            v = _dot(proj_ref[2], g, ((1,), (1,))).astype(BF16)
            for b0 in range(0, n_ch, 128):
                for j in range(128 // HEAD_DIM):
                    part = k[:, b0:b0 + 128]
                    part = part if j == 0 else pltpu.roll(part, 128 - j * HEAD_DIM, 1)
                    k_buf[j, tile, b0:b0 + 128] = part.astype(BF16)
            k = k.astype(BF16)
            q_buf[:, tile] = q
            v_buf[:, tile] = v
            q = q.astype(F32)
            q_top = jnp.maximum(q_top, jnp.sum((q * q).reshape(n_heads, HEAD_DIM, PROJ_TILE), axis=1))
            v_top = jnp.maximum(v_top, jnp.max(jnp.abs(v.astype(F32)), axis=0, keepdims=True))
        if last_k is not None:
            k2 = last_k.astype(F32) * last_k.astype(F32)
            k_top = jnp.maximum(k_top, _dot(head_rows, k2.astype(BF16), ((1,), (1,))))
        last_k = k
    q_top = jnp.max(q_top, axis=1, keepdims=True)
    k_top = jnp.max(k_top, axis=1, keepdims=True)[:n_heads]
    top2 = jnp.max(q_top * k_top, axis=0, keepdims=True) * (LOGIT_SCALE * LOGIT_SCALE)
    bound_ref[0:1] = jnp.broadcast_to(top2, (1, 128))
    bound_ref[1:2] = jnp.broadcast_to(jnp.max(v_top, axis=1, keepdims=True), (1, 128))


def _out_project(x_ref, ot_ref, proj_ref, o_ref, sums_ref):
    n_pos, n_ch = x_ref.shape
    s1, s2 = _zero_sums(n_ch)
    for r0 in range(0, n_pos, PROJ_TILE):
        tile = slice(r0, r0 + PROJ_TILE)
        acc = _dot(ot_ref[:, tile], proj_ref[3], ((0,), (0,)))
        out = (x_ref[tile].astype(F32) + acc).astype(BF16)
        o_ref[tile] = out
        d1, d2 = _chan_sums(out.astype(F32))
        s1, s2 = s1 + d1, s2 + d2
    sums_ref[0:1] = s1
    sums_ref[1:2] = s2


def _first_kernel(n_row, n_col, lat_ref, temb_hbm, rnorm_hbm, conv_hbm, wtemb_hbm, anorm_hbm, proj_hbm,
                  o_ref, sums_ref, next_w, next_temb, grp_ref, k_buf, q_buf, v_buf, bound_ref,
                  xv, wconv, w_t, temb_v, rnorm_v, wtemb, anorm_v, proj_v, act, temb_s, sums_s,
                  wsem, send_sem, recv_sem, loc_sem):
    me_r, me_c, peers = _me_and_peers(n_row, n_col)
    me = me_r * n_col + me_c
    n_img, hh, ww, n_ch = xv.shape
    n_pos = hh * ww
    bh, bw = hh // n_row, ww // n_col
    weights = [pltpu.make_async_copy(conv_hbm.at[i // 2, i % 2], wconv.at[i], wsem.at[i]) for i in range(4)]
    small = [pltpu.make_async_copy(a, b, wsem.at[4 + i]) for i, (a, b) in enumerate([
        (wtemb_hbm, wtemb), (temb_hbm, temb_v), (rnorm_hbm, rnorm_v), (anorm_hbm, anorm_v), (proj_hbm, proj_v)])]

    def place(s):
        return xv.at[s, pl.ds(me_r * bh, bh), pl.ds(pl.multiple_of(me_c * bw, bw), bw), :]

    def copy(s, k):
        r, c = peers[k]
        return pltpu.make_async_remote_copy(
            lat_ref.at[(r * n_col + c) * n_img + s], place(s), send_sem.at[s, k], recv_sem.at[s, k],
            device_id={'row': r, 'col': c}, device_id_type=MESH)

    def own(s):
        return pltpu.make_async_copy(lat_ref.at[me * n_img + s], place(s), loc_sem.at[s])

    _signal_peers(peers)
    _await_peers(peers)
    for k in range(len(peers)):
        copy(0, k).start()
    for s in range(n_img):
        own(s).start()
    for w in [*small, *weights]:
        w.start()

    blk = _ResBlock(hh, ww, n_ch, rnorm_v.at[0], w_t, act, None, temb_s, grp_ref, sums_s)
    blk.clear_borders()
    grp_ref[...] = _group_matrix(n_ch)
    for w in small:
        w.wait()
    te = temb_v[...].astype(F32)
    t_act = (te * jax.nn.sigmoid(te)).astype(BF16)
    temb_s[...] = _dot(t_act, wtemb[0])
    next_temb[...] = _dot(t_act, wtemb[1])
    for w in weights:
        w.wait()

    def turn(i, carry):
        t0 = pl.multiple_of(i * n_ch, n_ch)
        for j in range(4):
            out = w_t.at[j] if j < 2 else next_w.at[j - 2]
            out[:, pl.ds(t0, n_ch)] = wconv[j, pl.ds(t0, n_ch), :].T
        return carry

    lax.fori_loop(0, 9, turn, 0)
    for s in range(1, n_img):
        for k in range(len(peers)):
            copy(s - 1, k).wait_send()
            copy(s, k).start()

    def half_block(t, carry):
        s, j = t // 2, lax.rem(t, 2)

        @pl.when(t == 2)
        def _():
            _project(lambda r0, n: o_ref[0, r0:r0 + n], n_pos, (sums_ref[0, 0:1], sums_ref[0, 1:2]), grp_ref[...],
                     anorm_v, proj_v, k_buf, q_buf, v_buf, bound_ref)

        @pl.when(j == 0)
        def _():
            for k in range(len(peers)):
                copy(s, k).wait_recv()
            own(s).wait()

            def take(i, sums):
                v = xv[s, pl.ds(i * 4, 4)].reshape(4 * ww, n_ch)
                o_ref[s, pl.ds(pl.multiple_of(i * 4 * ww, 4 * ww), 4 * ww)] = v
                d1, d2 = _chan_sums(v.astype(F32))
                return sums[0] + d1, sums[1] + d2

            s1, s2 = lax.fori_loop(0, hh // 4, take, _zero_sums(n_ch))
            sums_s[0:1] = s1
            sums_s[1:2] = s2

        t_row = temb_s[pl.ds(me * n_img + s, 1), :]

        def epilogue(r0, acc):
            n = acc.shape[0]
            x = xv[s, r0 // ww:(r0 + n) // ww].reshape(n, n_ch).astype(F32)
            out = (acc + jnp.where(j == 0, t_row, x)).astype(BF16)
            o_ref[s, r0:r0 + n] = out
            return out

        blk.conv(j, lambda r0, n: o_ref[s, r0:r0 + n], (sums_s[0:1], sums_s[1:2]), CHUNK, epilogue)
        sums_ref[s] = sums_s[...]
        return carry

    lax.fori_loop(0, 2 * n_img, half_block, 0)
    for k in range(len(peers)):
        copy(n_img - 1, k).wait_send()


def _last_kernel(n_row, n_col, x1_ref, ot_ref, proj_ref, x_in, sums_in, rnorm_ref, w_t, temb_ref, grp_ref,
                 o_ref, x_ref, sums_ref, yv, act, hid, sums_s, send_sem, recv_sem, loc_sem):
    me_r, me_c, peers = _me_and_peers(n_row, n_col)
    me = me_r * n_col + me_c
    n_img, hh, ww, n_ch = yv.shape
    bh, bw = hh // n_row, ww // n_col
    blk = _ResBlock(hh, ww, n_ch, rnorm_ref.at[1], w_t, act, hid, temb_ref, grp_ref, sums_s)
    _signal_peers(peers)
    blk.clear_borders()

    def block(s, k, c):
        return yv.at[s, pl.ds(k * bh, bh), pl.ds(pl.multiple_of(c * bw, bw), bw), :]

    def rel(k, c):
        return lax.rem(k - me_r + n_row, n_row) * n_col + lax.rem(c - me_c + n_col, n_col)

    def copy(s, k, c):
        return pltpu.make_async_remote_copy(
            block(s, k, c), o_ref.at[me * n_img + s], send_sem.at[s, rel(k, c)], recv_sem.at[s, rel(k, c)],
            device_id={'row': k, 'col': c}, device_id_type=MESH)

    def own(s):
        return pltpu.make_async_copy(block(s, me_r, me_c), o_ref.at[me * n_img + s], loc_sem.at[s])

    def image(s, carry):
        def src(r0, n):
            return x_ref[s, r0:r0 + n]

        def ready(r0, end):
            size, blocks = bh * ww, []
            for k in range(n_row):
                if k * size < end and (k + 1) * size > r0:
                    done.setdefault(k, set()).update(range(max(r0, k * size), min(end, (k + 1) * size)))
                    if len(done[k]) == size:
                        done.pop(k)
                        blocks.append(k)
            return blocks

        done = {}

        def dst(r0, v):
            end, at = r0 + v.shape[0], r0
            while at < end:
                n = min(end, (at // ww + 1) * ww) - at
                yv[s, at // ww, at % ww:at % ww + n] = v[at - r0:at - r0 + n]
                at += n
            for k in ready(r0, end):
                for d in range(n_col):
                    c = lax.rem(me_c + 1 + d, n_col)
                    remote = (k != me_r) | (c != me_c)

                    @pl.when(remote)
                    def _():
                        copy(s, k, c).start()

                    @pl.when(jnp.logical_not(remote))
                    def _():
                        own(s).start()

        def before_last():
            @pl.when(s == 0)
            def _():
                _await_peers(peers)

        @pl.when(s == n_img - 1)
        def _():
            _out_project(x1_ref.at[s], ot_ref, proj_ref, x_ref.at[s], sums_ref.at[s])

        blk.run(src, (sums_ref[s, 0:1], sums_ref[s, 1:2]), me * n_img + s, LAST_CHUNK, before_last, dst,
                me_r < n_row // 2)
        return carry

    lax.fori_loop(0, n_img, image, 0)
    for s in range(n_img):
        for r, c in peers:
            copy(s, r, c).wait()
        own(s).wait()


def _attn_kernel(x_ref, sums_ref, anorm_ref, proj_ref, grp_ref, k_in, q_in, v_in, bound_in,
                 o_ref, osums_ref, k_buf, q_buf, v_buf, bound_ref, ot_buf):
    n_img, n_pos, n_ch = x_ref.shape
    head_dim, scale = HEAD_DIM, LOGIT_SCALE
    n_heads = n_ch // head_dim
    per_blk = 128 // head_dim

    def image(img, carry_img):
        @pl.when(img > 0)
        def _():
            _project(lambda r0, n: x_ref[img, r0:r0 + n], n_pos, (sums_ref[img, 0:1], sums_ref[img, 1:2]),
                     grp_ref[...], anorm_ref, proj_ref, k_buf, q_buf, v_buf, bound_ref)

        top2, v_max = jnp.max(bound_ref[0:1]), jnp.max(bound_ref[1:2])
        small = ((top2 < 96.0 ** 2) & (v_max < 2.0 ** 20)) | ((top2 < 108.0 ** 2) & (v_max < 2.0 ** 8))

        @pl.when(small)
        def _():
            n_kc = n_pos // K_CHUNK

            def heads(b, carry):
                b0 = pl.multiple_of(b * 128, 128)
                tiles = [(j, t * Q_TILE) for j in range(per_blk) for t in range(n_pos // Q_TILE)]
                steps = [(tile, c) for tile in tiles for c in range(n_kc)]

                def score(step):
                    (j, q0), c = step
                    h0 = pl.multiple_of(b0 + j * head_dim, head_dim)
                    keys = k_buf[j, c * K_CHUNK:(c + 1) * K_CHUNK, pl.ds(b0, 128)]
                    return _dot(keys[:, :head_dim], q_buf[pl.ds(h0, head_dim), q0:q0 + Q_TILE])

                pending = [score(s) for s in steps[:AHEAD]]
                tot = out = None
                for n, ((j, q0), c) in enumerate(steps):
                    if n + AHEAD < len(steps):
                        pending.append(score(steps[n + AHEAD]))
                    p = jnp.exp2(pending.pop(0) * scale)
                    h0 = pl.multiple_of(b0 + j * head_dim, head_dim)
                    part = jnp.sum(p.reshape(K_CHUNK // 8, 8, Q_TILE), axis=0)
                    pv = _dot(v_buf[pl.ds(h0, head_dim), c * K_CHUNK:(c + 1) * K_CHUNK], p.astype(BF16))
                    tot, out = (part, pv) if c == 0 else (tot + part, out + pv)
                    if c == n_kc - 1:
                        res = out / jnp.sum(tot, axis=0, keepdims=True)
                        ot_buf[pl.ds(h0, head_dim), q0:q0 + Q_TILE] = res.astype(BF16)
                return carry

            lax.fori_loop(0, n_ch // 128, heads, 0)

        @pl.when(jnp.logical_not(small))
        def _():
            rh = lax.broadcasted_iota(jnp.int32, (128, 256), 0) // head_dim
            n_tiles = n_pos // 256

            def tile(i, carry):
                h = i // n_tiles
                q0 = pl.multiple_of((i % n_tiles) * 256, 256)
                b0 = pl.multiple_of((h // per_blk) * 128, 128)
                h0 = pl.multiple_of(h * head_dim, head_dim)
                qm = jnp.where(rh == h % per_blk, q_buf[pl.ds(b0, 128), pl.ds(q0, 256)], 0)
                s = _dot(k_buf[0, :, pl.ds(b0, 128)], qm)
                p = jnp.exp2((s - jnp.max(s, axis=0, keepdims=True)) * scale)
                o = _dot(v_buf[pl.ds(h0, head_dim), :], p.astype(BF16))
                ot_buf[pl.ds(h0, head_dim), pl.ds(q0, 256)] = (o / jnp.sum(p, axis=0, keepdims=True)).astype(BF16)
                return carry

            lax.fori_loop(0, n_heads * n_tiles, tile, 0)

        @pl.when(img < n_img - 1)
        def _():
            _out_project(x_ref.at[img], ot_buf, proj_ref, o_ref.at[img], osums_ref.at[img])

        return carry_img

    lax.fori_loop(0, n_img, image, 0)


K1_LIMIT, K2_LIMIT, K3_LIMIT = 36, 16, 24


def solution(mesh):
    n_row, n_col = mesh.shape['row'], mesh.shape['col']
    n_dev = n_row * n_col
    vmem, hbm = pl.BlockSpec(memory_space=pltpu.VMEM), pl.BlockSpec(memory_space=pltpu.HBM)

    def run_stage(latent, t_emb, res_norm, res_conv, res_temb, attn_norm, attn_proj):
        n_batch, bh, bw, n_ch = latent.shape
        hh, ww = bh * n_row, bw * n_col
        n_pos, n_img = hh * ww, n_batch // n_dev
        proj = jnp.transpose(attn_proj, (0, 1, 3, 2)).reshape(4, n_ch, n_ch)
        conv_w = res_conv.reshape(2, 2, 9 * n_ch, n_ch)
        images = pltpu.VMEM((n_img, hh, ww, n_ch), BF16)
        act = pltpu.VMEM(((hh + 2) * ww, 3 * n_ch), BF16)
        chan_sums = pltpu.VMEM((8, n_ch), F32)
        remote = [pltpu.SemaphoreType.DMA((n_img, n_dev)), pltpu.SemaphoreType.DMA((n_img, n_dev)),
                  pltpu.SemaphoreType.DMA((n_img,))]
        x_out, sums_out = pltpu.VMEM((n_img, n_pos, n_ch), BF16), pltpu.VMEM((n_img, 8, n_ch), F32)
        qkv_out = [pltpu.VMEM((128 // HEAD_DIM, n_pos, n_ch), BF16), pltpu.VMEM((n_ch, n_pos), BF16),
                   pltpu.VMEM((n_ch, n_pos), BF16), pltpu.VMEM((8, 128), F32)]

        from_hbm = (latent, t_emb, res_norm, conv_w, res_temb, attn_norm, proj)
        x1, sums1, next_w, next_temb, grp, *qkv = pl.pallas_call(
            functools.partial(_first_kernel, n_row, n_col),
            out_shape=[x_out, sums_out, pltpu.VMEM((2, n_ch, 9 * n_ch), BF16), pltpu.VMEM((n_batch, n_ch), F32),
                       pltpu.VMEM((n_ch, n_ch), BF16), *qkv_out],
            in_specs=[hbm] * len(from_hbm),
            out_specs=[vmem] * 9,
            scratch_shapes=[
                images, pltpu.VMEM((4, 9 * n_ch, n_ch), BF16), pltpu.VMEM((2, n_ch, 9 * n_ch), BF16),
                *(pltpu.VMEM(a.shape, BF16) for a in (t_emb, res_norm, res_temb, attn_norm, proj)),
                act, pltpu.VMEM((n_batch, n_ch), F32), chan_sums, pltpu.SemaphoreType.DMA((9,)), *remote,
            ],
            compiler_params=pltpu.CompilerParams(collective_id=0, has_side_effects=True, vmem_limit_bytes=K1_LIMIT << 20),
        )(*(pltpu.with_memory_space_constraint(a, pltpu.HBM) for a in from_hbm))

        x2, sums2, _, _, _, _, ot = pl.pallas_call(
            _attn_kernel,
            out_shape=[x_out, sums_out, *qkv_out, pltpu.VMEM((n_ch, n_pos), BF16)],
            in_specs=[vmem] * 9,
            out_specs=[vmem] * 7,
            input_output_aliases={5: 2, 6: 3, 7: 4, 8: 5},
            compiler_params=pltpu.CompilerParams(vmem_limit_bytes=K2_LIMIT << 20),
        )(x1, sums1, attn_norm, proj, grp, *qkv)

        return pl.pallas_call(
            functools.partial(_last_kernel, n_row, n_col),
            out_shape=[pltpu.VMEM(latent.shape, BF16), x_out, sums_out],
            in_specs=[vmem] * 9,
            out_specs=[vmem] * 3,
            input_output_aliases={3: 1, 4: 2},
            scratch_shapes=[images, act, pltpu.VMEM((n_pos, n_ch), BF16), chan_sums, *remote],
            compiler_params=pltpu.CompilerParams(collective_id=1, has_side_effects=True, vmem_limit_bytes=K3_LIMIT << 20),
        )(x1, ot, proj, x2, sums2, res_norm, next_w, next_temb, grp)[0]

    spec_x = P('dp', 'row', 'col', None)
    return jax.shard_map(run_stage, mesh=mesh, in_specs=(spec_x, P('dp', None), P(), P(), P(), P(), P()), out_specs=spec_x, check_vma=False)
```
